8 devices in a mesh: tp: 2 (over z, y), ep: 4 (over x, core).
Axes of the slice: x: 2, y: 2, z: 1, core: 2. Of those that a mesh axis runs over, the one named last changes fastest.
Arguments:
- x: bfloat16 [1536, 1536], P(('ep', 'tp'))
- grad_y: bfloat16 [1536, 1536], P(('ep', 'tp'))
- w_router: bfloat16 [1536, 64], replicated
- w_gate: bfloat16 [64, 1536, 512], P('ep', None, 'tp')
- w_up: bfloat16 [64, 1536, 512], P('ep', None, 'tp')
- w_down: bfloat16 [64, 512, 1536], P('ep', 'tp')
- ws_gate: bfloat16 [1536, 1024], P(None, 'tp')
- ws_up: bfloat16 [1536, 1024], P(None, 'tp')
- ws_down: bfloat16 [1024, 1536], P('tp')
- topk_idx: int32 [1536, 6], P(('ep', 'tp'))
Outputs:
- output 1: bfloat16 [1536, 1536], P(('ep', 'tp'))
- output 2: bfloat16 [1536, 1536], P(('ep', 'tp'))
- output 3: float32 [1536, 64], replicated
- output 4: float32 [64, 1536, 512], P('ep', None, 'tp')
- output 5: float32 [64, 1536, 512], P('ep', None, 'tp')
- output 6: float32 [64, 512, 1536], P('ep', 'tp')
- output 7: float32 [1536, 1024], P(None, 'tp')
- output 8: float32 [1536, 1024], P(None, 'tp')
- output 9: float32 [1024, 1536], P('tp')
All inputs are finite; a program needn't handle non-finite values.
Results may differ from the reference program's by a relative error of at most 0.0131065.
Values are sent between devices in bfloat16 or wider.
A program may use at most 1 GiB of HBM per device.

```python
import jax
import jax.numpy as jnp
from jax import lax

D = 1536
EXPERTS = 64
FF = 512
SHARED_FF = 1024
TOP = 6
TOK = 192
TP = 2
EP = 4

GATE_SCALE = 16.0


def capacity():
    groups = TOP // 2
    most = groups * TOK // (2 * EP) + min(groups, EP // 2) * TOK // EP
    per_group = EXPERTS // EP
    return (2 * most + per_group - 1) // per_group


def draw_routes(key):
    devices = TP * EP
    groups = TOP // 2
    half_tok = TOK // 2
    per_group = EXPERTS // EP
    role_key, group_key, local_key = jax.random.split(key, 3)
    role_ids = jax.vmap(lambda sub_key: jax.random.permutation(sub_key, TOK))(jax.random.split(role_key, devices))
    base_group = jnp.where(role_ids < half_tok, role_ids % EP, role_ids % (EP // 2))
    visited = (base_group[:, :, None] + jnp.arange(groups)[None, None, :]) % EP
    hit_map = jax.nn.one_hot(visited.reshape(devices, TOK * groups), EP, dtype=jnp.int32)
    visit_num = jnp.sum((jnp.cumsum(hit_map, axis=1) - hit_map) * hit_map, axis=2).reshape(devices, TOK, groups)
    local_ids = (2 * visit_num[:, :, :, None] + jnp.arange(2)[None, None, None, :]) % per_group
    group_perm = jax.vmap(lambda sub_key: jax.random.permutation(sub_key, EP))(jax.random.split(group_key, devices))
    local_perm = jax.vmap(lambda sub_key: jax.random.permutation(sub_key, per_group))(jax.random.split(local_key, devices * EP)).reshape(devices, EP * per_group)
    true_group = jnp.take_along_axis(group_perm, visited.reshape(devices, TOK * groups), axis=1).reshape(devices, TOK, groups, 1)
    position = (true_group * per_group + local_ids).reshape(devices, TOK * TOP)
    local_pick = jnp.take_along_axis(local_perm, position, axis=1).reshape(devices, TOK, groups, 2)
    expert_ids = true_group * per_group + local_pick
    return expert_ids.reshape(devices * TOK, TOP).astype(jnp.int32)


def normal_bf16(key, arr_shape, std_dev):
    return (jax.random.normal(key, arr_shape, jnp.float32) * std_dev).astype(jnp.bfloat16)


def setup_inputs(seed: int = 0) -> dict:
    key_list = jax.random.split(jax.random.key(seed), 10)
    tokens = TOK * TP * EP
    return dict(
        x=normal_bf16(key_list[0], (tokens, D), 1.0),
        grad_y=normal_bf16(key_list[1], (tokens, D), 1.0),
        w_router=normal_bf16(key_list[2], (D, EXPERTS), D ** -0.5),
        w_gate=normal_bf16(key_list[3], (EXPERTS, D, FF), D ** -0.5),
        w_up=normal_bf16(key_list[4], (EXPERTS, D, FF), D ** -0.5),
        w_down=normal_bf16(key_list[5], (EXPERTS, FF, D), FF ** -0.5),
        ws_gate=normal_bf16(key_list[6], (D, SHARED_FF), D ** -0.5),
        ws_up=normal_bf16(key_list[7], (D, SHARED_FF), D ** -0.5),
        ws_down=normal_bf16(key_list[8], (SHARED_FF, D), SHARED_FF ** -0.5),
        topk_idx=draw_routes(key_list[9]),
    )


def swiglu(rows_in, w_a, w_b, w_c):
    gate_pre = jnp.dot(rows_in, w_a).astype(jnp.bfloat16).astype(jnp.float32)
    up_pre = jnp.dot(rows_in, w_b).astype(jnp.bfloat16).astype(jnp.float32)
    hidden = (jax.nn.silu(gate_pre) * up_pre).astype(jnp.bfloat16).astype(jnp.float32)
    return jnp.dot(hidden, w_c)


def reference(x, grad_y, w_router, w_gate, w_up, w_down, ws_gate, ws_up, ws_down, topk_idx):
    tokens = x.shape[0]
    cap_all = capacity() * TP * EP
    hit_count = jnp.sum(jax.nn.one_hot(topk_idx, EXPERTS, dtype=jnp.int32), axis=1)
    slot_rank = jnp.cumsum(hit_count, axis=0) - hit_count
    slot_of = topk_idx * cap_all + jnp.take_along_axis(slot_rank, topk_idx, axis=1)
    token_ids = jnp.broadcast_to(jnp.arange(tokens, dtype=jnp.int32)[:, None], slot_of.shape)
    slot_owner = jnp.zeros((EXPERTS * cap_all,), jnp.int32).at[slot_of.reshape(-1)].set(token_ids.reshape(-1)).reshape(EXPERTS, cap_all)

    def forward(x_wide, router_w, gate_w, up_w, down_w, sgate_w, sup_w, sdown_w):
        router_probs = jax.nn.softmax(jnp.dot(x_wide, router_w), axis=-1)
        route_gates = GATE_SCALE * jnp.take_along_axis(router_probs, topk_idx, axis=1)
        total = swiglu(x_wide, sgate_w, sup_w, sdown_w)

        def one_expert(operands):
            owner_ids, w_a, w_b, w_c = operands
            expert_rows = jnp.take(x_wide, owner_ids, axis=0).astype(jnp.bfloat16).astype(jnp.float32)
            return swiglu(expert_rows, w_a, w_b, w_c).astype(jnp.bfloat16)

        expert_out = lax.map(jax.checkpoint(one_expert), (slot_owner, gate_w, up_w, down_w)).reshape(EXPERTS * cap_all, D)
        for k in range(TOP):
            total = total + route_gates[:, k:k + 1] * jnp.take(expert_out, slot_of[:, k], axis=0).astype(jnp.float32)
        return total.astype(jnp.bfloat16)

    y_out, pullback = jax.vjp(forward, x.astype(jnp.float32), w_router.astype(jnp.float32), w_gate.astype(jnp.float32), w_up.astype(jnp.float32), w_down.astype(jnp.float32), ws_gate.astype(jnp.float32), ws_up.astype(jnp.float32), ws_down.astype(jnp.float32))
    grads = pullback(grad_y)
    return (y_out, grads[0].astype(jnp.bfloat16), grads[1], grads[2], grads[3], grads[4], grads[5], grads[6], grads[7])
```

```python
import functools

import jax
import jax.numpy as jnp
from jax import lax
from jax.experimental import pallas as pl
from jax.experimental.pallas import tpu as pltpu
from jax.sharding import PartitionSpec as P

GATE_SCALE = 16.0
BF16 = jnp.bfloat16
F32 = jnp.float32
FWD_CHUNKS = (2, 4, 10)
BWD_CHUNKS = (10, 4, 2)

NN = (((1,), (0,)), ((), ()))
NT = (((1,), (1,)), ((), ()))
TN = (((0,), (0,)), ((), ()))


def dot(a, b, dims=NN):
    return lax.dot_general(a, b, dims, preferred_element_type=F32)


def sigmoid(v):
    return 1.0 / (1.0 + jnp.exp(-jnp.maximum(v, -88.0)))


def swiglu_fwd(a, b):
    return (a * sigmoid(a) * b).astype(BF16)


def swiglu_bwd(a, b, dh):
    sig = sigmoid(a)
    silu = a * sig
    h = (silu * b).astype(BF16)
    da = (dh * b * (sig * (1.0 + a * (1.0 - sig)))).astype(BF16)
    db = (dh * silu).astype(BF16)
    return h, da, db


def rounded(v):
    return v.astype(BF16).astype(F32)


def half_rows(cap, ep_size):
    half = cap * ep_size
    return half, half + (-half) % 8


def store_parts(parity, part, send_ref, own_ref, half, padded):
    shift = padded - half

    @pl.when(parity == 0)
    def _():
        send_ref[0:half, :] = part[0:half]
        own_ref[0:half, :] = part[padded:padded + half]

    @pl.when(parity == 1)
    def _():
        send_ref[half:2 * half, :] = part[shift:padded]
        own_ref[half:2 * half, :] = part[padded + shift:2 * padded]


def pick_matrix(row_ref, rows):
    ids = row_ref[0]
    iota = lax.broadcasted_iota(jnp.int32, (rows, ids.shape[1]), 0)
    return iota == ids


def fwd_kernel(half, padded, x_ref, row_ref, w1_ref, w3_ref, w2_ref, send_ref, own_ref):
    hit = pick_matrix(row_ref, 2 * padded)
    rows = dot(jnp.where(hit, 1.0, 0.0).astype(BF16), x_ref[...]).astype(BF16)
    a = rounded(dot(rows, w1_ref[0]))
    b = rounded(dot(rows, w3_ref[0]))
    h = swiglu_fwd(a, b)
    part = dot(h, w2_ref[0])
    store_parts(pl.program_id(0) % 2, part, send_ref, own_ref, half, padded)


def bwd_kernel(half, padded, starts, x_ref, dy_ref, row_ref, gate_ref, w1_ref, w3_ref, w2_ref, *outs):
    dw1_ref, dw3_ref, dw2_ref = outs[:3]
    e = pl.program_id(0)
    hit = pick_matrix(row_ref, 2 * padded)
    pick = jnp.where(hit, 1.0, 0.0).astype(BF16)
    rows = dot(pick, x_ref[...]).astype(BF16)
    gates = jnp.sum(jnp.where(hit, gate_ref[0], 0.0), axis=1, keepdims=True)
    d_out = (dot(pick, dy_ref[...]) * gates).astype(BF16)
    a = rounded(dot(rows, w1_ref[0]))
    b = rounded(dot(rows, w3_ref[0]))
    dh = rounded(dot(d_out, w2_ref[0], NT))
    h, da, db = swiglu_bwd(a, b, dh)
    dw2_ref[0] = dot(h, d_out, TN)
    dw1_ref[0] = dot(rows, da, TN)
    dw3_ref[0] = dot(rows, db, TN)
    part = dot(da, w1_ref[0], NT) + dot(db, w3_ref[0], NT)
    for j in range(len(starts) - 1):
        @pl.when((e >= starts[j]) & (e < starts[j + 1]))
        def _():
            store_parts(e % 2, part, outs[3 + 2 * j], outs[4 + 2 * j], half, padded)


def expert_fwd(start, count, half, padded, x_all, row_ids, w_gate, w_up, w_down):
    tokens, model = x_all.shape
    width = w_gate.shape[2]
    out = jax.ShapeDtypeStruct((count * half, model), F32)
    return pl.pallas_call(
        functools.partial(fwd_kernel, half, padded),
        grid=(count,),
        in_specs=[
            pl.BlockSpec((tokens, model), lambda i: (0, 0), pipeline_mode=pl.Buffered(1)),
            pl.BlockSpec((1, 1, tokens), lambda i: (start + i, 0, 0)),
            pl.BlockSpec((1, model, width), lambda i: (start + i, 0, 0)),
            pl.BlockSpec((1, model, width), lambda i: (start + i, 0, 0)),
            pl.BlockSpec((1, width, model), lambda i: (start + i, 0, 0)),
        ],
        out_specs=[pl.BlockSpec((2 * half, model), lambda i: (i // 2, 0))] * 2,
        out_shape=[out, out],
        cost_estimate=pl.CostEstimate(
            flops=count * 2 * 2 * padded * model * (tokens + 3 * width),
            bytes_accessed=count * (6 * model * width + 8 * half * model) + 2 * tokens * model,
            transcendentals=count * 2 * padded * width),
        compiler_params=pltpu.CompilerParams(dimension_semantics=('arbitrary',), vmem_limit_bytes=48 << 20),
        name='expert_fwd_%d' % start,
    )(x_all, row_ids, w_gate, w_up, w_down)


def expert_bwd(chunks, half, padded, x_all, dy_all, row_ids, gates, w_gate, w_up, w_down):
    tokens, model = x_all.shape
    count, _, width = w_gate.shape
    starts = [0]
    for c in chunks:
        starts.append(starts[-1] + c)

    def chunk_spec(j):
        lo, n = starts[j] // 2, chunks[j] // 2
        return pl.BlockSpec((2 * half, model), lambda i: (jnp.clip(i // 2 - lo, 0, n - 1), 0))

    part_specs, part_shapes = [], []
    for j, c in enumerate(chunks):
        part_specs += [chunk_spec(j)] * 2
        part_shapes += [jax.ShapeDtypeStruct((c * half, model), F32)] * 2
    outs = pl.pallas_call(
        functools.partial(bwd_kernel, half, padded, starts),
        grid=(count,),
        in_specs=[
            pl.BlockSpec((tokens, model), lambda i: (0, 0), pipeline_mode=pl.Buffered(1)),
            pl.BlockSpec((tokens, model), lambda i: (0, 0), pipeline_mode=pl.Buffered(1)),
            pl.BlockSpec((1, 1, tokens), lambda i: (i, 0, 0)),
            pl.BlockSpec((1, 1, tokens), lambda i: (i, 0, 0)),
            pl.BlockSpec((1, model, width), lambda i: (i, 0, 0)),
            pl.BlockSpec((1, model, width), lambda i: (i, 0, 0)),
            pl.BlockSpec((1, width, model), lambda i: (i, 0, 0)),
        ],
        out_specs=[
            pl.BlockSpec((1, model, width), lambda i: (i, 0, 0)),
            pl.BlockSpec((1, model, width), lambda i: (i, 0, 0)),
            pl.BlockSpec((1, width, model), lambda i: (i, 0, 0)),
        ] + part_specs,
        out_shape=[
            jax.ShapeDtypeStruct((count, model, width), F32),
            jax.ShapeDtypeStruct((count, model, width), F32),
            jax.ShapeDtypeStruct((count, width, model), F32),
        ] + part_shapes,
        cost_estimate=pl.CostEstimate(
            flops=count * 2 * 2 * padded * model * (2 * tokens + 8 * width),
            bytes_accessed=count * (18 * model * width + 8 * half * model) + 4 * tokens * model,
            transcendentals=count * 2 * padded * width),
        compiler_params=pltpu.CompilerParams(dimension_semantics=('arbitrary',), vmem_limit_bytes=60 << 20),
        name='expert_bwd',
    )(x_all, dy_all, row_ids, gates, w_gate, w_up, w_down)
    return outs[:3], [(outs[3 + 2 * j], outs[4 + 2 * j]) for j in range(len(chunks))]


def split3(v):
    hi = lax.reduce_precision(v, 8, 7)
    rest = v - hi
    mid = lax.reduce_precision(rest, 8, 7)
    low = rest - mid
    return hi.astype(BF16), mid.astype(BF16), low.astype(BF16)


def solution(mesh):
    tp_size = mesh.shape['tp']
    ep_size = mesh.shape['ep']
    swap = [(i, tp_size - 1 - i) for i in range(tp_size)]

    def device_step(x, grad_y, w_router, w_gate, w_up, w_down, ws_gate, ws_up, ws_down, topk_idx):
        tok, model = x.shape
        top_k = topk_idx.shape[1]
        experts = w_router.shape[1]
        local_exp = w_gate.shape[0]
        groups = top_k // 2
        most = groups * tok // (2 * ep_size) + min(groups, ep_size // 2) * tok // ep_size
        cap = (2 * most + local_exp - 1) // local_exp
        half, padded = half_rows(cap, ep_size)
        shift = padded - half
        ep_i = lax.axis_index('ep')
        tp_i = lax.axis_index('tp')
        devices = ep_size * tp_size

        x_all = lax.all_gather(x, ('ep', 'tp'), axis=0, tiled=True)
        idx_all = lax.all_gather(topk_idx, ('ep', 'tp'), axis=0, tiled=True)
        dy_all = lax.all_gather(grad_y, ('ep', 'tp'), axis=0, tiled=True)

        lower = (lax.broadcasted_iota(jnp.int32, (tok, tok), 0) > lax.broadcasted_iota(jnp.int32, (tok, tok), 1)).astype(BF16)
        local_ids = ep_i * local_exp + jnp.arange(local_exp, dtype=jnp.int32)
        hit = jnp.any(idx_all.reshape(devices, 1, tok, top_k) == local_ids[None, :, None, None], axis=3)
        rank = jnp.einsum('dej,ij->edi', hit.astype(BF16), lower, preferred_element_type=F32).astype(jnp.int32)
        dev = jnp.arange(devices, dtype=jnp.int32)
        is_own = (dev % tp_size) == tp_i
        parity = jnp.arange(local_exp, dtype=jnp.int32) % 2
        base = (jnp.where(is_own, padded, 0) + (dev // tp_size) * cap)[None, :] + (parity * shift)[:, None]
        row_ids = jnp.where(jnp.transpose(hit, (1, 0, 2)), base[:, :, None] + rank, -1).reshape(local_exp, 1, devices * tok)

        fwd_parts = []
        start = 0
        for count in FWD_CHUNKS:
            send, own = expert_fwd(start, count, half, padded, x_all, row_ids, w_gate, w_up, w_down)
            fwd_parts.append((lax.ppermute(send, 'tp', swap), own))
            start += count

        logits_t = jnp.einsum('de,td->et', w_router, x_all, preferred_element_type=F32)
        probs_t = jax.nn.softmax(logits_t, axis=0)
        gates_local = GATE_SCALE * lax.dynamic_slice_in_dim(probs_t, ep_i * local_exp, local_exp, 0).reshape(local_exp, 1, devices * tok)

        (d_w_gate, d_w_up, d_w_down), bwd_out = expert_bwd(BWD_CHUNKS, half, padded, x_all, dy_all, row_ids, gates_local, w_gate, w_up, w_down)
        bwd_parts = [(lax.ppermute(send, 'tp', swap), own) for send, own in bwd_out]

        def other_half(w):
            n = w.shape[0] // ep_size
            quarter = lax.dynamic_slice_in_dim(w, ep_i * n, n, 0)
            return lax.all_gather(lax.ppermute(quarter, 'tp', swap), 'ep', axis=0, tiled=True)

        ws_other = (other_half(ws_gate), other_half(ws_up), other_half(ws_down))

        shared = jnp.zeros((tok, model), F32)
        dx_shared = jnp.zeros((tok, model), F32)
        for wg, wu, wd in ((ws_gate, ws_up, ws_down), ws_other):
            a = rounded(dot(x, wg))
            b = rounded(dot(x, wu))
            dh = rounded(dot(grad_y, wd, NT))
            h, da, db = swiglu_bwd(a, b, dh)
            shared = shared + dot(h, wd)
            dx_shared = dx_shared + dot(da, wg, NT) + dot(db, wu, NT)
        a = rounded(dot(x_all, ws_gate))
        b = rounded(dot(x_all, ws_up))
        dh = rounded(dot(dy_all, ws_down, NT))
        h, da, db = swiglu_bwd(a, b, dh)
        ds_down = dot(h, dy_all, TN)
        ds_gate = dot(x_all, da, TN)
        ds_up = dot(x_all, db, TN)

        def give_back(parts, count):
            recv, own = parts
            rows = (recv + own).astype(BF16)
            new = jnp.arange(ep_size * count * cap, dtype=jnp.int32)
            src, rest = new // (count * cap), new % (count * cap)
            old = (rest // cap) * half + src * cap + rest % cap
            perm = (old[:, None] == jnp.arange(count * half, dtype=jnp.int32)[None, :]).astype(BF16)
            out = dot(perm, rows).astype(BF16).reshape(ep_size, count * cap, model)
            return lax.all_to_all(out, 'ep', 0, 0).reshape(ep_size * count * cap, model)

        hit_own = jnp.any(topk_idx[:, None, :] == jnp.arange(experts, dtype=jnp.int32)[None, :, None], axis=2)
        rank_own = dot(lower, hit_own.astype(BF16)).astype(jnp.int32)
        probs = jax.nn.softmax(dot(x, w_router), axis=-1)

        def columns(v, start, count):
            picked = v.reshape(tok, ep_size, local_exp)[:, :, start:start + count]
            return jnp.broadcast_to(picked[..., None], (tok, ep_size, count, cap)).reshape(tok, ep_size * count * cap)

        def slot_hits(start, count):
            slot = jnp.arange(ep_size * count * cap, dtype=jnp.int32) % cap
            want = jnp.where(hit_own, rank_own, -1)
            return columns(want, start, count) == slot[None, :]

        routed = jnp.zeros((tok, model), F32)
        d_scores = []
        start = 0
        for parts, count in zip(fwd_parts, FWD_CHUNKS):
            back = give_back(parts, count)
            hits = slot_hits(start, count)
            gates = jnp.where(hits, GATE_SCALE * columns(probs, start, count), 0.0)
            for piece in split3(gates):
                routed = routed + dot(piece, back)
            score = jnp.where(hits, dot(grad_y, back, NT), 0.0)
            d_scores.append(jnp.sum(score.reshape(tok, ep_size, count, cap), axis=3))
            start += count
        y_out = (shared + routed).astype(BF16)

        d_scores = GATE_SCALE * jnp.concatenate(d_scores, axis=2).reshape(tok, experts)
        d_logits = probs * (d_scores - jnp.sum(probs * d_scores, axis=-1, keepdims=True))
        d_router = lax.psum(jnp.einsum('td,te->de', x, d_logits, preferred_element_type=F32), ('tp', 'ep'))
        dx_sum = jnp.einsum('te,de->td', d_logits, w_router, preferred_element_type=F32) + dx_shared

        start = 0
        for parts, count in zip(bwd_parts, BWD_CHUNKS):
            back = give_back(parts, count)
            dx_sum = dx_sum + dot(slot_hits(start, count).astype(BF16), back)
            start += count
        return y_out, dx_sum.astype(BF16), d_router, d_w_gate, d_w_up, d_w_down, ds_gate, ds_up, ds_down

    tok_spec = P(('ep', 'tp'), None)
    in_specs = (tok_spec, tok_spec, P(None, None), P('ep', None, 'tp'), P('ep', None, 'tp'), P('ep', 'tp', None), P(None, 'tp'), P(None, 'tp'), P('tp', None), tok_spec)
    out_specs = (tok_spec, tok_spec, P(None, None), P('ep', None, 'tp'), P('ep', None, 'tp'), P('ep', 'tp', None), P(None, 'tp'), P(None, 'tp'), P('tp', None))
    return jax.shard_map(device_step, mesh=mesh, in_specs=in_specs, out_specs=out_specs, check_vma=False)
```

```python
import functools

import jax
import jax.numpy as jnp
from jax import lax
from jax.experimental import pallas as pl
from jax.experimental.pallas import tpu as pltpu
from jax.sharding import PartitionSpec as P


GATE_SCALE = 16.0
BF16 = jnp.bfloat16
F32 = jnp.float32
FWD_CHUNKS = (2, 6, 8)
BWD_CHUNKS = (8, 6, 2)
MESH = pl.DeviceIdType.MESH

NN = (((1,), (0,)), ((), ()))
NT = (((1,), (1,)), ((), ()))
TN = (((0,), (0,)), ((), ()))


def dot(a, b, dims=NN):
    return lax.dot_general(a, b, dims, preferred_element_type=F32)


def sigmoid(v):
    return 1.0 / (1.0 + jnp.exp(-jnp.maximum(v, -88.0)))


def swiglu_fwd(a, b):
    return (a * sigmoid(a) * b).astype(BF16)


def swiglu_bwd(a, b, dh):
    sig = sigmoid(a)
    silu = a * sig
    h = (silu * b).astype(BF16)
    da = (dh * b * (sig * (1.0 + a * (1.0 - sig)))).astype(BF16)
    db = (dh * silu).astype(BF16)
    return h, da, db


def rounded(v):
    return v.astype(BF16).astype(F32)


def half_rows(cap, ep_size):
    half = cap * ep_size
    return half, half + (-half) % 8


def store_parts(parity, part, send_ref, own_ref, half, padded):
    shift = padded - half

    @pl.when(parity == 0)
    def _():
        send_ref[0:half, :] = part[0:half]
        own_ref[0:half, :] = part[padded:padded + half]

    @pl.when(parity == 1)
    def _():
        send_ref[half:2 * half, :] = part[shift:padded]
        own_ref[half:2 * half, :] = part[padded + shift:2 * padded]


def pick_matrix(row_ref, rows):
    ids = row_ref[0]
    iota = lax.broadcasted_iota(jnp.int32, (rows, ids.shape[1]), 0)
    return iota == ids


def fwd_kernel(half, padded, x_ref, row_ref, w1_ref, w3_ref, w2_ref, send_ref, own_ref):
    hit = pick_matrix(row_ref, 2 * padded)
    rows = dot(jnp.where(hit, 1.0, 0.0).astype(BF16), x_ref[...]).astype(BF16)
    a = rounded(dot(rows, w1_ref[0]))
    b = rounded(dot(rows, w3_ref[0]))
    h = swiglu_fwd(a, b)
    part = dot(h, w2_ref[0])
    store_parts(pl.program_id(0) % 2, part, send_ref, own_ref, half, padded)


def bwd_kernel(half, padded, starts, x_ref, dy_ref, row_ref, gate_ref, w1_ref, w3_ref, w2_ref, *outs):
    dw1_ref, dw3_ref, dw2_ref = outs[:3]
    e = pl.program_id(0)
    hit = pick_matrix(row_ref, 2 * padded)
    pick = jnp.where(hit, 1.0, 0.0).astype(BF16)
    rows = dot(pick, x_ref[...]).astype(BF16)
    gates = jnp.sum(jnp.where(hit, gate_ref[0], 0.0), axis=1, keepdims=True)
    d_out = (dot(pick, dy_ref[...]) * gates).astype(BF16)
    a = rounded(dot(rows, w1_ref[0]))
    b = rounded(dot(rows, w3_ref[0]))
    dh = rounded(dot(d_out, w2_ref[0], NT))
    h, da, db = swiglu_bwd(a, b, dh)
    dw2_ref[0] = dot(h, d_out, TN)
    dw1_ref[0] = dot(rows, da, TN)
    dw3_ref[0] = dot(rows, db, TN)
    part = dot(da, w1_ref[0], NT) + dot(db, w3_ref[0], NT)
    for j in range(len(starts) - 1):
        @pl.when((e >= starts[j]) & (e < starts[j + 1]))
        def _():
            store_parts(e % 2, part, outs[3 + 2 * j], outs[4 + 2 * j], half, padded)


def expert_fwd(start, count, half, padded, x_all, row_ids, w_gate, w_up, w_down):
    tokens, model = x_all.shape
    width = w_gate.shape[2]
    out = jax.ShapeDtypeStruct((count * half, model), F32)
    return pl.pallas_call(
        functools.partial(fwd_kernel, half, padded),
        grid=(count,),
        in_specs=[
            pl.BlockSpec((tokens, model), lambda i: (0, 0), pipeline_mode=pl.Buffered(1)),
            pl.BlockSpec((1, 1, tokens), lambda i: (start + i, 0, 0)),
            pl.BlockSpec((1, model, width), lambda i: (start + i, 0, 0)),
            pl.BlockSpec((1, model, width), lambda i: (start + i, 0, 0)),
            pl.BlockSpec((1, width, model), lambda i: (start + i, 0, 0)),
        ],
        out_specs=[pl.BlockSpec((2 * half, model), lambda i: (i // 2, 0))] * 2,
        out_shape=[out, out],
        cost_estimate=pl.CostEstimate(
            flops=count * 2 * 2 * padded * model * (tokens + 3 * width),
            bytes_accessed=count * (6 * model * width + 8 * half * model) + 2 * tokens * model,
            transcendentals=count * 2 * padded * width),
        compiler_params=pltpu.CompilerParams(dimension_semantics=('arbitrary',), vmem_limit_bytes=48 << 20),
    )(x_all, row_ids, w_gate, w_up, w_down)


def expert_bwd(chunks, half, padded, x_all, dy_all, row_ids, gates, w_gate, w_up, w_down):
    tokens, model = x_all.shape
    count, _, width = w_gate.shape
    starts = [0]
    for c in chunks:
        starts.append(starts[-1] + c)

    def chunk_spec(j):
        lo, n = starts[j] // 2, chunks[j] // 2
        return pl.BlockSpec((2 * half, model), lambda i: (jnp.clip(i // 2 - lo, 0, n - 1), 0))

    part_specs, part_shapes = [], []
    for j, c in enumerate(chunks):
        part_specs += [chunk_spec(j)] * 2
        part_shapes += [jax.ShapeDtypeStruct((c * half, model), F32)] * 2
    outs = pl.pallas_call(
        functools.partial(bwd_kernel, half, padded, starts),
        grid=(count,),
        in_specs=[
            pl.BlockSpec((tokens, model), lambda i: (0, 0), pipeline_mode=pl.Buffered(1)),
            pl.BlockSpec((tokens, model), lambda i: (0, 0), pipeline_mode=pl.Buffered(1)),
            pl.BlockSpec((1, 1, tokens), lambda i: (i, 0, 0)),
            pl.BlockSpec((1, 1, tokens), lambda i: (i, 0, 0)),
            pl.BlockSpec((1, model, width), lambda i: (i, 0, 0)),
            pl.BlockSpec((1, model, width), lambda i: (i, 0, 0)),
            pl.BlockSpec((1, width, model), lambda i: (i, 0, 0)),
        ],
        out_specs=[
            pl.BlockSpec((1, model, width), lambda i: (i, 0, 0)),
            pl.BlockSpec((1, model, width), lambda i: (i, 0, 0)),
            pl.BlockSpec((1, width, model), lambda i: (i, 0, 0)),
        ] + part_specs,
        out_shape=[
            jax.ShapeDtypeStruct((count, model, width), F32),
            jax.ShapeDtypeStruct((count, model, width), F32),
            jax.ShapeDtypeStruct((count, width, model), F32),
        ] + part_shapes,
        cost_estimate=pl.CostEstimate(
            flops=count * 2 * 2 * padded * model * (2 * tokens + 8 * width),
            bytes_accessed=count * (18 * model * width + 8 * half * model) + 4 * tokens * model,
            transcendentals=count * 2 * padded * width),
        compiler_params=pltpu.CompilerParams(dimension_semantics=('arbitrary',), vmem_limit_bytes=60 << 20),
        name='expert_bwd',
    )(x_all, dy_all, row_ids, gates, w_gate, w_up, w_down)
    return outs[:3], [(outs[3 + 2 * j], outs[4 + 2 * j]) for j in range(len(chunks))]


def split3(v):
    hi = lax.reduce_precision(v, 8, 7)
    rest = v - hi
    mid = lax.reduce_precision(rest, 8, 7)
    low = rest - mid
    return hi.astype(BF16), mid.astype(BF16), low.astype(BF16)


def core_partner(ep):
    return ep + 1 - 2 * (ep % 2)


def gather_kernel(x_ref, idx_ref, dy_ref, wd_ref, x_all, idx_all, dy_pair, wd_part, send_sem, recv_sem, idx_send, idx_recv, local_sem):
    tp = lax.axis_index('tp')
    ep = lax.axis_index('ep')
    eps = x_all.shape[0] // 2
    half = eps // 2
    tp_o = 1 - tp
    ep_x = (ep + half) % eps
    ep_c = core_partner(ep)

    def slot(e, t):
        return e * 2 + t

    others = [(tp_o, ep)]
    for k in range(1, eps):
        others += [(tp, (ep + k) % eps), (tp_o, (ep + k) % eps)]
    barrier = pltpu.get_barrier_semaphore()
    for t, e in others:
        pl.semaphore_signal(barrier, inc=1, device_id={'tp': t, 'ep': e}, device_id_type=MESH)
    pl.semaphore_wait(barrier, len(others))

    def send(k, src, dst, t, e):
        copy = pltpu.make_async_remote_copy(
            src_ref=src, dst_ref=dst, send_sem=send_sem.at[k], recv_sem=recv_sem.at[k],
            device_id={'tp': t, 'ep': e}, device_id_type=MESH)
        copy.start()
        return copy

    def block(e, t):
        return x_all.at[slot(e, t)]

    mine = block(ep, tp)
    to_y = send(0, x_ref, mine, tp_o, ep)
    to_x = send(1, x_ref, mine, tp, ep_x)
    to_c = send(2, x_ref, mine, tp, ep_c)
    own_idx = idx_all.at[slot(ep, tp)]
    idx_copies = []
    for k, (t, e) in enumerate(others):
        copy = pltpu.make_async_remote_copy(
            src_ref=idx_ref, dst_ref=own_idx, send_sem=idx_send.at[k], recv_sem=idx_recv.at[k],
            device_id={'tp': t, 'ep': e}, device_id_type=MESH)
        copy.start()
        idx_copies.append(copy)
    local = [
        pltpu.make_async_copy(x_ref, mine, local_sem.at[0]),
        pltpu.make_async_copy(idx_ref, own_idx, local_sem.at[1]),
        pltpu.make_async_copy(dy_ref, dy_pair.at[tp], local_sem.at[2]),
    ]
    for copy in local:
        copy.start()
    dy_y = send(3, dy_ref, dy_pair.at[tp], tp_o, ep)
    rows = wd_part.shape[0]
    wd_y = send(4, wd_ref.at[pl.ds(ep * rows, rows)], wd_part, tp_o, ep)

    to_y.wait_recv()
    y_to_x = send(5, block(ep, tp_o), block(ep, tp_o), tp, ep_x)
    y_to_c = send(6, block(ep, tp_o), block(ep, tp_o), tp, ep_c)
    to_x.wait_recv()
    x_to_c = send(7, block(ep_x, tp), block(ep_x, tp), tp, ep_c)
    y_to_x.wait_recv()
    xy_to_c = send(8, block(ep_x, tp_o), block(ep_x, tp_o), tp, ep_c)
    for copy in (to_c, dy_y, wd_y, y_to_c, x_to_c, xy_to_c):
        copy.wait_recv()
    for copy in idx_copies:
        copy.wait_recv()
    for copy in local:
        copy.wait()
    for copy in (to_y, to_x, to_c, dy_y, wd_y, y_to_x, y_to_c, x_to_c, xy_to_c):
        copy.wait_send()
    for copy in idx_copies:
        copy.wait_send()


def gather_rows(devices, ep_size, x, idx_t, dy, ws_down):
    _, model = x.shape
    any_spec = pl.BlockSpec(memory_space=pl.ANY)
    return pl.pallas_call(
        gather_kernel,
        in_specs=[any_spec] * 4,
        out_specs=[any_spec] * 4,
        out_shape=[
            jax.ShapeDtypeStruct((devices,) + x.shape, x.dtype),
            jax.ShapeDtypeStruct((devices,) + idx_t.shape, idx_t.dtype),
            jax.ShapeDtypeStruct((2,) + dy.shape, dy.dtype),
            jax.ShapeDtypeStruct((ws_down.shape[0] // ep_size, model), ws_down.dtype),
        ],
        scratch_shapes=[
            pltpu.SemaphoreType.DMA((9,)),
            pltpu.SemaphoreType.DMA((9,)),
            pltpu.SemaphoreType.DMA((devices - 1,)),
            pltpu.SemaphoreType.DMA((devices - 1,)),
            pltpu.SemaphoreType.DMA((3,)),
        ],
        cost_estimate=pl.CostEstimate(flops=60_000_000_000, bytes_accessed=4 * devices * x.size, transcendentals=0),
        compiler_params=pltpu.CompilerParams(collective_id=0, has_side_effects=True),
        name='gather_rows',
    )(x, idx_t, dy, ws_down)


def solution(mesh):
    tp_size = mesh.shape['tp']
    ep_size = mesh.shape['ep']
    swap_tp = [(i, tp_size - 1 - i) for i in range(tp_size)]
    swap_x = [(i, (i + ep_size // 2) % ep_size) for i in range(ep_size)]
    swap_c = [(i, core_partner(i)) for i in range(ep_size)]

    def device_step(x, grad_y, w_router, w_gate, w_up, w_down, ws_gate, ws_up, ws_down, topk_idx):
        tok, model = x.shape
        top_k = topk_idx.shape[1]
        experts = w_router.shape[1]
        local_exp = w_gate.shape[0]
        groups = top_k // 2
        most = groups * tok // (2 * ep_size) + min(groups, ep_size // 2) * tok // ep_size
        cap = (2 * most + local_exp - 1) // local_exp
        half, padded = half_rows(cap, ep_size)
        shift = padded - half
        ep_i = lax.axis_index('ep')
        tp_i = lax.axis_index('tp')
        devices = ep_size * tp_size
        ep_order = (ep_i, (ep_i + ep_size // 2) % ep_size, core_partner(ep_i), core_partner((ep_i + ep_size // 2) % ep_size))

        def ep_pieces(piece):
            far = lax.ppermute(piece, 'ep', swap_x)
            return piece, far, lax.ppermute(piece, 'ep', swap_c), lax.ppermute(far, 'ep', swap_c)

        def ep_gather(piece):
            out = jnp.zeros((ep_size,) + piece.shape, piece.dtype)
            for e, part in zip(ep_order, ep_pieces(piece)):
                out = lax.dynamic_update_slice_in_dim(out, part[None], e, 0)
            return out

        x_blocks, idx_all, dy_pair, wd_part = gather_rows(devices, ep_size, x, topk_idx.T, grad_y, ws_down)
        x_all = x_blocks.reshape(devices * tok, model)

        width_q = ws_gate.shape[1] // ep_size
        quarter = jnp.concatenate([lax.dynamic_slice_in_dim(w, ep_i * width_q, width_q, 1) for w in (ws_gate, ws_up)], axis=1)
        quarter, x_all = lax.optimization_barrier((quarter, x_all))
        gu_part = lax.ppermute(quarter, 'tp', swap_tp)

        lower = (lax.broadcasted_iota(jnp.int32, (tok, tok), 0) > lax.broadcasted_iota(jnp.int32, (tok, tok), 1)).astype(BF16)
        local_ids = ep_i * local_exp + jnp.arange(local_exp, dtype=jnp.int32)
        hit = jnp.any(idx_all[None] == local_ids[:, None, None, None], axis=2)
        rank = jnp.einsum('edj,ij->edi', hit.astype(BF16), lower, preferred_element_type=F32).astype(jnp.int32)
        dev = jnp.arange(devices, dtype=jnp.int32)
        is_own = (dev % tp_size) == tp_i
        parity = jnp.arange(local_exp, dtype=jnp.int32) % 2
        base = (jnp.where(is_own, padded, 0) + (dev // tp_size) * cap)[None, :] + (parity * shift)[:, None]
        row_ids = jnp.where(hit, base[:, :, None] + rank, -1).reshape(local_exp, 1, devices * tok)

        fwd_parts = []
        start = 0
        rows_now = row_ids
        for count in FWD_CHUNKS:
            send, own = expert_fwd(start, count, half, padded, x_all, rows_now, w_gate, w_up, w_down)
            start += count
            rows_now, own = lax.optimization_barrier((rows_now, own))
            fwd_parts.append((lax.ppermute(send, 'tp', swap_tp), own))

        own0 = fwd_parts[-1][1]
        x, grad_y, x_all, topk_idx, w_router, rows_now, wd_part, own0 = lax.optimization_barrier(
            (x, grad_y, x_all, topk_idx, w_router, rows_now, wd_part, own0))
        fwd_parts[-1] = (fwd_parts[-1][0], own0)

        logits_t = jnp.einsum('de,td->et', w_router, x_all, preferred_element_type=F32)
        probs_t = jax.nn.softmax(logits_t, axis=0)
        gates_local = GATE_SCALE * lax.dynamic_slice_in_dim(probs_t, ep_i * local_exp, local_exp, 0).reshape(local_exp, 1, devices * tok)

        dy_all = ep_gather(dy_pair).reshape(devices * tok, model)
        (d_w_gate, d_w_up, d_w_down), bwd_out = expert_bwd(BWD_CHUNKS, half, padded, x_all, dy_all, rows_now, gates_local, w_gate, w_up, w_down)

        gu_other = ep_pieces(gu_part)
        wd_other = jnp.concatenate(ep_pieces(wd_part), axis=0)
        wg_other = jnp.concatenate([p[:, :width_q] for p in gu_other], axis=1)
        wu_other = jnp.concatenate([p[:, width_q:] for p in gu_other], axis=1)
        shared = jnp.zeros((tok, model), F32)
        dx_shared = jnp.zeros((tok, model), F32)
        for wg, wu, wd in ((ws_gate, ws_up, ws_down), (wg_other, wu_other, wd_other)):
            a = rounded(dot(x, wg))
            b = rounded(dot(x, wu))
            dh = rounded(dot(grad_y, wd, NT))
            h, da, db = swiglu_bwd(a, b, dh)
            shared = shared + dot(h, wd)
            dx_shared = dx_shared + dot(da, wg, NT) + dot(db, wu, NT)
        a = rounded(dot(x_all, ws_gate))
        b = rounded(dot(x_all, ws_up))
        dh = rounded(dot(dy_all, ws_down, NT))
        h, da, db = swiglu_bwd(a, b, dh)
        ds_down = dot(h, dy_all, TN)
        ds_gate = dot(x_all, da, TN)
        ds_up = dot(x_all, db, TN)

        def back_rows(count):
            return count * cap + (-count * cap) % 8

        def slot_index(count):
            new = jnp.arange(ep_size * back_rows(count), dtype=jnp.int32)
            block, rest = new // back_rows(count), new % back_rows(count)
            return block, rest // cap, rest % cap, rest < count * cap

        def give_back(parts, count):
            recv, own = parts
            rows = (recv + own).astype(BF16)
            src, exp, rank, valid = slot_index(count)
            old = jnp.where(valid, exp * half + src * cap + rank, -1)
            perm = (old[:, None] == jnp.arange(count * half, dtype=jnp.int32)[None, :]).astype(BF16)
            out = dot(perm, rows).astype(BF16).reshape(ep_size, back_rows(count), model)
            return lax.all_to_all(out, 'ep', 0, 0).reshape(ep_size * back_rows(count), model)

        hit_own = jnp.any(topk_idx[:, None, :] == jnp.arange(experts, dtype=jnp.int32)[None, :, None], axis=2)
        rank_own = dot(lower, hit_own.astype(BF16))
        want = jnp.where(hit_own, rank_own, -1.0).astype(BF16)
        probs = jax.nn.softmax(dot(x, w_router), axis=-1)
        prob_parts = split3(probs)

        def expand(start, count):
            grp, exp, rank, valid = slot_index(count)
            col = jnp.where(valid, grp * local_exp + start + exp, -1)
            table = (jnp.arange(experts, dtype=jnp.int32)[:, None] == col[None, :]).astype(BF16)
            return table, jnp.where(valid, rank, -2).astype(F32)[None, :]

        routed = jnp.zeros((tok, model), F32)
        d_scores = jnp.zeros((tok, experts), F32)
        start = 0
        for parts, count in zip(fwd_parts, FWD_CHUNKS):
            back = give_back(parts, count)
            table, rank = expand(start, count)
            hits = dot(want, table) == rank
            for piece in prob_parts:
                routed = routed + GATE_SCALE * dot(jnp.where(hits, dot(piece, table), 0.0).astype(BF16), back)
            score = jnp.where(hits, dot(grad_y, back, NT), 0.0)
            for piece in split3(score):
                d_scores = d_scores + dot(piece, table, NT)
            start += count
        y_out = (shared + routed).astype(BF16)

        d_scores = GATE_SCALE * d_scores
        d_logits = probs * (d_scores - jnp.sum(probs * d_scores, axis=-1, keepdims=True))
        d_other = lax.ppermute(d_logits, 'tp', swap_tp)
        d_logits_now, send1 = lax.optimization_barrier((d_logits, bwd_out[1][0]))
        d_other, send2 = lax.optimization_barrier((d_other, bwd_out[2][0]))
        bwd_parts = []
        for send, own in ((bwd_out[0][0], bwd_out[0][1]), (send1, bwd_out[1][1]), (send2, bwd_out[2][1])):
            bwd_parts.append((lax.ppermute(send, 'tp', swap_tp), own))
        d_pair = jnp.where(tp_i == 0, jnp.stack([d_logits, d_other]), jnp.stack([d_other, d_logits]))
        d_logits_all = ep_gather(d_pair).reshape(devices * tok, experts)
        d_router = jnp.zeros((model, experts), F32)
        for piece in split3(d_logits_all):
            d_router = d_router + dot(x_all, piece, TN)
        dx_sum = dx_shared
        for piece in split3(d_logits_now):
            dx_sum = dx_sum + dot(piece, w_router, NT)

        start = 0
        for parts, count in zip(bwd_parts, BWD_CHUNKS):
            back = give_back(parts, count)
            table, rank = expand(start, count)
            dx_sum = dx_sum + dot((dot(want, table) == rank).astype(BF16), back)
            start += count
        return y_out, dx_sum.astype(BF16), d_router, d_w_gate, d_w_up, d_w_down, ds_gate, ds_up, ds_down

    tok_spec = P(('ep', 'tp'), None)
    in_specs = (tok_spec, tok_spec, P(None, None), P('ep', None, 'tp'), P('ep', None, 'tp'), P('ep', 'tp', None), P(None, 'tp'), P(None, 'tp'), P('tp', None), tok_spec)
    out_specs = (tok_spec, tok_spec, P(None, None), P('ep', None, 'tp'), P('ep', None, 'tp'), P('ep', 'tp', None), P(None, 'tp'), P(None, 'tp'), P('tp', None))

    return jax.shard_map(device_step, mesh=mesh, in_specs=in_specs, out_specs=out_specs, check_vma=False)
```

```python
import functools

import jax
import jax.numpy as jnp
from jax import lax
from jax.experimental import pallas as pl
from jax.experimental.pallas import tpu as pltpu
from jax.sharding import PartitionSpec as P


GATE_SCALE = 16.0
BF16 = jnp.bfloat16
F32 = jnp.float32
FWD_CHUNKS = (2, 8, 6)
BWD_CHUNKS = 2
MESH = pl.DeviceIdType.MESH

NN = (((1,), (0,)), ((), ()))
NT = (((1,), (1,)), ((), ()))
TN = (((0,), (0,)), ((), ()))


def dot(a, b, dims=NN):
    return lax.dot_general(a, b, dims, preferred_element_type=F32)


def sigmoid(v):
    return 1.0 / (1.0 + jnp.exp(-jnp.maximum(v, -88.0)))


def swiglu_fwd(a, b):
    return (a * sigmoid(a) * b).astype(BF16)


def swiglu_bwd(a, b, dh):
    sig = sigmoid(a)
    silu = a * sig
    h = (silu * b).astype(BF16)
    da = (dh * b * (sig * (1.0 + a * (1.0 - sig)))).astype(BF16)
    db = (dh * silu).astype(BF16)
    return h, da, db


def rounded(v):
    return v.astype(BF16).astype(F32)


def half_rows(cap, ep_size):
    half = cap * ep_size
    return half, half + (-half) % 8


def store_parts(parity, part, send_ref, own_ref, half, padded):
    shift = padded - half

    @pl.when(parity == 0)
    def _():
        send_ref[0:half, :] = part[0:half]
        own_ref[0:half, :] = part[padded:padded + half]

    @pl.when(parity == 1)
    def _():
        send_ref[half:2 * half, :] = part[shift:padded]
        own_ref[half:2 * half, :] = part[padded + shift:2 * padded]


def pick_matrix(row_ref, rows):
    ids = row_ref[0]
    iota = lax.broadcasted_iota(jnp.int32, (rows, ids.shape[1]), 0)
    return iota == ids


def pick_rows(pick_ref, table_ref, out_ref, scale=None, step=512):
    @pl.loop(0, table_ref.shape[1] // step)
    def _(i):
        cols = pl.ds(pl.multiple_of(i * step, step), step)
        rows = dot(pick_ref[...], table_ref[:, cols])
        out_ref[:, cols] = (rows if scale is None else rows * scale).astype(out_ref.dtype)


def fwd_kernel(half, padded, x_ref, row_ref, w1_ref, w3_ref, w2_ref, send_ref, own_ref, pick_ref, rows_ref):
    pick_ref[...] = jnp.where(pick_matrix(row_ref, 2 * padded), 1.0, 0.0).astype(BF16)
    pick_rows(pick_ref, x_ref, rows_ref)
    rows = rows_ref[...]
    a = rounded(dot(rows, w1_ref[0]))
    b = rounded(dot(rows, w3_ref[0]))
    h = swiglu_fwd(a, b)
    part = dot(h, w2_ref[0])
    store_parts(pl.program_id(0) % 2, part, send_ref, own_ref, half, padded)


def windows(cap, ep_size):
    other, own = (ep_size - 1) * cap, cap
    return other, other + 7 + (-other - 7) % 8, own, own + 7 + (-own - 7) % 8


def bwd_kernel(sizes, per_chunk, x_ref, dy_ref, row_ref, gate_ref, w1_ref, w3_ref, w2_ref, *refs):
    other, win_other, own, win_own = sizes
    dw1_ref, dw3_ref, dw2_ref = refs[:3]
    outs, (far_ref, near_ref, sem, pick_ref, rows_ref, d_out_ref) = refs[3:-6], refs[-6:]
    chunks = far_ref.shape[0] // 2
    e = pl.program_id(0)
    total = 2 * (win_other + win_own)

    @pl.when(e == 0)
    def _():
        far_ref[...] = jnp.zeros_like(far_ref)
        near_ref[...] = jnp.zeros_like(near_ref)

    hit = pick_matrix(row_ref, total)
    pick_ref[...] = jnp.where(hit, 1.0, 0.0).astype(BF16)
    gates = jnp.sum(jnp.where(hit, gate_ref[0], 0.0), axis=1, keepdims=True)
    pick_rows(pick_ref, x_ref, rows_ref)
    pick_rows(pick_ref, dy_ref, d_out_ref, gates)
    rows, d_out = rows_ref[...], d_out_ref[...]
    a = rounded(dot(rows, w1_ref[0]))
    b = rounded(dot(rows, w3_ref[0]))
    dh = rounded(dot(d_out, w2_ref[0], NT))
    h, da, db = swiglu_bwd(a, b, dh)

    chunk = e // per_chunk
    far_base = pl.multiple_of((e % per_chunk) * other // 8 * 8, 8)
    near_base = pl.multiple_of(e * own // 8 * 8, 8)
    step = 512

    @pl.loop(0, rows_ref.shape[1] // step)
    def _(i):
        cols = pl.ds(pl.multiple_of(i * step, step), step)
        dw2_ref[0, :, cols] = dot(h, d_out_ref[:, cols], TN)
        dw1_ref[0, cols, :] = dot(rows_ref[:, cols], da, TN)
        dw3_ref[0, cols, :] = dot(rows_ref[:, cols], db, TN)
        part = dot(da, w1_ref[0, cols, :], NT) + dot(db, w3_ref[0, cols, :], NT)
        for side in range(2):
            far_ref[chunk * 2 + side, pl.ds(far_base, win_other), cols] += part[side * win_other:(side + 1) * win_other]
            first = 2 * win_other + side * win_own
            near_ref[side, pl.ds(near_base, win_own), cols] += part[first:first + win_own]

    def copies(c):
        out = []
        for side in range(2):
            k = 2 * c + side
            src = far_ref.at[k] if c < chunks else near_ref.at[side]
            out.append(pltpu.make_async_copy(src.at[pl.ds(0, outs[k].shape[0])], outs[k], sem.at[k]))
        return out

    for c in range(chunks):
        @pl.when(e == (c + 1) * per_chunk - 1)
        def _():
            for copy in copies(c):
                copy.start()

    @pl.when(e == chunks * per_chunk - 1)
    def _():
        for copy in copies(chunks):
            copy.start()
        for c in range(chunks + 1):
            for copy in copies(c):
                copy.wait()


def expert_fwd(start, count, half, padded, x_all, row_ids, w_gate, w_up, w_down):
    tokens, model = x_all.shape
    width = w_gate.shape[2]
    out = jax.ShapeDtypeStruct((count * half, model), F32)
    return pl.pallas_call(
        functools.partial(fwd_kernel, half, padded),
        grid=(count,),
        in_specs=[
            pl.BlockSpec((tokens, model), lambda i: (0, 0), pipeline_mode=pl.Buffered(1)),
            pl.BlockSpec((1, 1, tokens), lambda i: (start + i, 0, 0)),
            pl.BlockSpec((1, model, width), lambda i: (start + i, 0, 0)),
            pl.BlockSpec((1, model, width), lambda i: (start + i, 0, 0)),
            pl.BlockSpec((1, width, model), lambda i: (start + i, 0, 0)),
        ],
        out_specs=[pl.BlockSpec((2 * half, model), lambda i: (i // 2, 0))] * 2,
        out_shape=[out, out],
        scratch_shapes=[pltpu.VMEM((2 * padded, tokens), BF16), pltpu.VMEM((2 * padded, model), BF16)],
        cost_estimate=pl.CostEstimate(
            flops=count * 2 * 2 * padded * model * (tokens + 3 * width),
            bytes_accessed=count * (6 * model * width + 8 * half * model) + 2 * tokens * model,
            transcendentals=count * 2 * padded * width),
        compiler_params=pltpu.CompilerParams(dimension_semantics=('arbitrary',), vmem_limit_bytes=48 << 20),
    )(x_all, row_ids, w_gate, w_up, w_down)


def expert_bwd(chunks, sizes, x_all, dy_all, row_ids, gates, w_gate, w_up, w_down):
    other, win_other, own, win_own = sizes
    tokens, model = x_all.shape
    count, _, width = w_gate.shape
    per_chunk = count // chunks
    far_rows, near_rows = per_chunk * other, count * own
    far_pad = max(j * other // 8 * 8 + win_other for j in range(per_chunk))
    near_pad = max(j * own // 8 * 8 + win_own for j in range(count))
    part_shapes = [jax.ShapeDtypeStruct((far_rows, model), F32)] * (2 * chunks) + [jax.ShapeDtypeStruct((near_rows, model), F32)] * 2
    rows = 2 * (win_other + win_own)
    outs = pl.pallas_call(
        functools.partial(bwd_kernel, sizes, per_chunk),
        grid=(count,),
        in_specs=[
            pl.BlockSpec((tokens, model), lambda i: (0, 0), pipeline_mode=pl.Buffered(1)),
            pl.BlockSpec((tokens, model), lambda i: (0, 0), pipeline_mode=pl.Buffered(1)),
            pl.BlockSpec((1, 1, tokens), lambda i: (i, 0, 0)),
            pl.BlockSpec((1, 1, tokens), lambda i: (i, 0, 0)),
            pl.BlockSpec((1, model, width), lambda i: (i, 0, 0)),
            pl.BlockSpec((1, model, width), lambda i: (i, 0, 0)),
            pl.BlockSpec((1, width, model), lambda i: (i, 0, 0)),
        ],
        out_specs=[
            pl.BlockSpec((1, model, width), lambda i: (i, 0, 0)),
            pl.BlockSpec((1, model, width), lambda i: (i, 0, 0)),
            pl.BlockSpec((1, width, model), lambda i: (i, 0, 0)),
        ] + [pl.BlockSpec(memory_space=pl.ANY)] * len(part_shapes),
        out_shape=[
            jax.ShapeDtypeStruct((count, model, width), F32),
            jax.ShapeDtypeStruct((count, model, width), F32),
            jax.ShapeDtypeStruct((count, width, model), F32),
        ] + part_shapes,
        scratch_shapes=[
            pltpu.VMEM((2 * chunks, far_pad, model), F32),
            pltpu.VMEM((2, near_pad, model), F32),
            pltpu.SemaphoreType.DMA((len(part_shapes),)),
            pltpu.VMEM((rows, tokens), BF16),
            pltpu.VMEM((rows, model), BF16),
            pltpu.VMEM((rows, model), BF16),
        ],
        cost_estimate=pl.CostEstimate(
            flops=count * 2 * rows * model * (2 * tokens + 8 * width),
            bytes_accessed=count * (18 * model * width + 4 * rows * model) + 4 * tokens * model,
            transcendentals=count * rows * width),
        compiler_params=pltpu.CompilerParams(dimension_semantics=('arbitrary',), vmem_limit_bytes=60 << 20),
        name='expert_bwd',
    )(x_all, dy_all, row_ids, gates, w_gate, w_up, w_down)
    parts = outs[3:]
    return outs[:3], [(parts[2 * c], parts[2 * c + 1]) for c in range(chunks + 1)]


def shared_grad_kernel(step, x_ref, dy_ref, wg_ref, wu_ref, wd_ref, dg_ref, du_ref, dd_ref, h_ref, da_ref, db_ref):
    tokens, model = x_ref.shape

    @pl.loop(0, tokens // step)
    def _(i):
        rows = pl.ds(pl.multiple_of(i * step, step), step)
        a = rounded(dot(x_ref[rows, :], wg_ref[...]))
        b = rounded(dot(x_ref[rows, :], wu_ref[...]))
        dh = rounded(dot(dy_ref[rows, :], wd_ref[...], NT))
        h_ref[rows, :], da_ref[rows, :], db_ref[rows, :] = swiglu_bwd(a, b, dh)

    @pl.loop(0, model // step)
    def _(i):
        cols = pl.ds(pl.multiple_of(i * step, step), step)
        dd_ref[:, cols] = dot(h_ref[...], dy_ref[:, cols], TN)
        dg_ref[cols, :] = dot(x_ref[:, cols], da_ref[...], TN)
        du_ref[cols, :] = dot(x_ref[:, cols], db_ref[...], TN)


def shared_grad(x_all, dy_all, ws_gate, ws_up, ws_down):
    tokens, model = x_all.shape
    width = ws_gate.shape[1]
    block = min(width, 256)
    full = pl.BlockSpec((tokens, model), lambda i: (0, 0), pipeline_mode=pl.Buffered(1))
    col = pl.BlockSpec((model, block), lambda i: (0, i))
    row = pl.BlockSpec((block, model), lambda i: (i, 0))
    return pl.pallas_call(
        functools.partial(shared_grad_kernel, 256),
        grid=(width // block,),
        in_specs=[full, full, col, col, row],
        out_specs=[col, col, row],
        out_shape=[jax.ShapeDtypeStruct((model, width), F32)] * 2 + [jax.ShapeDtypeStruct((width, model), F32)],
        scratch_shapes=[pltpu.VMEM((tokens, block), BF16)] * 3,
        cost_estimate=pl.CostEstimate(
            flops=12 * tokens * model * width, bytes_accessed=4 * tokens * model + 18 * model * width,
            transcendentals=tokens * width),
        compiler_params=pltpu.CompilerParams(dimension_semantics=('arbitrary',), vmem_limit_bytes=48 << 20),
        name='shared_grad',
    )(x_all, dy_all, ws_gate, ws_up, ws_down)


def split3(v):
    hi = lax.reduce_precision(v, 8, 7)
    rest = v - hi
    mid = lax.reduce_precision(rest, 8, 7)
    low = rest - mid
    return hi.astype(BF16), mid.astype(BF16), low.astype(BF16)


def sum3(v, axis):
    first, second, third = jnp.split(v, 3, axis=axis)
    return first + second + third


def core_partner(ep):
    return ep + 1 - 2 * (ep % 2)


def gather_kernel(x_ref, idx_ref, dy_ref, wg_ref, wu_ref, wd_ref, x_all, idx_all, dy_pair, wd_part, quarter, send_sem, recv_sem, idx_send, idx_recv, local_sem):
    tp = lax.axis_index('tp')
    ep = lax.axis_index('ep')
    eps = x_all.shape[0] // 2
    half = eps // 2
    tp_o = 1 - tp
    ep_x = (ep + half) % eps
    ep_c = core_partner(ep)

    def slot(e, t):
        return e * 2 + t

    others = [(tp_o, ep)]
    for k in range(1, eps):
        others += [(tp, (ep + k) % eps), (tp_o, (ep + k) % eps)]
    barrier = pltpu.get_barrier_semaphore()
    for t, e in others:
        pl.semaphore_signal(barrier, inc=1, device_id={'tp': t, 'ep': e}, device_id_type=MESH)
    pl.semaphore_wait(barrier, len(others))

    def send(k, src, dst, t, e):
        copy = pltpu.make_async_remote_copy(
            src_ref=src, dst_ref=dst, send_sem=send_sem.at[k], recv_sem=recv_sem.at[k],
            device_id={'tp': t, 'ep': e}, device_id_type=MESH)
        copy.start()
        return copy

    def block(e, t):
        return x_all.at[slot(e, t)]

    mine = block(ep, tp)
    to_y = send(0, x_ref, mine, tp_o, ep)
    to_x = send(1, x_ref, mine, tp, ep_x)
    to_c = send(2, x_ref, mine, tp, ep_c)
    own_idx = idx_all.at[slot(ep, tp)]
    idx_copies = []
    for k, (t, e) in enumerate(others):
        copy = pltpu.make_async_remote_copy(
            src_ref=idx_ref, dst_ref=own_idx, send_sem=idx_send.at[k], recv_sem=idx_recv.at[k],
            device_id={'tp': t, 'ep': e}, device_id_type=MESH)
        copy.start()
        idx_copies.append(copy)
    local = [
        pltpu.make_async_copy(x_ref, mine, local_sem.at[0]),
        pltpu.make_async_copy(idx_ref, own_idx, local_sem.at[1]),
        pltpu.make_async_copy(dy_ref, dy_pair.at[tp], local_sem.at[2]),
    ]
    width = quarter.shape[1] // 2
    cols = pl.ds(pl.multiple_of(ep * width, width), width)
    for k, ref in enumerate((wg_ref, wu_ref)):
        local.append(pltpu.make_async_copy(ref.at[:, cols], quarter.at[:, pl.ds(k * width, width)], local_sem.at[3 + k]))
    for copy in local:
        copy.start()
    dy_y = send(3, dy_ref, dy_pair.at[tp], tp_o, ep)
    rows = wd_part.shape[0]
    wd_y = send(4, wd_ref.at[pl.ds(ep * rows, rows)], wd_part, tp_o, ep)

    to_y.wait_recv()
    y_to_x = send(5, block(ep, tp_o), block(ep, tp_o), tp, ep_x)
    y_to_c = send(6, block(ep, tp_o), block(ep, tp_o), tp, ep_c)
    to_x.wait_recv()
    x_to_c = send(7, block(ep_x, tp), block(ep_x, tp), tp, ep_c)
    y_to_x.wait_recv()
    xy_to_c = send(8, block(ep_x, tp_o), block(ep_x, tp_o), tp, ep_c)
    for copy in (to_c, dy_y, wd_y, y_to_c, x_to_c, xy_to_c):
        copy.wait_recv()
    for copy in idx_copies:
        copy.wait_recv()
    for copy in local:
        copy.wait()
    for copy in (to_y, to_x, to_c, dy_y, wd_y, y_to_x, y_to_c, x_to_c, xy_to_c):
        copy.wait_send()
    for copy in idx_copies:
        copy.wait_send()


def gather_rows(devices, ep_size, x, idx_t, dy, ws_gate, ws_up, ws_down):
    _, model = x.shape
    any_spec = pl.BlockSpec(memory_space=pl.ANY)
    return pl.pallas_call(
        gather_kernel,
        in_specs=[any_spec] * 6,
        out_specs=[any_spec] * 5,
        out_shape=[
            jax.ShapeDtypeStruct((devices,) + x.shape, x.dtype),
            jax.ShapeDtypeStruct((devices,) + idx_t.shape, idx_t.dtype),
            jax.ShapeDtypeStruct((2,) + dy.shape, dy.dtype),
            jax.ShapeDtypeStruct((ws_down.shape[0] // ep_size, model), ws_down.dtype),
            jax.ShapeDtypeStruct((model, 2 * ws_gate.shape[1] // ep_size), ws_gate.dtype),
        ],
        scratch_shapes=[
            pltpu.SemaphoreType.DMA((9,)),
            pltpu.SemaphoreType.DMA((9,)),
            pltpu.SemaphoreType.DMA((devices - 1,)),
            pltpu.SemaphoreType.DMA((devices - 1,)),
            pltpu.SemaphoreType.DMA((5,)),
        ],
        cost_estimate=pl.CostEstimate(flops=60_000_000_000, bytes_accessed=4 * devices * x.size, transcendentals=0),
        compiler_params=pltpu.CompilerParams(collective_id=0, has_side_effects=True),
        name='gather_rows',
    )(x, idx_t, dy, ws_gate, ws_up, ws_down)


def solution(mesh):
    tp_size = mesh.shape['tp']
    ep_size = mesh.shape['ep']
    swap_tp = [(i, tp_size - 1 - i) for i in range(tp_size)]
    swap_x = [(i, (i + ep_size // 2) % ep_size) for i in range(ep_size)]
    swap_c = [(i, core_partner(i)) for i in range(ep_size)]

    def device_step(x, grad_y, w_router, w_gate, w_up, w_down, ws_gate, ws_up, ws_down, topk_idx):
        tok, model = x.shape
        top_k = topk_idx.shape[1]
        experts = w_router.shape[1]
        local_exp = w_gate.shape[0]
        groups = top_k // 2
        most = groups * tok // (2 * ep_size) + min(groups, ep_size // 2) * tok // ep_size
        cap = (2 * most + local_exp - 1) // local_exp
        half, padded = half_rows(cap, ep_size)
        shift = padded - half
        ep_i = lax.axis_index('ep')
        tp_i = lax.axis_index('tp')
        devices = ep_size * tp_size
        ep_order = (ep_i, (ep_i + ep_size // 2) % ep_size, core_partner(ep_i), core_partner((ep_i + ep_size // 2) % ep_size))

        def ep_pieces(piece):
            far = lax.ppermute(piece, 'ep', swap_x)
            return piece, far, lax.ppermute(piece, 'ep', swap_c), lax.ppermute(far, 'ep', swap_c)

        def ep_gather(piece):
            out = jnp.zeros((ep_size,) + piece.shape, piece.dtype)
            for e, part in zip(ep_order, ep_pieces(piece)):
                out = lax.dynamic_update_slice_in_dim(out, part[None], e, 0)
            return out

        x_blocks, idx_all, dy_pair, wd_part, quarter = gather_rows(devices, ep_size, x, topk_idx.T, grad_y, ws_gate, ws_up, ws_down)
        x_all = x_blocks.reshape(devices * tok, model)

        width_q = ws_gate.shape[1] // ep_size
        gu_part = lax.ppermute(quarter, 'tp', swap_tp)

        lower = (lax.broadcasted_iota(jnp.int32, (tok, tok), 0) > lax.broadcasted_iota(jnp.int32, (tok, tok), 1)).astype(BF16)
        local_ids = ep_i * local_exp + jnp.arange(local_exp, dtype=jnp.int32)
        hit = jnp.any(idx_all[None] == local_ids[:, None, None, None], axis=2)
        rank = jnp.einsum('edj,ij->edi', hit.astype(BF16), lower, preferred_element_type=F32).astype(jnp.int32)
        dev = jnp.arange(devices, dtype=jnp.int32)
        is_own = (dev % tp_size) == tp_i
        parity = jnp.arange(local_exp, dtype=jnp.int32) % 2
        base = (jnp.where(is_own, padded, 0) + (dev // tp_size) * cap)[None, :] + (parity * shift)[:, None]
        row_ids = jnp.where(hit, base[:, :, None] + rank, -1).reshape(local_exp, 1, devices * tok)

        fwd_parts = []
        start = 0
        rows_now = row_ids
        for count in FWD_CHUNKS:
            send, own = expert_fwd(start, count, half, padded, x_all, rows_now, w_gate, w_up, w_down)
            start += count
            rows_now, own = lax.optimization_barrier((rows_now, own))
            fwd_parts.append((lax.ppermute(send, 'tp', swap_tp), own))

        own0 = fwd_parts[-1][1]
        x_late, hit, rank, w_router, own0 = lax.optimization_barrier((x_all, hit, rank, w_router, own0))
        fwd_parts[-1] = (fwd_parts[-1][0], own0)

        logits_t = jnp.einsum('de,td->et', w_router, x_late, preferred_element_type=F32)
        probs_t = jax.nn.softmax(logits_t, axis=0)
        gates_local = GATE_SCALE * lax.dynamic_slice_in_dim(probs_t, ep_i * local_exp, local_exp, 0).reshape(local_exp, 1, devices * tok)

        sizes = windows(cap, ep_size)
        other, win_other, near, win_near = sizes
        per_chunk = local_exp // BWD_CHUNKS
        dev_ep = dev // tp_size
        place = jnp.zeros_like(dev)
        for k, e in enumerate(ep_order[1:]):
            place = jnp.where(dev_ep == e, k * cap, place)
        exp = jnp.arange(local_exp, dtype=jnp.int32)
        far_first = (jnp.where(is_own, win_other, 0) + place)[None, :] + ((exp % per_chunk) * other % 8)[:, None]
        near_first = jnp.where(is_own, win_near, 0)[None, :] + (2 * win_other + exp * near % 8)[:, None]
        first = jnp.where((dev_ep == ep_i)[None, :], near_first, far_first)
        bwd_ids = jnp.where(hit, first[:, :, None] + rank, -1).reshape(local_exp, 1, devices * tok)
        dy_all = ep_gather(dy_pair).reshape(devices * tok, model)
        (d_w_gate, d_w_up, d_w_down), bwd_out = expert_bwd(BWD_CHUNKS, sizes, x_all, dy_all, bwd_ids, gates_local, w_gate, w_up, w_down)
        bwd_parts = [(lax.ppermute(bwd_out[0][0], 'tp', swap_tp), bwd_out[0][1])]

        own_last = bwd_out[-1][1]
        x, grad_y, x_all, dy_all, topk_idx, w_router, own_last = lax.optimization_barrier(
            (x, grad_y, x_all, dy_all, topk_idx, w_router, own_last))
        bwd_out[-1] = (bwd_out[-1][0], own_last)

        gu_other = ep_pieces(gu_part)
        wd_other = jnp.concatenate(ep_pieces(wd_part), axis=0)
        wg_other = jnp.concatenate([p[:, :width_q] for p in gu_other], axis=1)
        wu_other = jnp.concatenate([p[:, width_q:] for p in gu_other], axis=1)
        shared = jnp.zeros((tok, model), F32)
        dx_shared = jnp.zeros((tok, model), F32)
        for wg, wu, wd in ((ws_gate, ws_up, ws_down), (wg_other, wu_other, wd_other)):
            a = rounded(dot(x, wg))
            b = rounded(dot(x, wu))
            dh = rounded(dot(grad_y, wd, NT))
            h, da, db = swiglu_bwd(a, b, dh)
            shared = shared + dot(h, wd)
            dx_shared = dx_shared + dot(da, wg, NT) + dot(db, wu, NT)
        ds_gate, ds_up, ds_down = shared_grad(x_all, dy_all, ws_gate, ws_up, ws_down)

        def back_rows(count):
            return count * cap + (-count * cap) % 8

        def slot_index(count):
            new = jnp.arange(ep_size * back_rows(count), dtype=jnp.int32)
            block, rest = new // back_rows(count), new % back_rows(count)
            return block, rest // cap, rest % cap, rest < count * cap

        def give_back(parts, count):
            recv, own = parts
            rows = (recv + own).astype(BF16)
            src, exp, rank, valid = slot_index(count)
            old = jnp.where(valid, exp * half + src * cap + rank, -1)
            perm = (old[:, None] == jnp.arange(count * half, dtype=jnp.int32)[None, :]).astype(BF16)
            out = dot(perm, rows).astype(BF16)
            out = out.reshape(ep_size, back_rows(count), model)
            return lax.all_to_all(out, 'ep', 0, 0).reshape(ep_size * back_rows(count), model)

        hit_own = jnp.any(topk_idx[:, None, :] == jnp.arange(experts, dtype=jnp.int32)[None, :, None], axis=2)
        rank_own = dot(lower, hit_own.astype(BF16))
        want = jnp.where(hit_own, rank_own, -1.0).astype(BF16)
        probs = jax.nn.softmax(dot(x, w_router), axis=-1)
        prob_parts = jnp.concatenate(split3(probs), axis=0)

        def expand(start, count):
            grp, exp, rank, valid = slot_index(count)
            col = jnp.where(valid, grp * local_exp + start + exp, -1)
            table = (jnp.arange(experts, dtype=jnp.int32)[:, None] == col[None, :]).astype(BF16)
            return table, jnp.where(valid, rank, -2).astype(F32)[None, :]

        routed = jnp.zeros((tok, model), F32)
        d_scores = jnp.zeros((tok, experts), F32)
        start = 0
        for parts, count in zip(fwd_parts, FWD_CHUNKS):
            back = give_back(parts, count)
            table, rank = expand(start, count)
            hits = dot(want, table) == rank
            gates = jnp.where(jnp.concatenate([hits] * 3, axis=0), dot(prob_parts, table), 0.0).astype(BF16)
            routed = routed + GATE_SCALE * sum3(dot(gates, back), 0)
            score = jnp.where(hits, dot(grad_y, back, NT), 0.0)
            part = dot(jnp.concatenate(split3(score), axis=0), table, NT)
            d_scores = d_scores + sum3(part, 0)
            start += count
        y_out = (shared + routed).astype(BF16)

        d_scores = GATE_SCALE * d_scores
        mean_score = jnp.sum(probs * d_scores, axis=-1, keepdims=True)
        d_logits = probs * (d_scores - mean_score)
        d_other = lax.ppermute(d_logits, 'tp', swap_tp)
        for send, own in bwd_out[1:]:
            bwd_parts.append((lax.ppermute(send, 'tp', swap_tp), own))
        d_pair = jnp.where(tp_i == 0, jnp.stack([d_logits, d_other]), jnp.stack([d_other, d_logits]))
        d_logits_all = ep_gather(d_pair).reshape(devices * tok, experts)
        d_router = sum3(dot(x_all, jnp.concatenate(split3(d_logits_all), axis=1), TN), 1)
        dx_sum = dx_shared + sum3(dot(jnp.concatenate(split3(d_logits), axis=0), w_router, NT), 0)

        def hits_of(grp, start, count):
            slot = jnp.arange(count * cap, dtype=jnp.int32)
            col = grp * local_exp + start + slot // cap
            table = (jnp.arange(experts, dtype=jnp.int32)[:, None] == col[None, :]).astype(BF16)
            return (dot(want, table) == (slot % cap).astype(F32)[None, :]).astype(BF16)

        swaps = (swap_x, swap_c, [(i, core_partner(d)) for i, d in swap_x])
        for c, (recv, own) in enumerate(bwd_parts[:-1]):
            rows = (recv + own).astype(BF16)
            slot = jnp.arange(per_chunk * cap, dtype=jnp.int32)
            for k, pairs in enumerate(swaps):
                old = slot // cap * other + k * cap + slot % cap
                perm = (old[:, None] == jnp.arange(per_chunk * other, dtype=jnp.int32)[None, :]).astype(BF16)
                back = dot(perm, rows).astype(BF16)
                back = lax.ppermute(back, 'ep', pairs)
                hits = hits_of(ep_order[1 + k], c * per_chunk, per_chunk)
                dx_sum = dx_sum + dot(hits, back)
        recv, own = bwd_parts[-1]
        dx_sum = lax.optimization_barrier(dx_sum)
        dx_sum = dx_sum + dot(hits_of(ep_i, 0, local_exp), (recv + own).astype(BF16))
        return y_out, dx_sum.astype(BF16), d_router, d_w_gate, d_w_up, d_w_down, ds_gate, ds_up, ds_down

    tok_spec = P(('ep', 'tp'), None)
    in_specs = (tok_spec, tok_spec, P(None, None), P('ep', None, 'tp'), P('ep', None, 'tp'), P('ep', 'tp', None), P(None, 'tp'), P(None, 'tp'), P('tp', None), tok_spec)
    out_specs = (tok_spec, tok_spec, P(None, None), P('ep', None, 'tp'), P('ep', None, 'tp'), P('ep', 'tp', None), P(None, 'tp'), P(None, 'tp'), P('tp', None))

    return jax.shard_map(device_step, mesh=mesh, in_specs=in_specs, out_specs=out_specs, check_vma=False)
```

```python
import functools

import jax
import jax.numpy as jnp
from jax import lax
from jax.experimental import pallas as pl
from jax.experimental.pallas import tpu as pltpu
from jax.sharding import PartitionSpec as P


GATE_SCALE = 16.0
BF16 = jnp.bfloat16
F32 = jnp.float32
FWD_CHUNKS = (2, 8, 6)
BWD_CHUNKS = 2
MESH = pl.DeviceIdType.MESH

NN = (((1,), (0,)), ((), ()))
NT = (((1,), (1,)), ((), ()))
TN = (((0,), (0,)), ((), ()))


def dot(a, b, dims=NN):
    return lax.dot_general(a, b, dims, preferred_element_type=F32)


def sigmoid(v):
    return 1.0 / (1.0 + jnp.exp(-jnp.maximum(v, -88.0)))


def swiglu_fwd(a, b):
    return (a * sigmoid(a) * b).astype(BF16)


def swiglu_bwd(a, b, dh):
    sig = sigmoid(a)
    silu = a * sig
    h = (silu * b).astype(BF16)
    da = (dh * b * (sig * (1.0 + a * (1.0 - sig)))).astype(BF16)
    db = (dh * silu).astype(BF16)
    return h, da, db


def rounded(v):
    return v.astype(BF16).astype(F32)


def half_rows(cap, ep_size):
    half = cap * ep_size
    return half, half + (-half) % 8


def store_parts(parity, part, send_ref, own_ref, half, padded):
    shift = padded - half

    @pl.when(parity == 0)
    def _():
        send_ref[0:half, :] = part[0:half]
        own_ref[0:half, :] = part[padded:padded + half]

    @pl.when(parity == 1)
    def _():
        send_ref[half:2 * half, :] = part[shift:padded]
        own_ref[half:2 * half, :] = part[padded + shift:2 * padded]


def pick_matrix(row_ref, rows):
    ids = row_ref[0]
    iota = lax.broadcasted_iota(jnp.int32, (rows, ids.shape[1]), 0)
    return iota == ids


def pick_rows(pick_ref, table_ref, out_ref, scale=None, step=512):
    @pl.loop(0, table_ref.shape[1] // step)
    def _(i):
        cols = pl.ds(pl.multiple_of(i * step, step), step)
        rows = dot(pick_ref[...], table_ref[:, cols])
        out_ref[:, cols] = (rows if scale is None else rows * scale).astype(out_ref.dtype)


def fwd_kernel(half, padded, x_ref, row_ref, w1_ref, w3_ref, w2_ref, send_ref, own_ref, pick_ref, rows_ref):
    pick_ref[...] = jnp.where(pick_matrix(row_ref, 2 * padded), 1.0, 0.0).astype(BF16)
    pick_rows(pick_ref, x_ref, rows_ref)
    rows = rows_ref[...]
    a = rounded(dot(rows, w1_ref[0]))
    b = rounded(dot(rows, w3_ref[0]))
    h = swiglu_fwd(a, b)
    part = dot(h, w2_ref[0])
    store_parts(pl.program_id(0) % 2, part, send_ref, own_ref, half, padded)


def windows(cap, ep_size):
    other, own = (ep_size - 1) * cap, cap
    return other, other + 7 + (-other - 7) % 8, own, own + 7 + (-own - 7) % 8


def bwd_kernel(sizes, per_chunk, x_ref, dy_ref, row_ref, gate_ref, w1_ref, w3_ref, w2_ref, *refs):
    other, win_other, own, win_own = sizes
    dw1_ref, dw3_ref, dw2_ref = refs[:3]
    outs, (far_ref, near_ref, sem, pick_ref, rows_ref, d_out_ref) = refs[3:-6], refs[-6:]
    chunks = far_ref.shape[0] // 2
    e = pl.program_id(0)
    total = 2 * (win_other + win_own)

    @pl.when(e == 0)
    def _():
        far_ref[...] = jnp.zeros_like(far_ref)
        near_ref[...] = jnp.zeros_like(near_ref)

    hit = pick_matrix(row_ref, total)
    pick_ref[...] = jnp.where(hit, 1.0, 0.0).astype(BF16)
    gates = jnp.sum(jnp.where(hit, gate_ref[0], 0.0), axis=1, keepdims=True)
    pick_rows(pick_ref, x_ref, rows_ref)
    pick_rows(pick_ref, dy_ref, d_out_ref, gates)
    rows, d_out = rows_ref[...], d_out_ref[...]
    a = rounded(dot(rows, w1_ref[0]))
    b = rounded(dot(rows, w3_ref[0]))
    dh = rounded(dot(d_out, w2_ref[0], NT))
    h, da, db = swiglu_bwd(a, b, dh)

    chunk = e // per_chunk
    far_base = pl.multiple_of((e % per_chunk) * other // 8 * 8, 8)
    near_base = pl.multiple_of(e * own // 8 * 8, 8)
    step = 512

    @pl.loop(0, rows_ref.shape[1] // step)
    def _(i):
        cols = pl.ds(pl.multiple_of(i * step, step), step)
        dw2_ref[0, :, cols] = dot(h, d_out_ref[:, cols], TN)
        dw1_ref[0, cols, :] = dot(rows_ref[:, cols], da, TN)
        dw3_ref[0, cols, :] = dot(rows_ref[:, cols], db, TN)
        part = dot(da, w1_ref[0, cols, :], NT) + dot(db, w3_ref[0, cols, :], NT)
        for side in range(2):
            far_ref[chunk * 2 + side, pl.ds(far_base, win_other), cols] += part[side * win_other:(side + 1) * win_other]
            first = 2 * win_other + side * win_own
            near_ref[side, pl.ds(near_base, win_own), cols] += part[first:first + win_own]

    def copies(c):
        out = []
        for side in range(2):
            k = 2 * c + side
            src = far_ref.at[k] if c < chunks else near_ref.at[side]
            out.append(pltpu.make_async_copy(src.at[pl.ds(0, outs[k].shape[0])], outs[k], sem.at[k]))
        return out

    for c in range(chunks):
        @pl.when(e == (c + 1) * per_chunk - 1)
        def _():
            for copy in copies(c):
                copy.start()

    @pl.when(e == chunks * per_chunk - 1)
    def _():
        for copy in copies(chunks):
            copy.start()
        for c in range(chunks + 1):
            for copy in copies(c):
                copy.wait()


def expert_fwd(start, count, half, padded, x_all, row_ids, w_gate, w_up, w_down):
    tokens, model = x_all.shape
    width = w_gate.shape[2]
    out = jax.ShapeDtypeStruct((count * half, model), F32)
    return pl.pallas_call(
        functools.partial(fwd_kernel, half, padded),
        grid=(count,),
        in_specs=[
            pl.BlockSpec((tokens, model), lambda i: (0, 0), pipeline_mode=pl.Buffered(1)),
            pl.BlockSpec((1, 1, tokens), lambda i: (start + i, 0, 0)),
            pl.BlockSpec((1, model, width), lambda i: (start + i, 0, 0)),
            pl.BlockSpec((1, model, width), lambda i: (start + i, 0, 0)),
            pl.BlockSpec((1, width, model), lambda i: (start + i, 0, 0)),
        ],
        out_specs=[pl.BlockSpec((2 * half, model), lambda i: (i // 2, 0))] * 2,
        out_shape=[out, out],
        scratch_shapes=[pltpu.VMEM((2 * padded, tokens), BF16), pltpu.VMEM((2 * padded, model), BF16)],
        cost_estimate=pl.CostEstimate(
            flops=count * 2 * 2 * padded * model * (tokens + 3 * width),
            bytes_accessed=count * (6 * model * width + 8 * half * model) + 2 * tokens * model,
            transcendentals=count * 2 * padded * width),
        compiler_params=pltpu.CompilerParams(dimension_semantics=('arbitrary',), vmem_limit_bytes=48 << 20),
    )(x_all, row_ids, w_gate, w_up, w_down)


def expert_bwd(chunks, sizes, x_all, dy_all, row_ids, gates, w_gate, w_up, w_down):
    other, win_other, own, win_own = sizes
    tokens, model = x_all.shape
    count, _, width = w_gate.shape
    per_chunk = count // chunks
    far_rows, near_rows = per_chunk * other, count * own
    far_pad = max(j * other // 8 * 8 + win_other for j in range(per_chunk))
    near_pad = max(j * own // 8 * 8 + win_own for j in range(count))
    part_shapes = [jax.ShapeDtypeStruct((far_rows, model), F32)] * (2 * chunks) + [jax.ShapeDtypeStruct((near_rows, model), F32)] * 2
    rows = 2 * (win_other + win_own)
    outs = pl.pallas_call(
        functools.partial(bwd_kernel, sizes, per_chunk),
        grid=(count,),
        in_specs=[
            pl.BlockSpec((tokens, model), lambda i: (0, 0), pipeline_mode=pl.Buffered(1)),
            pl.BlockSpec((tokens, model), lambda i: (0, 0), pipeline_mode=pl.Buffered(1)),
            pl.BlockSpec((1, 1, tokens), lambda i: (i, 0, 0)),
            pl.BlockSpec((1, 1, tokens), lambda i: (i, 0, 0)),
            pl.BlockSpec((1, model, width), lambda i: (i, 0, 0)),
            pl.BlockSpec((1, model, width), lambda i: (i, 0, 0)),
            pl.BlockSpec((1, width, model), lambda i: (i, 0, 0)),
        ],
        out_specs=[
            pl.BlockSpec((1, model, width), lambda i: (i, 0, 0)),
            pl.BlockSpec((1, model, width), lambda i: (i, 0, 0)),
            pl.BlockSpec((1, width, model), lambda i: (i, 0, 0)),
        ] + [pl.BlockSpec(memory_space=pl.ANY)] * len(part_shapes),
        out_shape=[
            jax.ShapeDtypeStruct((count, model, width), F32),
            jax.ShapeDtypeStruct((count, model, width), F32),
            jax.ShapeDtypeStruct((count, width, model), F32),
        ] + part_shapes,
        scratch_shapes=[
            pltpu.VMEM((2 * chunks, far_pad, model), F32),
            pltpu.VMEM((2, near_pad, model), F32),
            pltpu.SemaphoreType.DMA((len(part_shapes),)),
            pltpu.VMEM((rows, tokens), BF16),
            pltpu.VMEM((rows, model), BF16),
            pltpu.VMEM((rows, model), BF16),
        ],
        cost_estimate=pl.CostEstimate(
            flops=count * 2 * rows * model * (2 * tokens + 8 * width),
            bytes_accessed=count * (18 * model * width + 4 * rows * model) + 4 * tokens * model,
            transcendentals=count * rows * width),
        compiler_params=pltpu.CompilerParams(dimension_semantics=('arbitrary',), vmem_limit_bytes=60 << 20),
        name='expert_bwd',
    )(x_all, dy_all, row_ids, gates, w_gate, w_up, w_down)
    parts = outs[3:]
    return outs[:3], [(parts[2 * c], parts[2 * c + 1]) for c in range(chunks + 1)]


def shared_grad_kernel(step, x_ref, dy_ref, wg_ref, wu_ref, wd_ref, dg_ref, du_ref, dd_ref, h_ref, da_ref, db_ref):
    tokens, model = x_ref.shape

    @pl.loop(0, tokens // step)
    def _(i):
        rows = pl.ds(pl.multiple_of(i * step, step), step)
        a = rounded(dot(x_ref[rows, :], wg_ref[...]))
        b = rounded(dot(x_ref[rows, :], wu_ref[...]))
        dh = rounded(dot(dy_ref[rows, :], wd_ref[...], NT))
        h_ref[rows, :], da_ref[rows, :], db_ref[rows, :] = swiglu_bwd(a, b, dh)

    @pl.loop(0, model // step)
    def _(i):
        cols = pl.ds(pl.multiple_of(i * step, step), step)
        dd_ref[:, cols] = dot(h_ref[...], dy_ref[:, cols], TN)
        dg_ref[cols, :] = dot(x_ref[:, cols], da_ref[...], TN)
        du_ref[cols, :] = dot(x_ref[:, cols], db_ref[...], TN)


def shared_grad(x_all, dy_all, ws_gate, ws_up, ws_down):
    tokens, model = x_all.shape
    width = ws_gate.shape[1]
    block = min(width, 256)
    full = pl.BlockSpec((tokens, model), lambda i: (0, 0), pipeline_mode=pl.Buffered(1))
    col = pl.BlockSpec((model, block), lambda i: (0, i))
    row = pl.BlockSpec((block, model), lambda i: (i, 0))
    return pl.pallas_call(
        functools.partial(shared_grad_kernel, 256),
        grid=(width // block,),
        in_specs=[full, full, col, col, row],
        out_specs=[col, col, row],
        out_shape=[jax.ShapeDtypeStruct((model, width), F32)] * 2 + [jax.ShapeDtypeStruct((width, model), F32)],
        scratch_shapes=[pltpu.VMEM((tokens, block), BF16)] * 3,
        cost_estimate=pl.CostEstimate(
            flops=12 * tokens * model * width, bytes_accessed=4 * tokens * model + 18 * model * width,
            transcendentals=tokens * width),
        compiler_params=pltpu.CompilerParams(dimension_semantics=('arbitrary',), vmem_limit_bytes=48 << 20),
        name='shared_grad',
    )(x_all, dy_all, ws_gate, ws_up, ws_down)


def split3(v):
    hi = lax.reduce_precision(v, 8, 7)
    rest = v - hi
    mid = lax.reduce_precision(rest, 8, 7)
    low = rest - mid
    return hi.astype(BF16), mid.astype(BF16), low.astype(BF16)


def sum3(v, axis):
    first, second, third = jnp.split(v, 3, axis=axis)
    return first + second + third


def core_partner(ep):
    return ep + 1 - 2 * (ep % 2)


def gather_kernel(x_ref, idx_ref, dy_ref, wg_ref, wu_ref, wd_ref, x_all, idx_all, dy_pair, wd_part, quarter, send_sem, recv_sem, idx_send, idx_recv, local_sem, x_buf, dy_buf, q_buf):
    tp = lax.axis_index('tp')
    ep = lax.axis_index('ep')
    eps = x_all.shape[0] // 2
    half = eps // 2
    tp_o = 1 - tp
    ep_x = (ep + half) % eps
    ep_c = core_partner(ep)

    def slot(e, t):
        return e * 2 + t

    others = [(tp_o, ep)]
    for k in range(1, eps):
        others += [(tp, (ep + k) % eps), (tp_o, (ep + k) % eps)]
    barrier = pltpu.get_barrier_semaphore()
    for t, e in others:
        pl.semaphore_signal(barrier, inc=1, device_id={'tp': t, 'ep': e}, device_id_type=MESH)
    pl.semaphore_wait(barrier, len(others))

    def send(k, src, dst, t, e):
        copy = pltpu.make_async_remote_copy(
            src_ref=src, dst_ref=dst, send_sem=send_sem.at[k], recv_sem=recv_sem.at[k],
            device_id={'tp': t, 'ep': e}, device_id_type=MESH)
        copy.start()
        return copy

    def block(e, t):
        return x_all.at[slot(e, t)]

    mine = block(ep, tp)
    to_y = send(0, x_ref, mine, tp_o, ep)
    to_x = send(1, x_ref, mine, tp, ep_x)
    to_c = send(2, x_ref, mine, tp, ep_c)
    own_idx = idx_all.at[slot(ep, tp)]
    idx_copies = []
    for k, (t, e) in enumerate(others):
        copy = pltpu.make_async_remote_copy(
            src_ref=idx_ref, dst_ref=own_idx, send_sem=idx_send.at[k], recv_sem=idx_recv.at[k],
            device_id={'tp': t, 'ep': e}, device_id_type=MESH)
        copy.start()
        idx_copies.append(copy)
    width = quarter.shape[1] // 2
    cols = pl.ds(pl.multiple_of(ep * width, width), width)
    load = [
        pltpu.make_async_copy(x_ref, x_buf, local_sem.at[0]),
        pltpu.make_async_copy(dy_ref, dy_buf, local_sem.at[1]),
        pltpu.make_async_copy(wg_ref.at[:, cols], q_buf.at[:, pl.ds(0, width)], local_sem.at[2]),
        pltpu.make_async_copy(wu_ref.at[:, cols], q_buf.at[:, pl.ds(width, width)], local_sem.at[3]),
    ]
    store = [
        pltpu.make_async_copy(x_buf, mine, local_sem.at[4]),
        pltpu.make_async_copy(dy_buf, dy_pair.at[tp], local_sem.at[5]),
        pltpu.make_async_copy(q_buf, quarter, local_sem.at[6]),
        pltpu.make_async_copy(idx_ref, own_idx, local_sem.at[7]),
    ]
    for copy in load:
        copy.start()
    dy_y = send(3, dy_ref, dy_pair.at[tp], tp_o, ep)
    rows = wd_part.shape[0]
    wd_y = send(4, wd_ref.at[pl.ds(ep * rows, rows)], wd_part, tp_o, ep)

    for copy in load:
        copy.wait()
    for copy in store:
        copy.start()
    to_y.wait_recv()
    y_to_x = send(5, block(ep, tp_o), block(ep, tp_o), tp, ep_x)
    y_to_c = send(6, block(ep, tp_o), block(ep, tp_o), tp, ep_c)
    to_x.wait_recv()
    x_to_c = send(7, block(ep_x, tp), block(ep_x, tp), tp, ep_c)
    y_to_x.wait_recv()
    xy_to_c = send(8, block(ep_x, tp_o), block(ep_x, tp_o), tp, ep_c)
    for copy in (to_c, dy_y, wd_y, y_to_c, x_to_c, xy_to_c):
        copy.wait_recv()
    for copy in idx_copies:
        copy.wait_recv()
    for copy in store:
        copy.wait()
    for copy in (to_y, to_x, to_c, dy_y, wd_y, y_to_x, y_to_c, x_to_c, xy_to_c):
        copy.wait_send()
    for copy in idx_copies:
        copy.wait_send()


def gather_rows(devices, ep_size, x, idx_t, dy, ws_gate, ws_up, ws_down):
    _, model = x.shape
    any_spec = pl.BlockSpec(memory_space=pl.ANY)
    return pl.pallas_call(
        gather_kernel,
        in_specs=[any_spec] * 6,
        out_specs=[any_spec] * 5,
        out_shape=[
            jax.ShapeDtypeStruct((devices,) + x.shape, x.dtype),
            jax.ShapeDtypeStruct((devices,) + idx_t.shape, idx_t.dtype),
            jax.ShapeDtypeStruct((2,) + dy.shape, dy.dtype),
            jax.ShapeDtypeStruct((ws_down.shape[0] // ep_size, model), ws_down.dtype),
            jax.ShapeDtypeStruct((model, 2 * ws_gate.shape[1] // ep_size), ws_gate.dtype),
        ],
        scratch_shapes=[
            pltpu.SemaphoreType.DMA((9,)),
            pltpu.SemaphoreType.DMA((9,)),
            pltpu.SemaphoreType.DMA((devices - 1,)),
            pltpu.SemaphoreType.DMA((devices - 1,)),
            pltpu.SemaphoreType.DMA((8,)),
            pltpu.VMEM(x.shape, x.dtype),
            pltpu.VMEM(dy.shape, dy.dtype),
            pltpu.VMEM((model, 2 * ws_gate.shape[1] // ep_size), ws_gate.dtype),
        ],
        cost_estimate=pl.CostEstimate(flops=60_000_000_000, bytes_accessed=4 * devices * x.size, transcendentals=0),
        compiler_params=pltpu.CompilerParams(collective_id=0, has_side_effects=True),
        name='gather_rows',
    )(x, idx_t, dy, ws_gate, ws_up, ws_down)


def solution(mesh):
    tp_size = mesh.shape['tp']
    ep_size = mesh.shape['ep']
    swap_tp = [(i, tp_size - 1 - i) for i in range(tp_size)]
    swap_x = [(i, (i + ep_size // 2) % ep_size) for i in range(ep_size)]
    swap_c = [(i, core_partner(i)) for i in range(ep_size)]

    def device_step(x, grad_y, w_router, w_gate, w_up, w_down, ws_gate, ws_up, ws_down, topk_idx):
        tok, model = x.shape
        top_k = topk_idx.shape[1]
        experts = w_router.shape[1]
        local_exp = w_gate.shape[0]
        groups = top_k // 2
        most = groups * tok // (2 * ep_size) + min(groups, ep_size // 2) * tok // ep_size
        cap = (2 * most + local_exp - 1) // local_exp
        half, padded = half_rows(cap, ep_size)
        shift = padded - half
        ep_i = lax.axis_index('ep')
        tp_i = lax.axis_index('tp')
        devices = ep_size * tp_size
        ep_order = (ep_i, (ep_i + ep_size // 2) % ep_size, core_partner(ep_i), core_partner((ep_i + ep_size // 2) % ep_size))

        def ep_pieces(piece):
            far = lax.ppermute(piece, 'ep', swap_x)
            return piece, far, lax.ppermute(piece, 'ep', swap_c), lax.ppermute(far, 'ep', swap_c)

        def ep_gather(piece):
            out = jnp.zeros((ep_size,) + piece.shape, piece.dtype)
            for e, part in zip(ep_order, ep_pieces(piece)):
                out = lax.dynamic_update_slice_in_dim(out, part[None], e, 0)
            return out

        x_blocks, idx_all, dy_pair, wd_part, quarter = gather_rows(devices, ep_size, x, topk_idx.T, grad_y, ws_gate, ws_up, ws_down)
        x_all = x_blocks.reshape(devices * tok, model)

        width_q = ws_gate.shape[1] // ep_size
        gu_part = lax.ppermute(quarter, 'tp', swap_tp)

        lower = (lax.broadcasted_iota(jnp.int32, (tok, tok), 0) > lax.broadcasted_iota(jnp.int32, (tok, tok), 1)).astype(BF16)
        local_ids = ep_i * local_exp + jnp.arange(local_exp, dtype=jnp.int32)
        hit = jnp.any(idx_all[None] == local_ids[:, None, None, None], axis=2)
        rank = jnp.einsum('edj,ij->edi', hit.astype(BF16), lower, preferred_element_type=F32).astype(jnp.int32)
        dev = jnp.arange(devices, dtype=jnp.int32)
        is_own = (dev % tp_size) == tp_i
        parity = jnp.arange(local_exp, dtype=jnp.int32) % 2
        base = (jnp.where(is_own, padded, 0) + (dev // tp_size) * cap)[None, :] + (parity * shift)[:, None]
        row_ids = jnp.where(hit, base[:, :, None] + rank, -1).reshape(local_exp, 1, devices * tok)

        fwd_parts = []
        start = 0
        rows_now = row_ids
        for count in FWD_CHUNKS:
            send, own = expert_fwd(start, count, half, padded, x_all, rows_now, w_gate, w_up, w_down)
            start += count
            rows_now, own = lax.optimization_barrier((rows_now, own))
            fwd_parts.append((lax.ppermute(send, 'tp', swap_tp), own))

        own0 = fwd_parts[-1][1]
        x_late, hit, rank, w_router, own0 = lax.optimization_barrier((x_all, hit, rank, w_router, own0))
        fwd_parts[-1] = (fwd_parts[-1][0], own0)

        logits_t = jnp.einsum('de,td->et', w_router, x_late, preferred_element_type=F32)
        probs_t = jax.nn.softmax(logits_t, axis=0)
        gates_local = GATE_SCALE * lax.dynamic_slice_in_dim(probs_t, ep_i * local_exp, local_exp, 0).reshape(local_exp, 1, devices * tok)

        sizes = windows(cap, ep_size)
        other, win_other, near, win_near = sizes
        per_chunk = local_exp // BWD_CHUNKS
        dev_ep = dev // tp_size
        place = jnp.zeros_like(dev)
        for k, e in enumerate(ep_order[1:]):
            place = jnp.where(dev_ep == e, k * cap, place)
        exp = jnp.arange(local_exp, dtype=jnp.int32)
        far_first = (jnp.where(is_own, win_other, 0) + place)[None, :] + ((exp % per_chunk) * other % 8)[:, None]
        near_first = jnp.where(is_own, win_near, 0)[None, :] + (2 * win_other + exp * near % 8)[:, None]
        first = jnp.where((dev_ep == ep_i)[None, :], near_first, far_first)
        bwd_ids = jnp.where(hit, first[:, :, None] + rank, -1).reshape(local_exp, 1, devices * tok)
        dy_all = ep_gather(dy_pair).reshape(devices * tok, model)
        (d_w_gate, d_w_up, d_w_down), bwd_out = expert_bwd(BWD_CHUNKS, sizes, x_all, dy_all, bwd_ids, gates_local, w_gate, w_up, w_down)
        bwd_parts = [(lax.ppermute(bwd_out[0][0], 'tp', swap_tp), bwd_out[0][1])]

        own_last = bwd_out[-1][1]
        x, grad_y, x_all, dy_all, topk_idx, w_router, own_last = lax.optimization_barrier(
            (x, grad_y, x_all, dy_all, topk_idx, w_router, own_last))
        bwd_out[-1] = (bwd_out[-1][0], own_last)

        gu_other = ep_pieces(gu_part)
        wd_other = jnp.concatenate(ep_pieces(wd_part), axis=0)
        wg_other = jnp.concatenate([p[:, :width_q] for p in gu_other], axis=1)
        wu_other = jnp.concatenate([p[:, width_q:] for p in gu_other], axis=1)
        shared = jnp.zeros((tok, model), F32)
        dx_shared = jnp.zeros((tok, model), F32)
        for wg, wu, wd in ((ws_gate, ws_up, ws_down), (wg_other, wu_other, wd_other)):
            a = rounded(dot(x, wg))
            b = rounded(dot(x, wu))
            dh = rounded(dot(grad_y, wd, NT))
            h, da, db = swiglu_bwd(a, b, dh)
            shared = shared + dot(h, wd)
            dx_shared = dx_shared + dot(da, wg, NT) + dot(db, wu, NT)
        ds_gate, ds_up, ds_down = shared_grad(x_all, dy_all, ws_gate, ws_up, ws_down)

        def back_rows(count):
            return count * cap + (-count * cap) % 8

        def slot_index(count):
            new = jnp.arange(ep_size * back_rows(count), dtype=jnp.int32)
            block, rest = new // back_rows(count), new % back_rows(count)
            return block, rest // cap, rest % cap, rest < count * cap

        def give_back(parts, count):
            recv, own = parts
            rows = (recv + own).astype(BF16)
            src, exp, rank, valid = slot_index(count)
            old = jnp.where(valid, exp * half + src * cap + rank, -1)
            perm = (old[:, None] == jnp.arange(count * half, dtype=jnp.int32)[None, :]).astype(BF16)
            out = dot(perm, rows).astype(BF16)
            out = out.reshape(ep_size, back_rows(count), model)
            return lax.all_to_all(out, 'ep', 0, 0).reshape(ep_size * back_rows(count), model)

        hit_own = jnp.any(topk_idx[:, None, :] == jnp.arange(experts, dtype=jnp.int32)[None, :, None], axis=2)
        rank_own = dot(lower, hit_own.astype(BF16))
        want = jnp.where(hit_own, rank_own, -1.0).astype(BF16)
        probs = jax.nn.softmax(dot(x, w_router), axis=-1)
        prob_parts = jnp.concatenate(split3(probs), axis=0)

        def expand(start, count):
            grp, exp, rank, valid = slot_index(count)
            col = jnp.where(valid, grp * local_exp + start + exp, -1)
            table = (jnp.arange(experts, dtype=jnp.int32)[:, None] == col[None, :]).astype(BF16)
            return table, jnp.where(valid, rank, -2).astype(F32)[None, :]

        routed = jnp.zeros((tok, model), F32)
        d_scores = jnp.zeros((tok, experts), F32)
        start = 0
        for parts, count in zip(fwd_parts, FWD_CHUNKS):
            back = give_back(parts, count)
            table, rank = expand(start, count)
            hits = dot(want, table) == rank
            gates = jnp.where(jnp.concatenate([hits] * 3, axis=0), dot(prob_parts, table), 0.0).astype(BF16)
            routed = routed + GATE_SCALE * sum3(dot(gates, back), 0)
            score = jnp.where(hits, dot(grad_y, back, NT), 0.0)
            part = dot(jnp.concatenate(split3(score), axis=0), table, NT)
            d_scores = d_scores + sum3(part, 0)
            start += count
        y_out = (shared + routed).astype(BF16)

        d_scores = GATE_SCALE * d_scores
        mean_score = jnp.sum(probs * d_scores, axis=-1, keepdims=True)
        d_logits = probs * (d_scores - mean_score)
        d_other = lax.ppermute(d_logits, 'tp', swap_tp)
        for send, own in bwd_out[1:]:
            bwd_parts.append((lax.ppermute(send, 'tp', swap_tp), own))
        d_pair = jnp.where(tp_i == 0, jnp.stack([d_logits, d_other]), jnp.stack([d_other, d_logits]))
        d_logits_all = ep_gather(d_pair).reshape(devices * tok, experts)
        d_router = sum3(dot(x_all, jnp.concatenate(split3(d_logits_all), axis=1), TN), 1)
        dx_sum = dx_shared + sum3(dot(jnp.concatenate(split3(d_logits), axis=0), w_router, NT), 0)

        def hits_of(grp, start, count):
            slot = jnp.arange(count * cap, dtype=jnp.int32)
            col = grp * local_exp + start + slot // cap
            table = (jnp.arange(experts, dtype=jnp.int32)[:, None] == col[None, :]).astype(BF16)
            return (dot(want, table) == (slot % cap).astype(F32)[None, :]).astype(BF16)

        swaps = (swap_x, swap_c, [(i, core_partner(d)) for i, d in swap_x])
        for c, (recv, own) in enumerate(bwd_parts[:-1]):
            rows = (recv + own).astype(BF16)
            slot = jnp.arange(per_chunk * cap, dtype=jnp.int32)
            for k, pairs in enumerate(swaps):
                old = slot // cap * other + k * cap + slot % cap
                perm = (old[:, None] == jnp.arange(per_chunk * other, dtype=jnp.int32)[None, :]).astype(BF16)
                back = dot(perm, rows).astype(BF16)
                back = lax.ppermute(back, 'ep', pairs)
                hits = hits_of(ep_order[1 + k], c * per_chunk, per_chunk)
                dx_sum = dx_sum + dot(hits, back)
        recv, own = bwd_parts[-1]
        dx_sum = lax.optimization_barrier(dx_sum)
        dx_sum = dx_sum + dot(hits_of(ep_i, 0, local_exp), (recv + own).astype(BF16))
        return y_out, dx_sum.astype(BF16), d_router, d_w_gate, d_w_up, d_w_down, ds_gate, ds_up, ds_down

    tok_spec = P(('ep', 'tp'), None)
    in_specs = (tok_spec, tok_spec, P(None, None), P('ep', None, 'tp'), P('ep', None, 'tp'), P('ep', 'tp', None), P(None, 'tp'), P(None, 'tp'), P('tp', None), tok_spec)
    out_specs = (tok_spec, tok_spec, P(None, None), P('ep', None, 'tp'), P('ep', None, 'tp'), P('ep', 'tp', None), P(None, 'tp'), P(None, 'tp'), P('tp', None))

    return jax.shard_map(device_step, mesh=mesh, in_specs=in_specs, out_specs=out_specs, check_vma=False)
```

```python
import functools

import jax
import jax.numpy as jnp
from jax import lax
from jax.experimental import pallas as pl
from jax.experimental.pallas import tpu as pltpu
from jax.sharding import PartitionSpec as P


GATE_SCALE = 16.0
BF16 = jnp.bfloat16
F32 = jnp.float32
FWD_CHUNKS = (2, 8, 6)
BWD_CHUNKS = 2
MESH = pl.DeviceIdType.MESH

NN = (((1,), (0,)), ((), ()))
NT = (((1,), (1,)), ((), ()))
TN = (((0,), (0,)), ((), ()))


def dot(a, b, dims=NN):
    return lax.dot_general(a, b, dims, preferred_element_type=F32)


def sigmoid(v):
    return 1.0 / (1.0 + jnp.exp(-jnp.maximum(v, -88.0)))


def swiglu_fwd(a, b):
    return (a * sigmoid(a) * b).astype(BF16)


def swiglu_bwd(a, b, dh):
    sig = sigmoid(a)
    silu = a * sig
    h = (silu * b).astype(BF16)
    da = (dh * b * (sig * (1.0 + a * (1.0 - sig)))).astype(BF16)
    db = (dh * silu).astype(BF16)
    return h, da, db


def rounded(v):
    return v.astype(BF16).astype(F32)


def half_rows(cap, ep_size):
    half = cap * ep_size
    return half, half + (-half) % 8


def store_parts(parity, part, send_ref, own_ref, half, padded):
    shift = padded - half

    @pl.when(parity == 0)
    def _():
        send_ref[0:half, :] = part[0:half]
        own_ref[0:half, :] = part[padded:padded + half]

    @pl.when(parity == 1)
    def _():
        send_ref[half:2 * half, :] = part[shift:padded]
        own_ref[half:2 * half, :] = part[padded + shift:2 * padded]


def pick_matrix(row_ref, rows):
    ids = row_ref[0]
    iota = lax.broadcasted_iota(jnp.int32, (rows, ids.shape[1]), 0)
    return iota == ids


def pick_rows(pick_ref, table_ref, out_ref, scale=None, step=512):
    @pl.loop(0, table_ref.shape[1] // step)
    def _(i):
        cols = pl.ds(pl.multiple_of(i * step, step), step)
        rows = dot(pick_ref[...], table_ref[:, cols])
        out_ref[:, cols] = (rows if scale is None else rows * scale).astype(out_ref.dtype)


def fwd_kernel(half, padded, x_ref, row_ref, w1_ref, w3_ref, w2_ref, send_ref, own_ref, pick_ref, rows_ref):
    pick_ref[...] = jnp.where(pick_matrix(row_ref, 2 * padded), 1.0, 0.0).astype(BF16)
    pick_rows(pick_ref, x_ref, rows_ref)
    rows = rows_ref[...]
    a = rounded(dot(rows, w1_ref[0]))
    b = rounded(dot(rows, w3_ref[0]))
    h = swiglu_fwd(a, b)
    part = dot(h, w2_ref[0])
    store_parts(pl.program_id(0) % 2, part, send_ref, own_ref, half, padded)


def windows(cap, ep_size):
    other, own = (ep_size - 1) * cap, cap
    return other, other + 7 + (-other - 7) % 8, own, own + 7 + (-own - 7) % 8


def bwd_kernel(sizes, per_chunk, x_ref, dy_ref, row_ref, gate_ref, w1_ref, w3_ref, w2_ref, *refs):
    other, win_other, own, win_own = sizes
    dw1_ref, dw3_ref, dw2_ref = refs[:3]
    outs, (far_ref, near_ref, sem, pick_ref, rows_ref, d_out_ref) = refs[3:-6], refs[-6:]
    chunks = far_ref.shape[0] // 2
    e = pl.program_id(0)
    total = 2 * (win_other + win_own)

    @pl.when(e == 0)
    def _():
        far_ref[...] = jnp.zeros_like(far_ref)
        near_ref[...] = jnp.zeros_like(near_ref)

    hit = pick_matrix(row_ref, total)
    pick_ref[...] = jnp.where(hit, 1.0, 0.0).astype(BF16)
    gates = jnp.sum(jnp.where(hit, gate_ref[0], 0.0), axis=1, keepdims=True)
    pick_rows(pick_ref, x_ref, rows_ref)
    pick_rows(pick_ref, dy_ref, d_out_ref, gates)
    rows, d_out = rows_ref[...], d_out_ref[...]
    a = rounded(dot(rows, w1_ref[0]))
    b = rounded(dot(rows, w3_ref[0]))
    dh = rounded(dot(d_out, w2_ref[0], NT))
    h, da, db = swiglu_bwd(a, b, dh)

    chunk = e // per_chunk
    far_base = pl.multiple_of((e % per_chunk) * other // 8 * 8, 8)
    near_base = pl.multiple_of(e * own // 8 * 8, 8)
    step = 512

    @pl.loop(0, rows_ref.shape[1] // step)
    def _(i):
        cols = pl.ds(pl.multiple_of(i * step, step), step)
        dw2_ref[0, :, cols] = dot(h, d_out_ref[:, cols], TN)
        dw1_ref[0, cols, :] = dot(rows_ref[:, cols], da, TN)
        dw3_ref[0, cols, :] = dot(rows_ref[:, cols], db, TN)
        part = dot(da, w1_ref[0, cols, :], NT) + dot(db, w3_ref[0, cols, :], NT)
        for side in range(2):
            far_ref[chunk * 2 + side, pl.ds(far_base, win_other), cols] += part[side * win_other:(side + 1) * win_other]
            first = 2 * win_other + side * win_own
            near_ref[side, pl.ds(near_base, win_own), cols] += part[first:first + win_own]

    def copies(c):
        out = []
        for side in range(2):
            k = 2 * c + side
            src = far_ref.at[k] if c < chunks else near_ref.at[side]
            out.append(pltpu.make_async_copy(src.at[pl.ds(0, outs[k].shape[0])], outs[k], sem.at[k]))
        return out

    for c in range(chunks):
        @pl.when(e == (c + 1) * per_chunk - 1)
        def _():
            for copy in copies(c):
                copy.start()

    @pl.when(e == chunks * per_chunk - 1)
    def _():
        for copy in copies(chunks):
            copy.start()
        for c in range(chunks + 1):
            for copy in copies(c):
                copy.wait()


def expert_fwd(start, count, half, padded, x_all, row_ids, w_gate, w_up, w_down):
    tokens, model = x_all.shape
    width = w_gate.shape[2]
    out = jax.ShapeDtypeStruct((count * half, model), F32)
    return pl.pallas_call(
        functools.partial(fwd_kernel, half, padded),
        grid=(count,),
        in_specs=[
            pl.BlockSpec((tokens, model), lambda i: (0, 0), pipeline_mode=pl.Buffered(1)),
            pl.BlockSpec((1, 1, tokens), lambda i: (start + i, 0, 0)),
            pl.BlockSpec((1, model, width), lambda i: (start + i, 0, 0)),
            pl.BlockSpec((1, model, width), lambda i: (start + i, 0, 0)),
            pl.BlockSpec((1, width, model), lambda i: (start + i, 0, 0)),
        ],
        out_specs=[pl.BlockSpec((2 * half, model), lambda i: (i // 2, 0))] * 2,
        out_shape=[out, out],
        scratch_shapes=[pltpu.VMEM((2 * padded, tokens), BF16), pltpu.VMEM((2 * padded, model), BF16)],
        cost_estimate=pl.CostEstimate(
            flops=count * 2 * 2 * padded * model * (tokens + 3 * width),
            bytes_accessed=count * (6 * model * width + 8 * half * model) + 2 * tokens * model,
            transcendentals=count * 2 * padded * width),
        compiler_params=pltpu.CompilerParams(dimension_semantics=('arbitrary',), vmem_limit_bytes=48 << 20),
    )(x_all, row_ids, w_gate, w_up, w_down)


def expert_bwd(chunks, sizes, x_all, dy_all, row_ids, gates, w_gate, w_up, w_down):
    other, win_other, own, win_own = sizes
    tokens, model = x_all.shape
    count, _, width = w_gate.shape
    per_chunk = count // chunks
    far_rows, near_rows = per_chunk * other, count * own
    far_pad = max(j * other // 8 * 8 + win_other for j in range(per_chunk))
    near_pad = max(j * own // 8 * 8 + win_own for j in range(count))
    part_shapes = [jax.ShapeDtypeStruct((far_rows, model), F32)] * (2 * chunks) + [jax.ShapeDtypeStruct((near_rows, model), F32)] * 2
    rows = 2 * (win_other + win_own)
    outs = pl.pallas_call(
        functools.partial(bwd_kernel, sizes, per_chunk),
        grid=(count,),
        in_specs=[
            pl.BlockSpec((tokens, model), lambda i: (0, 0), pipeline_mode=pl.Buffered(1)),
            pl.BlockSpec((tokens, model), lambda i: (0, 0), pipeline_mode=pl.Buffered(1)),
            pl.BlockSpec((1, 1, tokens), lambda i: (i, 0, 0)),
            pl.BlockSpec((1, 1, tokens), lambda i: (i, 0, 0)),
            pl.BlockSpec((1, model, width), lambda i: (i, 0, 0)),
            pl.BlockSpec((1, model, width), lambda i: (i, 0, 0)),
            pl.BlockSpec((1, width, model), lambda i: (i, 0, 0)),
        ],
        out_specs=[
            pl.BlockSpec((1, model, width), lambda i: (i, 0, 0)),
            pl.BlockSpec((1, model, width), lambda i: (i, 0, 0)),
            pl.BlockSpec((1, width, model), lambda i: (i, 0, 0)),
        ] + [pl.BlockSpec(memory_space=pl.ANY)] * len(part_shapes),
        out_shape=[
            jax.ShapeDtypeStruct((count, model, width), F32),
            jax.ShapeDtypeStruct((count, model, width), F32),
            jax.ShapeDtypeStruct((count, width, model), F32),
        ] + part_shapes,
        scratch_shapes=[
            pltpu.VMEM((2 * chunks, far_pad, model), F32),
            pltpu.VMEM((2, near_pad, model), F32),
            pltpu.SemaphoreType.DMA((len(part_shapes),)),
            pltpu.VMEM((rows, tokens), BF16),
            pltpu.VMEM((rows, model), BF16),
            pltpu.VMEM((rows, model), BF16),
        ],
        cost_estimate=pl.CostEstimate(
            flops=count * 2 * rows * model * (2 * tokens + 8 * width),
            bytes_accessed=count * (18 * model * width + 4 * rows * model) + 4 * tokens * model,
            transcendentals=count * rows * width),
        compiler_params=pltpu.CompilerParams(dimension_semantics=('arbitrary',), vmem_limit_bytes=60 << 20),
        name='expert_bwd',
    )(x_all, dy_all, row_ids, gates, w_gate, w_up, w_down)
    parts = outs[3:]
    return outs[:3], [(parts[2 * c], parts[2 * c + 1]) for c in range(chunks + 1)]


def shared_grad_kernel(step, x_ref, dy_ref, wg_ref, wu_ref, wd_ref, dg_ref, du_ref, dd_ref, h_ref, da_ref, db_ref):
    tokens, model = x_ref.shape

    @pl.loop(0, tokens // step)
    def _(i):
        rows = pl.ds(pl.multiple_of(i * step, step), step)
        a = rounded(dot(x_ref[rows, :], wg_ref[...]))
        b = rounded(dot(x_ref[rows, :], wu_ref[...]))
        dh = rounded(dot(dy_ref[rows, :], wd_ref[...], NT))
        h_ref[rows, :], da_ref[rows, :], db_ref[rows, :] = swiglu_bwd(a, b, dh)

    @pl.loop(0, model // step)
    def _(i):
        cols = pl.ds(pl.multiple_of(i * step, step), step)
        dd_ref[:, cols] = dot(h_ref[...], dy_ref[:, cols], TN)
        dg_ref[cols, :] = dot(x_ref[:, cols], da_ref[...], TN)
        du_ref[cols, :] = dot(x_ref[:, cols], db_ref[...], TN)


def shared_grad(x_all, dy_all, ws_gate, ws_up, ws_down):
    tokens, model = x_all.shape
    width = ws_gate.shape[1]
    block = min(width, 256)
    full = pl.BlockSpec((tokens, model), lambda i: (0, 0), pipeline_mode=pl.Buffered(1))
    col = pl.BlockSpec((model, block), lambda i: (0, i))
    row = pl.BlockSpec((block, model), lambda i: (i, 0))
    return pl.pallas_call(
        functools.partial(shared_grad_kernel, 256),
        grid=(width // block,),
        in_specs=[full, full, col, col, row],
        out_specs=[col, col, row],
        out_shape=[jax.ShapeDtypeStruct((model, width), F32)] * 2 + [jax.ShapeDtypeStruct((width, model), F32)],
        scratch_shapes=[pltpu.VMEM((tokens, block), BF16)] * 3,
        cost_estimate=pl.CostEstimate(
            flops=12 * tokens * model * width, bytes_accessed=4 * tokens * model + 18 * model * width,
            transcendentals=tokens * width),
        compiler_params=pltpu.CompilerParams(dimension_semantics=('arbitrary',), vmem_limit_bytes=48 << 20),
        name='shared_grad',
    )(x_all, dy_all, ws_gate, ws_up, ws_down)


def split3(v):
    hi = lax.reduce_precision(v, 8, 7)
    rest = v - hi
    mid = lax.reduce_precision(rest, 8, 7)
    low = rest - mid
    return hi.astype(BF16), mid.astype(BF16), low.astype(BF16)


def sum3(v, axis):
    first, second, third = jnp.split(v, 3, axis=axis)
    return first + second + third


def core_partner(ep):
    return ep + 1 - 2 * (ep % 2)


def gather_kernel(x_ref, idx_ref, dy_ref, wg_ref, wu_ref, wd_ref, x_all, idx_all, dy_pair, wd_part, quarter, send_sem, recv_sem, idx_send, idx_recv, local_sem, x_buf, dy_buf, q_buf):
    tp = lax.axis_index('tp')
    ep = lax.axis_index('ep')
    eps = x_all.shape[0] // 2
    half = eps // 2
    tp_o = 1 - tp
    ep_x = (ep + half) % eps
    ep_c = core_partner(ep)

    def slot(e, t):
        return e * 2 + t

    others = [(tp_o, ep)]
    for k in range(1, eps):
        others += [(tp, (ep + k) % eps), (tp_o, (ep + k) % eps)]
    barrier = pltpu.get_barrier_semaphore()
    for t, e in others:
        pl.semaphore_signal(barrier, inc=1, device_id={'tp': t, 'ep': e}, device_id_type=MESH)
    pl.semaphore_wait(barrier, len(others))

    def send(k, src, dst, t, e):
        copy = pltpu.make_async_remote_copy(
            src_ref=src, dst_ref=dst, send_sem=send_sem.at[k], recv_sem=recv_sem.at[k],
            device_id={'tp': t, 'ep': e}, device_id_type=MESH)
        copy.start()
        return copy

    def block(e, t):
        return x_all.at[slot(e, t)]

    mine = block(ep, tp)
    to_y = send(0, x_ref, mine, tp_o, ep)
    to_x = send(1, x_ref, mine, tp, ep_x)
    to_c = send(2, x_ref, mine, tp, ep_c)
    own_idx = idx_all.at[slot(ep, tp)]
    idx_copies = []
    for k, (t, e) in enumerate(others):
        copy = pltpu.make_async_remote_copy(
            src_ref=idx_ref, dst_ref=own_idx, send_sem=idx_send.at[k], recv_sem=idx_recv.at[k],
            device_id={'tp': t, 'ep': e}, device_id_type=MESH)
        copy.start()
        idx_copies.append(copy)
    width = quarter.shape[1] // 2
    cols = pl.ds(pl.multiple_of(ep * width, width), width)
    load = [
        pltpu.make_async_copy(x_ref, x_buf, local_sem.at[0]),
        pltpu.make_async_copy(dy_ref, dy_buf, local_sem.at[1]),
        pltpu.make_async_copy(wg_ref.at[:, cols], q_buf.at[:, pl.ds(0, width)], local_sem.at[2]),
        pltpu.make_async_copy(wu_ref.at[:, cols], q_buf.at[:, pl.ds(width, width)], local_sem.at[3]),
    ]
    store = [
        pltpu.make_async_copy(x_buf, mine, local_sem.at[4]),
        pltpu.make_async_copy(dy_buf, dy_pair.at[tp], local_sem.at[5]),
        pltpu.make_async_copy(q_buf, quarter, local_sem.at[6]),
        pltpu.make_async_copy(idx_ref, own_idx, local_sem.at[7]),
    ]
    for copy in load:
        copy.start()
    dy_y = send(3, dy_ref, dy_pair.at[tp], tp_o, ep)
    rows = wd_part.shape[0]
    wd_y = send(4, wd_ref.at[pl.ds(ep * rows, rows)], wd_part, tp_o, ep)

    for copy in load:
        copy.wait()
    for copy in store:
        copy.start()
    to_y.wait_recv()
    y_to_x = send(5, block(ep, tp_o), block(ep, tp_o), tp, ep_x)
    y_to_c = send(6, block(ep, tp_o), block(ep, tp_o), tp, ep_c)
    to_x.wait_recv()
    x_to_c = send(7, block(ep_x, tp), block(ep_x, tp), tp, ep_c)
    y_to_x.wait_recv()
    xy_to_c = send(8, block(ep_x, tp_o), block(ep_x, tp_o), tp, ep_c)
    for copy in (to_c, dy_y, wd_y, y_to_c, x_to_c, xy_to_c):
        copy.wait_recv()
    for copy in idx_copies:
        copy.wait_recv()
    for copy in store:
        copy.wait()
    for copy in (to_y, to_x, to_c, dy_y, wd_y, y_to_x, y_to_c, x_to_c, xy_to_c):
        copy.wait_send()
    for copy in idx_copies:
        copy.wait_send()


def gather_rows(devices, ep_size, x, idx_t, dy, ws_gate, ws_up, ws_down):
    _, model = x.shape
    any_spec = pl.BlockSpec(memory_space=pl.ANY)
    return pl.pallas_call(
        gather_kernel,
        in_specs=[any_spec] * 6,
        out_specs=[any_spec] * 5,
        out_shape=[
            jax.ShapeDtypeStruct((devices,) + x.shape, x.dtype),
            jax.ShapeDtypeStruct((devices,) + idx_t.shape, idx_t.dtype),
            jax.ShapeDtypeStruct((2,) + dy.shape, dy.dtype),
            jax.ShapeDtypeStruct((ws_down.shape[0] // ep_size, model), ws_down.dtype),
            jax.ShapeDtypeStruct((model, 2 * ws_gate.shape[1] // ep_size), ws_gate.dtype),
        ],
        scratch_shapes=[
            pltpu.SemaphoreType.DMA((9,)),
            pltpu.SemaphoreType.DMA((9,)),
            pltpu.SemaphoreType.DMA((devices - 1,)),
            pltpu.SemaphoreType.DMA((devices - 1,)),
            pltpu.SemaphoreType.DMA((8,)),
            pltpu.VMEM(x.shape, x.dtype),
            pltpu.VMEM(dy.shape, dy.dtype),
            pltpu.VMEM((model, 2 * ws_gate.shape[1] // ep_size), ws_gate.dtype),
        ],
        cost_estimate=pl.CostEstimate(flops=60_000_000_000, bytes_accessed=4 * devices * x.size, transcendentals=0),
        compiler_params=pltpu.CompilerParams(collective_id=0, has_side_effects=True),
        name='gather_rows',
    )(x, idx_t, dy, ws_gate, ws_up, ws_down)


def solution(mesh):
    tp_size = mesh.shape['tp']
    ep_size = mesh.shape['ep']
    swap_tp = [(i, tp_size - 1 - i) for i in range(tp_size)]
    swap_x = [(i, (i + ep_size // 2) % ep_size) for i in range(ep_size)]
    swap_c = [(i, core_partner(i)) for i in range(ep_size)]

    def device_step(x, grad_y, w_router, w_gate, w_up, w_down, ws_gate, ws_up, ws_down, topk_idx):
        tok, model = x.shape
        top_k = topk_idx.shape[1]
        experts = w_router.shape[1]
        local_exp = w_gate.shape[0]
        groups = top_k // 2
        most = groups * tok // (2 * ep_size) + min(groups, ep_size // 2) * tok // ep_size
        cap = (2 * most + local_exp - 1) // local_exp
        half, padded = half_rows(cap, ep_size)
        shift = padded - half
        ep_i = lax.axis_index('ep')
        tp_i = lax.axis_index('tp')
        devices = ep_size * tp_size
        ep_order = (ep_i, (ep_i + ep_size // 2) % ep_size, core_partner(ep_i), core_partner((ep_i + ep_size // 2) % ep_size))

        def ep_pieces(piece):
            far = lax.ppermute(piece, 'ep', swap_x)
            return piece, far, lax.ppermute(piece, 'ep', swap_c), lax.ppermute(far, 'ep', swap_c)

        def ep_gather(piece):
            out = jnp.zeros((ep_size,) + piece.shape, piece.dtype)
            for e, part in zip(ep_order, ep_pieces(piece)):
                out = lax.dynamic_update_slice_in_dim(out, part[None], e, 0)
            return out

        x_blocks, idx_all, dy_pair, wd_part, quarter = gather_rows(devices, ep_size, x, topk_idx.T, grad_y, ws_gate, ws_up, ws_down)
        x_all = x_blocks.reshape(devices * tok, model)

        width_q = ws_gate.shape[1] // ep_size
        gu_part = lax.ppermute(quarter, 'tp', swap_tp)

        lower = (lax.broadcasted_iota(jnp.int32, (tok, tok), 0) > lax.broadcasted_iota(jnp.int32, (tok, tok), 1)).astype(BF16)
        local_ids = ep_i * local_exp + jnp.arange(local_exp, dtype=jnp.int32)
        hit = jnp.any(idx_all[None] == local_ids[:, None, None, None], axis=2)
        rank = jnp.einsum('edj,ij->edi', hit.astype(BF16), lower, preferred_element_type=F32).astype(jnp.int32)
        dev = jnp.arange(devices, dtype=jnp.int32)
        is_own = (dev % tp_size) == tp_i
        parity = jnp.arange(local_exp, dtype=jnp.int32) % 2
        base = (jnp.where(is_own, padded, 0) + (dev // tp_size) * cap)[None, :] + (parity * shift)[:, None]
        row_ids = jnp.where(hit, base[:, :, None] + rank, -1).reshape(local_exp, 1, devices * tok)

        fwd_parts = []
        start = 0
        rows_now = row_ids
        for count in FWD_CHUNKS:
            send, own = expert_fwd(start, count, half, padded, x_all, rows_now, w_gate, w_up, w_down)
            start += count
            rows_now, own = lax.optimization_barrier((rows_now, own))
            fwd_parts.append((lax.ppermute(send, 'tp', swap_tp), own))

        own0 = fwd_parts[-1][1]
        x_late, hit, rank, w_router, own0 = lax.optimization_barrier((x_all, hit, rank, w_router, own0))
        fwd_parts[-1] = (fwd_parts[-1][0], own0)

        logits_t = jnp.einsum('de,td->et', w_router, x_late, preferred_element_type=F32)
        probs_t = jax.nn.softmax(logits_t, axis=0)
        gates_local = GATE_SCALE * lax.dynamic_slice_in_dim(probs_t, ep_i * local_exp, local_exp, 0).reshape(local_exp, 1, devices * tok)

        sizes = windows(cap, ep_size)
        other, win_other, near, win_near = sizes
        per_chunk = local_exp // BWD_CHUNKS
        dev_ep = dev // tp_size
        place = jnp.zeros_like(dev)
        for k, e in enumerate(ep_order[1:]):
            place = jnp.where(dev_ep == e, k * cap, place)
        exp = jnp.arange(local_exp, dtype=jnp.int32)
        far_first = (jnp.where(is_own, win_other, 0) + place)[None, :] + ((exp % per_chunk) * other % 8)[:, None]
        near_first = jnp.where(is_own, win_near, 0)[None, :] + (2 * win_other + exp * near % 8)[:, None]
        first = jnp.where((dev_ep == ep_i)[None, :], near_first, far_first)
        bwd_ids = jnp.where(hit, first[:, :, None] + rank, -1).reshape(local_exp, 1, devices * tok)
        dy_all = ep_gather(dy_pair).reshape(devices * tok, model)
        (d_w_gate, d_w_up, d_w_down), bwd_out = expert_bwd(BWD_CHUNKS, sizes, x_all, dy_all, bwd_ids, gates_local, w_gate, w_up, w_down)
        bwd_parts = [(lax.ppermute(bwd_out[0][0], 'tp', swap_tp), bwd_out[0][1])]

        own_last = bwd_out[-1][1]
        own_first = fwd_parts[0][1]
        x, grad_y, x_all, dy_all, topk_idx, w_router, gu_part, wd_part, own_first, own_last = lax.optimization_barrier(
            (x, grad_y, x_all, dy_all, topk_idx, w_router, gu_part, wd_part, own_first, own_last))
        fwd_parts[0] = (fwd_parts[0][0], own_first)
        bwd_out[-1] = (bwd_out[-1][0], own_last)

        gu_other = ep_pieces(gu_part)
        wd_other = jnp.concatenate(ep_pieces(wd_part), axis=0)
        wg_other = jnp.concatenate([p[:, :width_q] for p in gu_other], axis=1)
        wu_other = jnp.concatenate([p[:, width_q:] for p in gu_other], axis=1)
        shared = jnp.zeros((tok, model), F32)
        dx_shared = jnp.zeros((tok, model), F32)
        for wg, wu, wd in ((ws_gate, ws_up, ws_down), (wg_other, wu_other, wd_other)):
            a = rounded(dot(x, wg))
            b = rounded(dot(x, wu))
            dh = rounded(dot(grad_y, wd, NT))
            h, da, db = swiglu_bwd(a, b, dh)
            shared = shared + dot(h, wd)
            dx_shared = dx_shared + dot(da, wg, NT) + dot(db, wu, NT)
        ds_gate, ds_up, ds_down = shared_grad(x_all, dy_all, ws_gate, ws_up, ws_down)

        def back_rows(count):
            return count * cap + (-count * cap) % 8

        def slot_index(count):
            new = jnp.arange(ep_size * back_rows(count), dtype=jnp.int32)
            block, rest = new // back_rows(count), new % back_rows(count)
            return block, rest // cap, rest % cap, rest < count * cap

        def give_back(parts, count):
            recv, own = parts
            rows = (recv + own).astype(BF16)
            src, exp, rank, valid = slot_index(count)
            old = jnp.where(valid, exp * half + src * cap + rank, -1)
            perm = (old[:, None] == jnp.arange(count * half, dtype=jnp.int32)[None, :]).astype(BF16)
            out = dot(perm, rows).astype(BF16)
            out = out.reshape(ep_size, back_rows(count), model)
            return lax.all_to_all(out, 'ep', 0, 0).reshape(ep_size * back_rows(count), model)

        hit_own = jnp.any(topk_idx[:, None, :] == jnp.arange(experts, dtype=jnp.int32)[None, :, None], axis=2)
        rank_own = dot(lower, hit_own.astype(BF16))
        want = jnp.where(hit_own, rank_own, -1.0).astype(BF16)
        probs = jax.nn.softmax(dot(x, w_router), axis=-1)
        prob_parts = jnp.concatenate(split3(probs), axis=0)

        def expand(start, count):
            grp, exp, rank, valid = slot_index(count)
            col = jnp.where(valid, grp * local_exp + start + exp, -1)
            table = (jnp.arange(experts, dtype=jnp.int32)[:, None] == col[None, :]).astype(BF16)
            return table, jnp.where(valid, rank, -2).astype(F32)[None, :]

        routed = jnp.zeros((tok, model), F32)
        d_scores = jnp.zeros((tok, experts), F32)
        start = 0
        for parts, count in zip(fwd_parts, FWD_CHUNKS):
            back = give_back(parts, count)
            table, rank = expand(start, count)
            hits = dot(want, table) == rank
            gates = jnp.where(jnp.concatenate([hits] * 3, axis=0), dot(prob_parts, table), 0.0).astype(BF16)
            routed = routed + GATE_SCALE * sum3(dot(gates, back), 0)
            score = jnp.where(hits, dot(grad_y, back, NT), 0.0)
            part = dot(jnp.concatenate(split3(score), axis=0), table, NT)
            d_scores = d_scores + sum3(part, 0)
            start += count
        y_out = (shared + routed).astype(BF16)

        d_scores = GATE_SCALE * d_scores
        mean_score = jnp.sum(probs * d_scores, axis=-1, keepdims=True)
        d_logits = probs * (d_scores - mean_score)
        d_other = lax.ppermute(d_logits, 'tp', swap_tp)
        for send, own in bwd_out[1:]:
            bwd_parts.append((lax.ppermute(send, 'tp', swap_tp), own))
        d_pair = jnp.where(tp_i == 0, jnp.stack([d_logits, d_other]), jnp.stack([d_other, d_logits]))
        d_logits_all = ep_gather(d_pair).reshape(devices * tok, experts)
        d_router = dot(x_all, jnp.concatenate(split3(d_logits_all), axis=1), TN)
        d_router = sum3(d_router, 1)
        dx_sum = dx_shared + sum3(dot(jnp.concatenate(split3(d_logits), axis=0), w_router, NT), 0)

        def hits_of(grp, start, count):
            slot = jnp.arange(count * cap, dtype=jnp.int32)
            col = grp * local_exp + start + slot // cap
            table = (jnp.arange(experts, dtype=jnp.int32)[:, None] == col[None, :]).astype(BF16)
            return (dot(want, table) == (slot % cap).astype(F32)[None, :]).astype(BF16)

        swaps = (swap_x, swap_c, [(i, core_partner(d)) for i, d in swap_x])
        for c, (recv, own) in enumerate(bwd_parts[:-1]):
            rows = (recv + own).astype(BF16)
            slot = jnp.arange(per_chunk * cap, dtype=jnp.int32)
            for k, pairs in enumerate(swaps):
                old = slot // cap * other + k * cap + slot % cap
                perm = (old[:, None] == jnp.arange(per_chunk * other, dtype=jnp.int32)[None, :]).astype(BF16)
                back = dot(perm, rows).astype(BF16)
                back = lax.ppermute(back, 'ep', pairs)
                hits = hits_of(ep_order[1 + k], c * per_chunk, per_chunk)
                dx_sum = dx_sum + dot(hits, back)
            dx_sum = lax.optimization_barrier(dx_sum)
        recv, own = bwd_parts[-1]
        dx_sum = dx_sum + dot(hits_of(ep_i, 0, local_exp), (recv + own).astype(BF16))
        return y_out, dx_sum.astype(BF16), d_router, d_w_gate, d_w_up, d_w_down, ds_gate, ds_up, ds_down

    tok_spec = P(('ep', 'tp'), None)
    in_specs = (tok_spec, tok_spec, P(None, None), P('ep', None, 'tp'), P('ep', None, 'tp'), P('ep', 'tp', None), P(None, 'tp'), P(None, 'tp'), P('tp', None), tok_spec)
    out_specs = (tok_spec, tok_spec, P(None, None), P('ep', None, 'tp'), P('ep', None, 'tp'), P('ep', 'tp', None), P(None, 'tp'), P(None, 'tp'), P('tp', None))

    return jax.shard_map(device_step, mesh=mesh, in_specs=in_specs, out_specs=out_specs, check_vma=False)
```

```python
import functools

import jax
import jax.numpy as jnp
from jax import lax
from jax.experimental import pallas as pl
from jax.experimental.pallas import tpu as pltpu
from jax.sharding import PartitionSpec as P


GATE_SCALE = 16.0
BF16 = jnp.bfloat16
F32 = jnp.float32
FWD_CHUNKS = (2, 8, 6)
BWD_CHUNKS = 2
MESH = pl.DeviceIdType.MESH

NN = (((1,), (0,)), ((), ()))
NT = (((1,), (1,)), ((), ()))
TN = (((0,), (0,)), ((), ()))


def dot(a, b, dims=NN):
    return lax.dot_general(a, b, dims, preferred_element_type=F32)


def sigmoid(v):
    return 1.0 / (1.0 + jnp.exp(-jnp.maximum(v, -88.0)))


def swiglu_fwd(a, b):
    return (a * sigmoid(a) * b).astype(BF16)


def swiglu_bwd(a, b, dh):
    sig = sigmoid(a)
    silu = a * sig
    h = (silu * b).astype(BF16)
    da = (dh * b * (sig * (1.0 + a * (1.0 - sig)))).astype(BF16)
    db = (dh * silu).astype(BF16)
    return h, da, db


def rounded(v):
    return v.astype(BF16).astype(F32)


def half_rows(cap, ep_size):
    half = cap * ep_size
    return half, half + (-half) % 8


def store_parts(parity, part, send_ref, own_ref, half, padded):
    shift = padded - half

    @pl.when(parity == 0)
    def _():
        send_ref[0:half, :] = part[0:half]
        own_ref[0:half, :] = part[padded:padded + half]

    @pl.when(parity == 1)
    def _():
        send_ref[half:2 * half, :] = part[shift:padded]
        own_ref[half:2 * half, :] = part[padded + shift:2 * padded]


def pick_matrix(row_ref, rows):
    ids = row_ref[0]
    iota = lax.broadcasted_iota(jnp.int32, (rows, ids.shape[1]), 0)
    return iota == ids


def pick_rows(pick_ref, table_ref, out_ref, scale=None, step=512):
    @pl.loop(0, table_ref.shape[1] // step)
    def _(i):
        cols = pl.ds(pl.multiple_of(i * step, step), step)
        rows = dot(pick_ref[...], table_ref[:, cols])
        out_ref[:, cols] = (rows if scale is None else rows * scale).astype(out_ref.dtype)


def fwd_kernel(half, padded, x_ref, row_ref, w1_ref, w3_ref, w2_ref, send_ref, own_ref, pick_ref, rows_ref):
    pick_ref[...] = jnp.where(pick_matrix(row_ref, 2 * padded), 1.0, 0.0).astype(BF16)
    pick_rows(pick_ref, x_ref, rows_ref)
    rows = rows_ref[...]
    a = rounded(dot(rows, w1_ref[0]))
    b = rounded(dot(rows, w3_ref[0]))
    h = swiglu_fwd(a, b)
    part = dot(h, w2_ref[0])
    store_parts(pl.program_id(0) % 2, part, send_ref, own_ref, half, padded)


def windows(cap, ep_size):
    other, own = (ep_size - 1) * cap, cap
    return other, other + 7 + (-other - 7) % 8, own, own + 7 + (-own - 7) % 8


def bwd_kernel(sizes, per_chunk, x_ref, dy_ref, row_ref, gate_ref, w1_ref, w3_ref, w2_ref, *refs):
    other, win_other, own, win_own = sizes
    dw1_ref, dw3_ref, dw2_ref = refs[:3]
    outs, (far_ref, near_ref, sem, pick_ref, rows_ref, d_out_ref) = refs[3:-6], refs[-6:]
    chunks = far_ref.shape[0] // 2
    e = pl.program_id(0)
    total = 2 * (win_other + win_own)

    @pl.when(e == 0)
    def _():
        far_ref[...] = jnp.zeros_like(far_ref)
        near_ref[...] = jnp.zeros_like(near_ref)

    hit = pick_matrix(row_ref, total)
    pick_ref[...] = jnp.where(hit, 1.0, 0.0).astype(BF16)
    gates = jnp.sum(jnp.where(hit, gate_ref[0], 0.0), axis=1, keepdims=True)
    pick_rows(pick_ref, x_ref, rows_ref)
    pick_rows(pick_ref, dy_ref, d_out_ref, gates)
    rows, d_out = rows_ref[...], d_out_ref[...]
    a = rounded(dot(rows, w1_ref[0]))
    b = rounded(dot(rows, w3_ref[0]))
    dh = rounded(dot(d_out, w2_ref[0], NT))
    h, da, db = swiglu_bwd(a, b, dh)

    chunk = e // per_chunk
    far_base = pl.multiple_of((e % per_chunk) * other // 8 * 8, 8)
    near_base = pl.multiple_of(e * own // 8 * 8, 8)
    step = 512

    @pl.loop(0, rows_ref.shape[1] // step)
    def _(i):
        cols = pl.ds(pl.multiple_of(i * step, step), step)
        dw2_ref[0, :, cols] = dot(h, d_out_ref[:, cols], TN)
        dw1_ref[0, cols, :] = dot(rows_ref[:, cols], da, TN)
        dw3_ref[0, cols, :] = dot(rows_ref[:, cols], db, TN)
        part = dot(da, w1_ref[0, cols, :], NT) + dot(db, w3_ref[0, cols, :], NT)
        for side in range(2):
            far_ref[chunk * 2 + side, pl.ds(far_base, win_other), cols] += part[side * win_other:(side + 1) * win_other]
            first = 2 * win_other + side * win_own
            near_ref[side, pl.ds(near_base, win_own), cols] += part[first:first + win_own]

    def copies(c):
        out = []
        for side in range(2):
            k = 2 * c + side
            src = far_ref.at[k] if c < chunks else near_ref.at[side]
            out.append(pltpu.make_async_copy(src.at[pl.ds(0, outs[k].shape[0])], outs[k], sem.at[k]))
        return out

    for c in range(chunks):
        @pl.when(e == (c + 1) * per_chunk - 1)
        def _():
            for copy in copies(c):
                copy.start()

    @pl.when(e == chunks * per_chunk - 1)
    def _():
        for copy in copies(chunks):
            copy.start()
        for c in range(chunks + 1):
            for copy in copies(c):
                copy.wait()


def expert_fwd(start, count, half, padded, x_all, row_ids, w_gate, w_up, w_down):
    tokens, model = x_all.shape
    width = w_gate.shape[2]
    out = jax.ShapeDtypeStruct((count * half, model), F32)
    return pl.pallas_call(
        functools.partial(fwd_kernel, half, padded),
        grid=(count,),
        in_specs=[
            pl.BlockSpec((tokens, model), lambda i: (0, 0), pipeline_mode=pl.Buffered(1)),
            pl.BlockSpec((1, 1, tokens), lambda i: (start + i, 0, 0)),
            pl.BlockSpec((1, model, width), lambda i: (start + i, 0, 0)),
            pl.BlockSpec((1, model, width), lambda i: (start + i, 0, 0)),
            pl.BlockSpec((1, width, model), lambda i: (start + i, 0, 0)),
        ],
        out_specs=[pl.BlockSpec((2 * half, model), lambda i: (i // 2, 0))] * 2,
        out_shape=[out, out],
        scratch_shapes=[pltpu.VMEM((2 * padded, tokens), BF16), pltpu.VMEM((2 * padded, model), BF16)],
        cost_estimate=pl.CostEstimate(
            flops=count * 2 * 2 * padded * model * (tokens + 3 * width),
            bytes_accessed=count * (6 * model * width + 8 * half * model) + 2 * tokens * model,
            transcendentals=count * 2 * padded * width),
        compiler_params=pltpu.CompilerParams(dimension_semantics=('arbitrary',), vmem_limit_bytes=48 << 20),
    )(x_all, row_ids, w_gate, w_up, w_down)


def expert_bwd(chunks, sizes, x_all, dy_all, row_ids, gates, w_gate, w_up, w_down):
    other, win_other, own, win_own = sizes
    tokens, model = x_all.shape
    count, _, width = w_gate.shape
    per_chunk = count // chunks
    far_rows, near_rows = per_chunk * other, count * own
    far_pad = max(j * other // 8 * 8 + win_other for j in range(per_chunk))
    near_pad = max(j * own // 8 * 8 + win_own for j in range(count))
    part_shapes = [jax.ShapeDtypeStruct((far_rows, model), F32)] * (2 * chunks) + [jax.ShapeDtypeStruct((near_rows, model), F32)] * 2
    rows = 2 * (win_other + win_own)
    outs = pl.pallas_call(
        functools.partial(bwd_kernel, sizes, per_chunk),
        grid=(count,),
        in_specs=[
            pl.BlockSpec((tokens, model), lambda i: (0, 0), pipeline_mode=pl.Buffered(1)),
            pl.BlockSpec((tokens, model), lambda i: (0, 0), pipeline_mode=pl.Buffered(1)),
            pl.BlockSpec((1, 1, tokens), lambda i: (i, 0, 0)),
            pl.BlockSpec((1, 1, tokens), lambda i: (i, 0, 0)),
            pl.BlockSpec((1, model, width), lambda i: (i, 0, 0)),
            pl.BlockSpec((1, model, width), lambda i: (i, 0, 0)),
            pl.BlockSpec((1, width, model), lambda i: (i, 0, 0)),
        ],
        out_specs=[
            pl.BlockSpec((1, model, width), lambda i: (i, 0, 0)),
            pl.BlockSpec((1, model, width), lambda i: (i, 0, 0)),
            pl.BlockSpec((1, width, model), lambda i: (i, 0, 0)),
        ] + [pl.BlockSpec(memory_space=pl.ANY)] * len(part_shapes),
        out_shape=[
            jax.ShapeDtypeStruct((count, model, width), F32),
            jax.ShapeDtypeStruct((count, model, width), F32),
            jax.ShapeDtypeStruct((count, width, model), F32),
        ] + part_shapes,
        scratch_shapes=[
            pltpu.VMEM((2 * chunks, far_pad, model), F32),
            pltpu.VMEM((2, near_pad, model), F32),
            pltpu.SemaphoreType.DMA((len(part_shapes),)),
            pltpu.VMEM((rows, tokens), BF16),
            pltpu.VMEM((rows, model), BF16),
            pltpu.VMEM((rows, model), BF16),
        ],
        cost_estimate=pl.CostEstimate(
            flops=count * 2 * rows * model * (2 * tokens + 8 * width),
            bytes_accessed=count * (18 * model * width + 4 * rows * model) + 4 * tokens * model,
            transcendentals=count * rows * width),
        compiler_params=pltpu.CompilerParams(dimension_semantics=('arbitrary',), vmem_limit_bytes=60 << 20),
        name='expert_bwd',
    )(x_all, dy_all, row_ids, gates, w_gate, w_up, w_down)
    parts = outs[3:]
    return outs[:3], [(parts[2 * c], parts[2 * c + 1]) for c in range(chunks + 1)]


def shared_grad_kernel(step, x_ref, dy_ref, wg_ref, wu_ref, wd_ref, dg_ref, du_ref, dd_ref, h_ref, da_ref, db_ref):
    tokens, model = x_ref.shape

    @pl.loop(0, tokens // step)
    def _(i):
        rows = pl.ds(pl.multiple_of(i * step, step), step)
        a = rounded(dot(x_ref[rows, :], wg_ref[...]))
        b = rounded(dot(x_ref[rows, :], wu_ref[...]))
        dh = rounded(dot(dy_ref[rows, :], wd_ref[...], NT))
        h_ref[rows, :], da_ref[rows, :], db_ref[rows, :] = swiglu_bwd(a, b, dh)

    @pl.loop(0, model // step)
    def _(i):
        cols = pl.ds(pl.multiple_of(i * step, step), step)
        dd_ref[:, cols] = dot(h_ref[...], dy_ref[:, cols], TN)
        dg_ref[cols, :] = dot(x_ref[:, cols], da_ref[...], TN)
        du_ref[cols, :] = dot(x_ref[:, cols], db_ref[...], TN)


def shared_grad(x_all, dy_all, ws_gate, ws_up, ws_down):
    tokens, model = x_all.shape
    width = ws_gate.shape[1]
    block = min(width, 256)
    full = pl.BlockSpec((tokens, model), lambda i: (0, 0), pipeline_mode=pl.Buffered(1))
    col = pl.BlockSpec((model, block), lambda i: (0, i))
    row = pl.BlockSpec((block, model), lambda i: (i, 0))
    return pl.pallas_call(
        functools.partial(shared_grad_kernel, 256),
        grid=(width // block,),
        in_specs=[full, full, col, col, row],
        out_specs=[col, col, row],
        out_shape=[jax.ShapeDtypeStruct((model, width), F32)] * 2 + [jax.ShapeDtypeStruct((width, model), F32)],
        scratch_shapes=[pltpu.VMEM((tokens, block), BF16)] * 3,
        cost_estimate=pl.CostEstimate(
            flops=12 * tokens * model * width, bytes_accessed=4 * tokens * model + 18 * model * width,
            transcendentals=tokens * width),
        compiler_params=pltpu.CompilerParams(dimension_semantics=('arbitrary',), vmem_limit_bytes=48 << 20),
        name='shared_grad',
    )(x_all, dy_all, ws_gate, ws_up, ws_down)


def split3(v):
    hi = lax.reduce_precision(v, 8, 7)
    rest = v - hi
    mid = lax.reduce_precision(rest, 8, 7)
    low = rest - mid
    return hi.astype(BF16), mid.astype(BF16), low.astype(BF16)


def sum3(v, axis):
    first, second, third = jnp.split(v, 3, axis=axis)
    return first + second + third


def core_partner(ep):
    return ep + 1 - 2 * (ep % 2)


def gather_kernel(x_ref, idx_ref, dy_ref, wg_ref, wu_ref, wd_ref, x_all, idx_all, dy_pair, wd_part, quarter, send_sem, recv_sem, idx_send, idx_recv, local_sem, x_buf, dy_buf, q_buf):
    tp = lax.axis_index('tp')
    ep = lax.axis_index('ep')
    eps = x_all.shape[0] // 2
    half = eps // 2
    tp_o = 1 - tp
    ep_x = (ep + half) % eps
    ep_c = core_partner(ep)

    def slot(e, t):
        return e * 2 + t

    others = [(tp_o, ep)]
    for k in range(1, eps):
        others += [(tp, (ep + k) % eps), (tp_o, (ep + k) % eps)]
    barrier = pltpu.get_barrier_semaphore()
    for t, e in others:
        pl.semaphore_signal(barrier, inc=1, device_id={'tp': t, 'ep': e}, device_id_type=MESH)
    pl.semaphore_wait(barrier, len(others))

    def send(k, src, dst, t, e):
        copy = pltpu.make_async_remote_copy(
            src_ref=src, dst_ref=dst, send_sem=send_sem.at[k], recv_sem=recv_sem.at[k],
            device_id={'tp': t, 'ep': e}, device_id_type=MESH)
        copy.start()
        return copy

    def block(e, t):
        return x_all.at[slot(e, t)]

    mine = block(ep, tp)
    to_y = send(0, x_ref, mine, tp_o, ep)
    to_x = send(1, x_ref, mine, tp, ep_x)
    to_c = send(2, x_ref, mine, tp, ep_c)
    own_idx = idx_all.at[slot(ep, tp)]
    idx_copies = []
    for k, (t, e) in enumerate(others):
        copy = pltpu.make_async_remote_copy(
            src_ref=idx_ref, dst_ref=own_idx, send_sem=idx_send.at[k], recv_sem=idx_recv.at[k],
            device_id={'tp': t, 'ep': e}, device_id_type=MESH)
        copy.start()
        idx_copies.append(copy)
    width = quarter.shape[1] // 2
    cols = pl.ds(pl.multiple_of(ep * width, width), width)
    load = [
        pltpu.make_async_copy(x_ref, x_buf, local_sem.at[0]),
        pltpu.make_async_copy(dy_ref, dy_buf, local_sem.at[1]),
        pltpu.make_async_copy(wg_ref.at[:, cols], q_buf.at[:, pl.ds(0, width)], local_sem.at[2]),
        pltpu.make_async_copy(wu_ref.at[:, cols], q_buf.at[:, pl.ds(width, width)], local_sem.at[3]),
    ]
    store = [
        pltpu.make_async_copy(x_buf, mine, local_sem.at[4]),
        pltpu.make_async_copy(dy_buf, dy_pair.at[tp], local_sem.at[5]),
        pltpu.make_async_copy(q_buf, quarter, local_sem.at[6]),
        pltpu.make_async_copy(idx_ref, own_idx, local_sem.at[7]),
    ]
    for copy in load:
        copy.start()
    dy_y = send(3, dy_ref, dy_pair.at[tp], tp_o, ep)
    rows = wd_part.shape[0]
    wd_y = send(4, wd_ref.at[pl.ds(ep * rows, rows)], wd_part, tp_o, ep)

    for copy in load:
        copy.wait()
    for copy in store:
        copy.start()
    to_y.wait_recv()
    y_to_x = send(5, block(ep, tp_o), block(ep, tp_o), tp, ep_x)
    y_to_c = send(6, block(ep, tp_o), block(ep, tp_o), tp, ep_c)
    to_x.wait_recv()
    x_to_c = send(7, block(ep_x, tp), block(ep_x, tp), tp, ep_c)
    y_to_x.wait_recv()
    xy_to_c = send(8, block(ep_x, tp_o), block(ep_x, tp_o), tp, ep_c)
    for copy in (to_c, dy_y, wd_y, y_to_c, x_to_c, xy_to_c):
        copy.wait_recv()
    for copy in idx_copies:
        copy.wait_recv()
    for copy in store:
        copy.wait()
    for copy in (to_y, to_x, to_c, dy_y, wd_y, y_to_x, y_to_c, x_to_c, xy_to_c):
        copy.wait_send()
    for copy in idx_copies:
        copy.wait_send()


def gather_rows(devices, ep_size, x, idx_t, dy, ws_gate, ws_up, ws_down):
    _, model = x.shape
    any_spec = pl.BlockSpec(memory_space=pl.ANY)
    return pl.pallas_call(
        gather_kernel,
        in_specs=[any_spec] * 6,
        out_specs=[any_spec] * 5,
        out_shape=[
            jax.ShapeDtypeStruct((devices,) + x.shape, x.dtype),
            jax.ShapeDtypeStruct((devices,) + idx_t.shape, idx_t.dtype),
            jax.ShapeDtypeStruct((2,) + dy.shape, dy.dtype),
            jax.ShapeDtypeStruct((ws_down.shape[0] // ep_size, model), ws_down.dtype),
            jax.ShapeDtypeStruct((model, 2 * ws_gate.shape[1] // ep_size), ws_gate.dtype),
        ],
        scratch_shapes=[
            pltpu.SemaphoreType.DMA((9,)),
            pltpu.SemaphoreType.DMA((9,)),
            pltpu.SemaphoreType.DMA((devices - 1,)),
            pltpu.SemaphoreType.DMA((devices - 1,)),
            pltpu.SemaphoreType.DMA((8,)),
            pltpu.VMEM(x.shape, x.dtype),
            pltpu.VMEM(dy.shape, dy.dtype),
            pltpu.VMEM((model, 2 * ws_gate.shape[1] // ep_size), ws_gate.dtype),
        ],
        cost_estimate=pl.CostEstimate(flops=60_000_000_000, bytes_accessed=4 * devices * x.size, transcendentals=0),
        compiler_params=pltpu.CompilerParams(collective_id=0, has_side_effects=True),
        name='gather_rows',
    )(x, idx_t, dy, ws_gate, ws_up, ws_down)


def solution(mesh):
    tp_size = mesh.shape['tp']
    ep_size = mesh.shape['ep']
    swap_tp = [(i, tp_size - 1 - i) for i in range(tp_size)]
    swap_x = [(i, (i + ep_size // 2) % ep_size) for i in range(ep_size)]
    swap_c = [(i, core_partner(i)) for i in range(ep_size)]

    def device_step(x, grad_y, w_router, w_gate, w_up, w_down, ws_gate, ws_up, ws_down, topk_idx):
        tok, model = x.shape
        top_k = topk_idx.shape[1]
        experts = w_router.shape[1]
        local_exp = w_gate.shape[0]
        groups = top_k // 2
        most = groups * tok // (2 * ep_size) + min(groups, ep_size // 2) * tok // ep_size
        cap = (2 * most + local_exp - 1) // local_exp
        half, padded = half_rows(cap, ep_size)
        shift = padded - half
        ep_i = lax.axis_index('ep')
        tp_i = lax.axis_index('tp')
        devices = ep_size * tp_size
        ep_order = (ep_i, (ep_i + ep_size // 2) % ep_size, core_partner(ep_i), core_partner((ep_i + ep_size // 2) % ep_size))

        def ep_pieces(piece):
            far = lax.ppermute(piece, 'ep', swap_x)
            return piece, far, lax.ppermute(piece, 'ep', swap_c), lax.ppermute(far, 'ep', swap_c)

        def ep_gather(piece):
            out = jnp.zeros((ep_size,) + piece.shape, piece.dtype)
            for e, part in zip(ep_order, ep_pieces(piece)):
                out = lax.dynamic_update_slice_in_dim(out, part[None], e, 0)
            return out

        x_blocks, idx_all, dy_pair, wd_part, quarter = gather_rows(devices, ep_size, x, topk_idx.T, grad_y, ws_gate, ws_up, ws_down)
        x_all = x_blocks.reshape(devices * tok, model)

        width_q = ws_gate.shape[1] // ep_size
        gu_part = lax.ppermute(quarter, 'tp', swap_tp)

        lower = (lax.broadcasted_iota(jnp.int32, (tok, tok), 0) > lax.broadcasted_iota(jnp.int32, (tok, tok), 1)).astype(BF16)
        local_ids = ep_i * local_exp + jnp.arange(local_exp, dtype=jnp.int32)
        hit = jnp.any(idx_all[None] == local_ids[:, None, None, None], axis=2)
        rank = jnp.einsum('edj,ij->edi', hit.astype(BF16), lower, preferred_element_type=F32).astype(jnp.int32)
        dev = jnp.arange(devices, dtype=jnp.int32)
        is_own = (dev % tp_size) == tp_i
        parity = jnp.arange(local_exp, dtype=jnp.int32) % 2
        base = (jnp.where(is_own, padded, 0) + (dev // tp_size) * cap)[None, :] + (parity * shift)[:, None]
        row_ids = jnp.where(hit, base[:, :, None] + rank, -1).reshape(local_exp, 1, devices * tok)

        fwd_parts = []
        start = 0
        rows_now = row_ids
        for count in FWD_CHUNKS:
            send, own = expert_fwd(start, count, half, padded, x_all, rows_now, w_gate, w_up, w_down)
            start += count
            rows_now, own = lax.optimization_barrier((rows_now, own))
            fwd_parts.append((lax.ppermute(send, 'tp', swap_tp), own))

        own0 = fwd_parts[-1][1]
        x_late, hit, rank, w_router, own0 = lax.optimization_barrier((x_all, hit, rank, w_router, own0))
        fwd_parts[-1] = (fwd_parts[-1][0], own0)

        logits_t = jnp.einsum('de,td->et', w_router, x_late, preferred_element_type=F32)
        probs_t = jax.nn.softmax(logits_t, axis=0)
        gates_local = GATE_SCALE * lax.dynamic_slice_in_dim(probs_t, ep_i * local_exp, local_exp, 0).reshape(local_exp, 1, devices * tok)

        sizes = windows(cap, ep_size)
        other, win_other, near, win_near = sizes
        per_chunk = local_exp // BWD_CHUNKS
        dev_ep = dev // tp_size
        place = jnp.zeros_like(dev)
        for k, e in enumerate(ep_order[1:]):
            place = jnp.where(dev_ep == e, k * cap, place)
        exp = jnp.arange(local_exp, dtype=jnp.int32)
        far_first = (jnp.where(is_own, win_other, 0) + place)[None, :] + ((exp % per_chunk) * other % 8)[:, None]
        near_first = jnp.where(is_own, win_near, 0)[None, :] + (2 * win_other + exp * near % 8)[:, None]
        first = jnp.where((dev_ep == ep_i)[None, :], near_first, far_first)
        bwd_ids = jnp.where(hit, first[:, :, None] + rank, -1).reshape(local_exp, 1, devices * tok)
        dy_all = ep_gather(dy_pair).reshape(devices * tok, model)
        (d_w_gate, d_w_up, d_w_down), bwd_out = expert_bwd(BWD_CHUNKS, sizes, x_all, dy_all, bwd_ids, gates_local, w_gate, w_up, w_down)
        bwd_parts = [(lax.ppermute(bwd_out[0][0], 'tp', swap_tp), bwd_out[0][1])]

        own_last = bwd_out[-1][1]
        own_first = fwd_parts[0][1]
        x, grad_y, x_all, dy_all, topk_idx, w_router, gu_part, wd_part, own_first, own_last = lax.optimization_barrier(
            (x, grad_y, x_all, dy_all, topk_idx, w_router, gu_part, wd_part, own_first, own_last))
        fwd_parts[0] = (fwd_parts[0][0], own_first)
        bwd_out[-1] = (bwd_out[-1][0], own_last)

        gu_other = ep_pieces(gu_part)
        wd_other = jnp.concatenate(ep_pieces(wd_part), axis=0)
        wg_other = jnp.concatenate([p[:, :width_q] for p in gu_other], axis=1)
        wu_other = jnp.concatenate([p[:, width_q:] for p in gu_other], axis=1)
        shared = jnp.zeros((tok, model), F32)
        dx_shared = jnp.zeros((tok, model), F32)
        for wg, wu, wd in ((ws_gate, ws_up, ws_down), (wg_other, wu_other, wd_other)):
            a = rounded(dot(x, wg))
            b = rounded(dot(x, wu))
            dh = rounded(dot(grad_y, wd, NT))
            h, da, db = swiglu_bwd(a, b, dh)
            shared = shared + dot(h, wd)
            dx_shared = dx_shared + dot(da, wg, NT) + dot(db, wu, NT)
        ds_gate, ds_up, ds_down = shared_grad(x_all, dy_all, ws_gate, ws_up, ws_down)

        def back_rows(count):
            return count * cap + (-count * cap) % 8

        def slot_index(count):
            new = jnp.arange(ep_size * back_rows(count), dtype=jnp.int32)
            block, rest = new // back_rows(count), new % back_rows(count)
            return block, rest // cap, rest % cap, rest < count * cap

        def give_back(parts, count):
            recv, own = parts
            rows = (recv + own).astype(BF16)
            src, exp, rank, valid = slot_index(count)
            old = jnp.where(valid, exp * half + src * cap + rank, -1)
            perm = (old[:, None] == jnp.arange(count * half, dtype=jnp.int32)[None, :]).astype(BF16)
            out = dot(perm, rows).astype(BF16)
            out = out.reshape(ep_size, back_rows(count), model)
            out = lax.all_to_all(out, 'ep', 0, 0)
            return out.reshape(ep_size * back_rows(count), model)

        hit_own = jnp.any(topk_idx[:, None, :] == jnp.arange(experts, dtype=jnp.int32)[None, :, None], axis=2)
        rank_own = dot(lower, hit_own.astype(BF16))
        want = jnp.where(hit_own, rank_own, -1.0).astype(BF16)
        probs = jax.nn.softmax(dot(x, w_router), axis=-1)
        prob_parts = jnp.concatenate(split3(probs), axis=0)

        def expand(start, count):
            grp, exp, rank, valid = slot_index(count)
            col = jnp.where(valid, grp * local_exp + start + exp, -1)
            table = (jnp.arange(experts, dtype=jnp.int32)[:, None] == col[None, :]).astype(BF16)
            return table, jnp.where(valid, rank, -2).astype(F32)[None, :]

        routed = jnp.zeros((tok, model), F32)
        d_scores = jnp.zeros((tok, experts), F32)
        start = 0
        for parts, count in zip(fwd_parts, FWD_CHUNKS):
            back = give_back(parts, count)
            table, rank = expand(start, count)
            hits = dot(want, table) == rank
            gates = jnp.where(jnp.concatenate([hits] * 3, axis=0), dot(prob_parts, table), 0.0).astype(BF16)
            mixed = dot(gates, back)
            routed = routed + GATE_SCALE * sum3(mixed, 0)
            score = jnp.where(hits, dot(grad_y, back, NT), 0.0)
            part = dot(jnp.concatenate(split3(score), axis=0), table, NT)
            d_scores = d_scores + sum3(part, 0)
            start += count
        y_out = (shared + routed).astype(BF16)

        d_scores = GATE_SCALE * d_scores
        mean_score = jnp.sum(probs * d_scores, axis=-1, keepdims=True)
        d_logits = probs * (d_scores - mean_score)
        d_other = lax.ppermute(d_logits, 'tp', swap_tp)
        for send, own in bwd_out[1:]:
            bwd_parts.append((lax.ppermute(send, 'tp', swap_tp), own))
        d_pair = jnp.where(tp_i == 0, jnp.stack([d_logits, d_other]), jnp.stack([d_other, d_logits]))
        d_logits_all = ep_gather(d_pair).reshape(devices * tok, experts)
        d_router = dot(x_all, jnp.concatenate(split3(d_logits_all), axis=1), TN)
        d_router = sum3(d_router, 1)
        dx_sum = dx_shared + sum3(dot(jnp.concatenate(split3(d_logits), axis=0), w_router, NT), 0)

        def hits_of(grp, start, count):
            slot = jnp.arange(count * cap, dtype=jnp.int32)
            col = grp * local_exp + start + slot // cap
            table = (jnp.arange(experts, dtype=jnp.int32)[:, None] == col[None, :]).astype(BF16)
            return (dot(want, table) == (slot % cap).astype(F32)[None, :]).astype(BF16)

        swaps = (swap_x, swap_c, [(i, core_partner(d)) for i, d in swap_x])
        for c, (recv, own) in enumerate(bwd_parts[:-1]):
            rows = (recv + own).astype(BF16)
            slot = jnp.arange(per_chunk * cap, dtype=jnp.int32)
            for k, pairs in enumerate(swaps):
                old = slot // cap * other + k * cap + slot % cap
                perm = (old[:, None] == jnp.arange(per_chunk * other, dtype=jnp.int32)[None, :]).astype(BF16)
                back = dot(perm, rows).astype(BF16)
                back = lax.ppermute(back, 'ep', pairs)
                hits = hits_of(ep_order[1 + k], c * per_chunk, per_chunk)
                dx_sum = dx_sum + dot(hits, back)
            dx_sum = lax.optimization_barrier(dx_sum)
        recv, own = bwd_parts[-1]
        dx_sum = dx_sum + dot(hits_of(ep_i, 0, local_exp), (recv + own).astype(BF16))
        return y_out, dx_sum.astype(BF16), d_router, d_w_gate, d_w_up, d_w_down, ds_gate, ds_up, ds_down

    tok_spec = P(('ep', 'tp'), None)
    in_specs = (tok_spec, tok_spec, P(None, None), P('ep', None, 'tp'), P('ep', None, 'tp'), P('ep', 'tp', None), P(None, 'tp'), P(None, 'tp'), P('tp', None), tok_spec)
    out_specs = (tok_spec, tok_spec, P(None, None), P('ep', None, 'tp'), P('ep', None, 'tp'), P('ep', 'tp', None), P(None, 'tp'), P(None, 'tp'), P('tp', None))

    return jax.shard_map(device_step, mesh=mesh, in_specs=in_specs, out_specs=out_specs, check_vma=False)
```

```python
import functools

import jax
import jax.numpy as jnp
from jax import lax
from jax.experimental import pallas as pl
from jax.experimental.pallas import tpu as pltpu
from jax.sharding import PartitionSpec as P


GATE_SCALE = 16.0
BF16 = jnp.bfloat16
F32 = jnp.float32
FWD_CHUNKS = (2, 8, 6)
BWD_CHUNKS = 2
RETURN_ORDER = (1, 0, 2)
MESH = pl.DeviceIdType.MESH

NN = (((1,), (0,)), ((), ()))
NT = (((1,), (1,)), ((), ()))
TN = (((0,), (0,)), ((), ()))


def dot(a, b, dims=NN):
    return lax.dot_general(a, b, dims, preferred_element_type=F32)


def sigmoid(v):
    return 1.0 / (1.0 + jnp.exp(-jnp.maximum(v, -88.0)))


def swiglu_fwd(a, b):
    return (a * sigmoid(a) * b).astype(BF16)


def swiglu_bwd(a, b, dh):
    sig = sigmoid(a)
    silu = a * sig
    h = (silu * b).astype(BF16)
    da = (dh * b * (sig * (1.0 + a * (1.0 - sig)))).astype(BF16)
    db = (dh * silu).astype(BF16)
    return h, da, db


def rounded(v):
    return v.astype(BF16).astype(F32)


def half_rows(cap, ep_size):
    half = cap * ep_size
    return half, half + (-half) % 8


def store_parts(parity, part, send_ref, own_ref, half, padded):
    shift = padded - half

    @pl.when(parity == 0)
    def _():
        send_ref[0:half, :] = part[0:half]
        own_ref[0:half, :] = part[padded:padded + half]

    @pl.when(parity == 1)
    def _():
        send_ref[half:2 * half, :] = part[shift:padded]
        own_ref[half:2 * half, :] = part[padded + shift:2 * padded]


def pick_matrix(row_ref, rows):
    ids = row_ref[0]
    iota = lax.broadcasted_iota(jnp.int32, (rows, ids.shape[1]), 0)
    return iota == ids


def pick_rows(pick_ref, table_ref, out_ref, scale=None, step=512):
    @pl.loop(0, table_ref.shape[1] // step)
    def _(i):
        cols = pl.ds(pl.multiple_of(i * step, step), step)
        rows = dot(pick_ref[...], table_ref[:, cols])
        out_ref[:, cols] = (rows if scale is None else rows * scale).astype(out_ref.dtype)


def fwd_kernel(half, padded, x_ref, row_ref, w1_ref, w3_ref, w2_ref, send_ref, own_ref, pick_ref, rows_ref):
    pick_ref[...] = jnp.where(pick_matrix(row_ref, 2 * padded), 1.0, 0.0).astype(BF16)
    pick_rows(pick_ref, x_ref, rows_ref)
    rows = rows_ref[...]
    a = rounded(dot(rows, w1_ref[0]))
    b = rounded(dot(rows, w3_ref[0]))
    h = swiglu_fwd(a, b)
    part = dot(h, w2_ref[0])
    store_parts(pl.program_id(0) % 2, part, send_ref, own_ref, half, padded)


def windows(cap, ep_size):
    other, own = (ep_size - 1) * cap, cap
    return other, other + 7 + (-other - 7) % 8, own, own + 7 + (-own - 7) % 8


def bwd_kernel(sizes, per_chunk, x_ref, dy_ref, row_ref, gate_ref, w1_ref, w3_ref, w2_ref, *refs):
    other, win_other, own, win_own = sizes
    dw1_ref, dw3_ref, dw2_ref = refs[:3]
    outs, (far_ref, near_ref, sem, pick_ref, rows_ref, d_out_ref) = refs[3:-6], refs[-6:]
    chunks = far_ref.shape[0] // 2
    e = pl.program_id(0)
    total = 2 * (win_other + win_own)

    @pl.when(e == 0)
    def _():
        far_ref[...] = jnp.zeros_like(far_ref)
        near_ref[...] = jnp.zeros_like(near_ref)

    hit = pick_matrix(row_ref, total)
    pick_ref[...] = jnp.where(hit, 1.0, 0.0).astype(BF16)
    gates = jnp.sum(jnp.where(hit, gate_ref[0], 0.0), axis=1, keepdims=True)
    pick_rows(pick_ref, x_ref, rows_ref)
    pick_rows(pick_ref, dy_ref, d_out_ref, gates)
    rows, d_out = rows_ref[...], d_out_ref[...]
    a = rounded(dot(rows, w1_ref[0]))
    b = rounded(dot(rows, w3_ref[0]))
    dh = rounded(dot(d_out, w2_ref[0], NT))
    h, da, db = swiglu_bwd(a, b, dh)

    chunk = e // per_chunk
    far_base = pl.multiple_of((e % per_chunk) * other // 8 * 8, 8)
    near_base = pl.multiple_of(e * own // 8 * 8, 8)
    step = 512

    @pl.loop(0, rows_ref.shape[1] // step)
    def _(i):
        cols = pl.ds(pl.multiple_of(i * step, step), step)
        dw2_ref[0, :, cols] = dot(h, d_out_ref[:, cols], TN)
        dw1_ref[0, cols, :] = dot(rows_ref[:, cols], da, TN)
        dw3_ref[0, cols, :] = dot(rows_ref[:, cols], db, TN)
        part = dot(da, w1_ref[0, cols, :], NT) + dot(db, w3_ref[0, cols, :], NT)
        for side in range(2):
            far_ref[chunk * 2 + side, pl.ds(far_base, win_other), cols] += part[side * win_other:(side + 1) * win_other]
            first = 2 * win_other + side * win_own
            near_ref[side, pl.ds(near_base, win_own), cols] += part[first:first + win_own]

    def copies(c):
        out = []
        for side in range(2):
            k = 2 * c + side
            src = far_ref.at[k] if c < chunks else near_ref.at[side]
            out.append(pltpu.make_async_copy(src.at[pl.ds(0, outs[k].shape[0])], outs[k], sem.at[k]))
        return out

    for c in range(chunks):
        @pl.when(e == (c + 1) * per_chunk - 1)
        def _():
            for copy in copies(c):
                copy.start()

    @pl.when(e == chunks * per_chunk - 1)
    def _():
        for copy in copies(chunks):
            copy.start()
        for c in range(chunks + 1):
            for copy in copies(c):
                copy.wait()


def expert_fwd(start, count, half, padded, x_all, row_ids, w_gate, w_up, w_down):
    tokens, model = x_all.shape
    width = w_gate.shape[2]
    out = jax.ShapeDtypeStruct((count * half, model), F32)
    return pl.pallas_call(
        functools.partial(fwd_kernel, half, padded),
        grid=(count,),
        in_specs=[
            pl.BlockSpec((tokens, model), lambda i: (0, 0), pipeline_mode=pl.Buffered(1)),
            pl.BlockSpec((1, 1, tokens), lambda i: (start + i, 0, 0)),
            pl.BlockSpec((1, model, width), lambda i: (start + i, 0, 0)),
            pl.BlockSpec((1, model, width), lambda i: (start + i, 0, 0)),
            pl.BlockSpec((1, width, model), lambda i: (start + i, 0, 0)),
        ],
        out_specs=[pl.BlockSpec((2 * half, model), lambda i: (i // 2, 0))] * 2,
        out_shape=[out, out],
        scratch_shapes=[pltpu.VMEM((2 * padded, tokens), BF16), pltpu.VMEM((2 * padded, model), BF16)],
        cost_estimate=pl.CostEstimate(
            flops=count * 2 * 2 * padded * model * (tokens + 3 * width),
            bytes_accessed=count * (6 * model * width + 8 * half * model) + 2 * tokens * model,
            transcendentals=count * 2 * padded * width),
        compiler_params=pltpu.CompilerParams(dimension_semantics=('arbitrary',), vmem_limit_bytes=48 << 20),
    )(x_all, row_ids, w_gate, w_up, w_down)


def expert_bwd(chunks, sizes, x_all, dy_all, row_ids, gates, w_gate, w_up, w_down):
    other, win_other, own, win_own = sizes
    tokens, model = x_all.shape
    count, _, width = w_gate.shape
    per_chunk = count // chunks
    far_rows, near_rows = per_chunk * other, count * own
    far_pad = max(j * other // 8 * 8 + win_other for j in range(per_chunk))
    near_pad = max(j * own // 8 * 8 + win_own for j in range(count))
    part_shapes = [jax.ShapeDtypeStruct((far_rows, model), F32)] * (2 * chunks) + [jax.ShapeDtypeStruct((near_rows, model), F32)] * 2
    rows = 2 * (win_other + win_own)
    outs = pl.pallas_call(
        functools.partial(bwd_kernel, sizes, per_chunk),
        grid=(count,),
        in_specs=[
            pl.BlockSpec((tokens, model), lambda i: (0, 0), pipeline_mode=pl.Buffered(1)),
            pl.BlockSpec((tokens, model), lambda i: (0, 0), pipeline_mode=pl.Buffered(1)),
            pl.BlockSpec((1, 1, tokens), lambda i: (i, 0, 0)),
            pl.BlockSpec((1, 1, tokens), lambda i: (i, 0, 0)),
            pl.BlockSpec((1, model, width), lambda i: (i, 0, 0)),
            pl.BlockSpec((1, model, width), lambda i: (i, 0, 0)),
            pl.BlockSpec((1, width, model), lambda i: (i, 0, 0)),
        ],
        out_specs=[
            pl.BlockSpec((1, model, width), lambda i: (i, 0, 0)),
            pl.BlockSpec((1, model, width), lambda i: (i, 0, 0)),
            pl.BlockSpec((1, width, model), lambda i: (i, 0, 0)),
        ] + [pl.BlockSpec(memory_space=pl.ANY)] * len(part_shapes),
        out_shape=[
            jax.ShapeDtypeStruct((count, model, width), F32),
            jax.ShapeDtypeStruct((count, model, width), F32),
            jax.ShapeDtypeStruct((count, width, model), F32),
        ] + part_shapes,
        scratch_shapes=[
            pltpu.VMEM((2 * chunks, far_pad, model), F32),
            pltpu.VMEM((2, near_pad, model), F32),
            pltpu.SemaphoreType.DMA((len(part_shapes),)),
            pltpu.VMEM((rows, tokens), BF16),
            pltpu.VMEM((rows, model), BF16),
            pltpu.VMEM((rows, model), BF16),
        ],
        cost_estimate=pl.CostEstimate(
            flops=count * 2 * rows * model * (2 * tokens + 8 * width),
            bytes_accessed=count * (18 * model * width + 4 * rows * model) + 4 * tokens * model,
            transcendentals=count * rows * width),
        compiler_params=pltpu.CompilerParams(dimension_semantics=('arbitrary',), vmem_limit_bytes=60 << 20),
        name='expert_bwd',
    )(x_all, dy_all, row_ids, gates, w_gate, w_up, w_down)
    parts = outs[3:]
    return outs[:3], [(parts[2 * c], parts[2 * c + 1]) for c in range(chunks + 1)]


def shared_grad_kernel(step, x_ref, dy_ref, wg_ref, wu_ref, wd_ref, dg_ref, du_ref, dd_ref, h_ref, da_ref, db_ref):
    tokens, model = x_ref.shape

    @pl.loop(0, tokens // step)
    def _(i):
        rows = pl.ds(pl.multiple_of(i * step, step), step)
        a = rounded(dot(x_ref[rows, :], wg_ref[...]))
        b = rounded(dot(x_ref[rows, :], wu_ref[...]))
        dh = rounded(dot(dy_ref[rows, :], wd_ref[...], NT))
        h_ref[rows, :], da_ref[rows, :], db_ref[rows, :] = swiglu_bwd(a, b, dh)

    @pl.loop(0, model // step)
    def _(i):
        cols = pl.ds(pl.multiple_of(i * step, step), step)
        dd_ref[:, cols] = dot(h_ref[...], dy_ref[:, cols], TN)
        dg_ref[cols, :] = dot(x_ref[:, cols], da_ref[...], TN)
        du_ref[cols, :] = dot(x_ref[:, cols], db_ref[...], TN)


def shared_grad(x_all, dy_all, ws_gate, ws_up, ws_down):
    tokens, model = x_all.shape
    width = ws_gate.shape[1]
    block = min(width, 256)
    full = pl.BlockSpec((tokens, model), lambda i: (0, 0), pipeline_mode=pl.Buffered(1))
    col = pl.BlockSpec((model, block), lambda i: (0, i))
    row = pl.BlockSpec((block, model), lambda i: (i, 0))
    return pl.pallas_call(
        functools.partial(shared_grad_kernel, 256),
        grid=(width // block,),
        in_specs=[full, full, col, col, row],
        out_specs=[col, col, row],
        out_shape=[jax.ShapeDtypeStruct((model, width), F32)] * 2 + [jax.ShapeDtypeStruct((width, model), F32)],
        scratch_shapes=[pltpu.VMEM((tokens, block), BF16)] * 3,
        cost_estimate=pl.CostEstimate(
            flops=12 * tokens * model * width, bytes_accessed=4 * tokens * model + 18 * model * width,
            transcendentals=tokens * width),
        compiler_params=pltpu.CompilerParams(dimension_semantics=('arbitrary',), vmem_limit_bytes=48 << 20),
        name='shared_grad',
    )(x_all, dy_all, ws_gate, ws_up, ws_down)


def split3(v):
    hi = lax.reduce_precision(v, 8, 7)
    rest = v - hi
    mid = lax.reduce_precision(rest, 8, 7)
    low = rest - mid
    return hi.astype(BF16), mid.astype(BF16), low.astype(BF16)


def sum3(v, axis):
    first, second, third = jnp.split(v, 3, axis=axis)
    return first + second + third


def core_partner(ep):
    return ep + 1 - 2 * (ep % 2)


def gather_kernel(x_ref, idx_ref, dy_ref, wg_ref, wu_ref, wd_ref, x_all, idx_all, dy_pair, wd_part, quarter, send_sem, recv_sem, idx_send, idx_recv, local_sem, x_buf, dy_buf, q_buf):
    tp = lax.axis_index('tp')
    ep = lax.axis_index('ep')
    eps = x_all.shape[0] // 2
    half = eps // 2
    tp_o = 1 - tp
    ep_x = (ep + half) % eps
    ep_c = core_partner(ep)

    def slot(e, t):
        return e * 2 + t

    others = [(tp_o, ep)]
    for k in range(1, eps):
        others += [(tp, (ep + k) % eps), (tp_o, (ep + k) % eps)]
    barrier = pltpu.get_barrier_semaphore()
    for t, e in others:
        pl.semaphore_signal(barrier, inc=1, device_id={'tp': t, 'ep': e}, device_id_type=MESH)
    pl.semaphore_wait(barrier, len(others))

    def send(k, src, dst, t, e):
        copy = pltpu.make_async_remote_copy(
            src_ref=src, dst_ref=dst, send_sem=send_sem.at[k], recv_sem=recv_sem.at[k],
            device_id={'tp': t, 'ep': e}, device_id_type=MESH)
        copy.start()
        return copy

    def block(e, t):
        return x_all.at[slot(e, t)]

    mine = block(ep, tp)
    to_y = send(0, x_ref, mine, tp_o, ep)
    to_x = send(1, x_ref, mine, tp, ep_x)
    to_c = send(2, x_ref, mine, tp, ep_c)
    own_idx = idx_all.at[slot(ep, tp)]
    idx_copies = []
    for k, (t, e) in enumerate(others):
        copy = pltpu.make_async_remote_copy(
            src_ref=idx_ref, dst_ref=own_idx, send_sem=idx_send.at[k], recv_sem=idx_recv.at[k],
            device_id={'tp': t, 'ep': e}, device_id_type=MESH)
        copy.start()
        idx_copies.append(copy)
    width = quarter.shape[1] // 2
    cols = pl.ds(pl.multiple_of(ep * width, width), width)
    load = [
        pltpu.make_async_copy(x_ref, x_buf, local_sem.at[0]),
        pltpu.make_async_copy(dy_ref, dy_buf, local_sem.at[1]),
        pltpu.make_async_copy(wg_ref.at[:, cols], q_buf.at[:, pl.ds(0, width)], local_sem.at[2]),
        pltpu.make_async_copy(wu_ref.at[:, cols], q_buf.at[:, pl.ds(width, width)], local_sem.at[3]),
    ]
    store = [
        pltpu.make_async_copy(x_buf, mine, local_sem.at[4]),
        pltpu.make_async_copy(dy_buf, dy_pair.at[tp], local_sem.at[5]),
        pltpu.make_async_copy(q_buf, quarter, local_sem.at[6]),
        pltpu.make_async_copy(idx_ref, own_idx, local_sem.at[7]),
    ]
    for copy in load:
        copy.start()
    dy_y = send(3, dy_ref, dy_pair.at[tp], tp_o, ep)
    rows = wd_part.shape[0]
    wd_y = send(4, wd_ref.at[pl.ds(ep * rows, rows)], wd_part, tp_o, ep)

    for copy in load:
        copy.wait()
    for copy in store:
        copy.start()
    to_y.wait_recv()
    y_to_x = send(5, block(ep, tp_o), block(ep, tp_o), tp, ep_x)
    y_to_c = send(6, block(ep, tp_o), block(ep, tp_o), tp, ep_c)
    to_x.wait_recv()
    x_to_c = send(7, block(ep_x, tp), block(ep_x, tp), tp, ep_c)
    y_to_x.wait_recv()
    xy_to_c = send(8, block(ep_x, tp_o), block(ep_x, tp_o), tp, ep_c)
    for copy in (to_c, dy_y, wd_y, y_to_c, x_to_c, xy_to_c):
        copy.wait_recv()
    for copy in idx_copies:
        copy.wait_recv()
    for copy in store:
        copy.wait()
    for copy in (to_y, to_x, to_c, dy_y, wd_y, y_to_x, y_to_c, x_to_c, xy_to_c):
        copy.wait_send()
    for copy in idx_copies:
        copy.wait_send()


def gather_rows(devices, ep_size, x, idx_t, dy, ws_gate, ws_up, ws_down):
    _, model = x.shape
    any_spec = pl.BlockSpec(memory_space=pl.ANY)
    return pl.pallas_call(
        gather_kernel,
        in_specs=[any_spec] * 6,
        out_specs=[any_spec] * 5,
        out_shape=[
            jax.ShapeDtypeStruct((devices,) + x.shape, x.dtype),
            jax.ShapeDtypeStruct((devices,) + idx_t.shape, idx_t.dtype),
            jax.ShapeDtypeStruct((2,) + dy.shape, dy.dtype),
            jax.ShapeDtypeStruct((ws_down.shape[0] // ep_size, model), ws_down.dtype),
            jax.ShapeDtypeStruct((model, 2 * ws_gate.shape[1] // ep_size), ws_gate.dtype),
        ],
        scratch_shapes=[
            pltpu.SemaphoreType.DMA((9,)),
            pltpu.SemaphoreType.DMA((9,)),
            pltpu.SemaphoreType.DMA((devices - 1,)),
            pltpu.SemaphoreType.DMA((devices - 1,)),
            pltpu.SemaphoreType.DMA((8,)),
            pltpu.VMEM(x.shape, x.dtype),
            pltpu.VMEM(dy.shape, dy.dtype),
            pltpu.VMEM((model, 2 * ws_gate.shape[1] // ep_size), ws_gate.dtype),
        ],
        cost_estimate=pl.CostEstimate(flops=60_000_000_000, bytes_accessed=4 * devices * x.size, transcendentals=0),
        compiler_params=pltpu.CompilerParams(collective_id=0, has_side_effects=True),
        name='gather_rows',
    )(x, idx_t, dy, ws_gate, ws_up, ws_down)


def solution(mesh):
    tp_size = mesh.shape['tp']
    ep_size = mesh.shape['ep']
    swap_tp = [(i, tp_size - 1 - i) for i in range(tp_size)]
    swap_x = [(i, (i + ep_size // 2) % ep_size) for i in range(ep_size)]
    swap_c = [(i, core_partner(i)) for i in range(ep_size)]

    def device_step(x, grad_y, w_router, w_gate, w_up, w_down, ws_gate, ws_up, ws_down, topk_idx):
        tok, model = x.shape
        top_k = topk_idx.shape[1]
        experts = w_router.shape[1]
        local_exp = w_gate.shape[0]
        groups = top_k // 2
        most = groups * tok // (2 * ep_size) + min(groups, ep_size // 2) * tok // ep_size
        cap = (2 * most + local_exp - 1) // local_exp
        half, padded = half_rows(cap, ep_size)
        shift = padded - half
        ep_i = lax.axis_index('ep')
        tp_i = lax.axis_index('tp')
        devices = ep_size * tp_size
        ep_order = (ep_i, (ep_i + ep_size // 2) % ep_size, core_partner(ep_i), core_partner((ep_i + ep_size // 2) % ep_size))

        def ep_pieces(piece):
            far = lax.ppermute(piece, 'ep', swap_x)
            return piece, far, lax.ppermute(piece, 'ep', swap_c), lax.ppermute(far, 'ep', swap_c)

        def ep_gather(piece):
            out = jnp.zeros((ep_size,) + piece.shape, piece.dtype)
            for e, part in zip(ep_order, ep_pieces(piece)):
                out = lax.dynamic_update_slice_in_dim(out, part[None], e, 0)
            return out

        x_blocks, idx_all, dy_pair, wd_part, quarter = gather_rows(devices, ep_size, x, topk_idx.T, grad_y, ws_gate, ws_up, ws_down)
        x_all = x_blocks.reshape(devices * tok, model)

        width_q = ws_gate.shape[1] // ep_size
        gu_part = lax.ppermute(quarter, 'tp', swap_tp)

        lower = (lax.broadcasted_iota(jnp.int32, (tok, tok), 0) > lax.broadcasted_iota(jnp.int32, (tok, tok), 1)).astype(BF16)
        local_ids = ep_i * local_exp + jnp.arange(local_exp, dtype=jnp.int32)
        hit = jnp.any(idx_all[None] == local_ids[:, None, None, None], axis=2)
        rank = jnp.einsum('edj,ij->edi', hit.astype(BF16), lower, preferred_element_type=F32).astype(jnp.int32)
        dev = jnp.arange(devices, dtype=jnp.int32)
        is_own = (dev % tp_size) == tp_i
        parity = jnp.arange(local_exp, dtype=jnp.int32) % 2
        base = (jnp.where(is_own, padded, 0) + (dev // tp_size) * cap)[None, :] + (parity * shift)[:, None]
        row_ids = jnp.where(hit, base[:, :, None] + rank, -1).reshape(local_exp, 1, devices * tok)

        fwd_parts = []
        start = 0
        rows_now = row_ids
        for count in FWD_CHUNKS:
            send, own = expert_fwd(start, count, half, padded, x_all, rows_now, w_gate, w_up, w_down)
            start += count
            rows_now, own = lax.optimization_barrier((rows_now, own))
            fwd_parts.append((lax.ppermute(send, 'tp', swap_tp), own))

        own0 = fwd_parts[-1][1]
        x_late, hit, rank, w_router, own0 = lax.optimization_barrier((x_all, hit, rank, w_router, own0))
        fwd_parts[-1] = (fwd_parts[-1][0], own0)

        logits_t = jnp.einsum('de,td->et', w_router, x_late, preferred_element_type=F32)
        probs_t = jax.nn.softmax(logits_t, axis=0)
        gates_local = GATE_SCALE * lax.dynamic_slice_in_dim(probs_t, ep_i * local_exp, local_exp, 0).reshape(local_exp, 1, devices * tok)

        sizes = windows(cap, ep_size)
        other, win_other, near, win_near = sizes
        per_chunk = local_exp // BWD_CHUNKS
        dev_ep = dev // tp_size
        place = jnp.zeros_like(dev)
        for k, e in enumerate(ep_order[1:]):
            place = jnp.where(dev_ep == e, k * cap, place)
        exp = jnp.arange(local_exp, dtype=jnp.int32)
        far_first = (jnp.where(is_own, win_other, 0) + place)[None, :] + ((exp % per_chunk) * other % 8)[:, None]
        near_first = jnp.where(is_own, win_near, 0)[None, :] + (2 * win_other + exp * near % 8)[:, None]
        first = jnp.where((dev_ep == ep_i)[None, :], near_first, far_first)
        bwd_ids = jnp.where(hit, first[:, :, None] + rank, -1).reshape(local_exp, 1, devices * tok)
        dy_all = ep_gather(dy_pair).reshape(devices * tok, model)
        (d_w_gate, d_w_up, d_w_down), bwd_out = expert_bwd(BWD_CHUNKS, sizes, x_all, dy_all, bwd_ids, gates_local, w_gate, w_up, w_down)
        bwd_parts = [(lax.ppermute(bwd_out[0][0], 'tp', swap_tp), bwd_out[0][1])]

        own_last = bwd_out[-1][1]
        own_first = fwd_parts[0][1]
        gu_far = lax.ppermute(gu_part, 'ep', swap_x)
        wd_far = lax.ppermute(wd_part, 'ep', swap_x)
        x, grad_y, x_all, dy_all, topk_idx, w_router, gu_part, wd_part, gu_far, wd_far, own_first, own_last = lax.optimization_barrier(
            (x, grad_y, x_all, dy_all, topk_idx, w_router, gu_part, wd_part, gu_far, wd_far, own_first, own_last))
        fwd_parts[0] = (fwd_parts[0][0], own_first)
        bwd_out[-1] = (bwd_out[-1][0], own_last)

        def back_rows(count):
            return count * cap + (-count * cap) % 8

        def slot_index(count):
            new = jnp.arange(ep_size * back_rows(count), dtype=jnp.int32)
            block, rest = new // back_rows(count), new % back_rows(count)
            return block, rest // cap, rest % cap, rest < count * cap

        def turn(parts, count):
            recv, own = parts
            rows = (recv + own).astype(BF16)
            src, exp, rank, valid = slot_index(count)
            old = jnp.where(valid, exp * half + src * cap + rank, -1)
            perm = (old[:, None] == jnp.arange(count * half, dtype=jnp.int32)[None, :]).astype(BF16)
            return dot(perm, rows).astype(BF16)

        def send_home(out, count):
            out = out.reshape(ep_size, back_rows(count), model)
            out = lax.all_to_all(out, 'ep', 0, 0)
            return out.reshape(ep_size * back_rows(count), model)

        early = RETURN_ORDER[0]
        early_rows = turn(fwd_parts[early], FWD_CHUNKS[early])
        x, grad_y, topk_idx, gu_part, wd_part, gu_far, wd_far, early_rows = lax.optimization_barrier(
            (x, grad_y, topk_idx, gu_part, wd_part, gu_far, wd_far, early_rows))
        early_back = send_home(early_rows, FWD_CHUNKS[early])

        gu_other = (gu_part, gu_far, lax.ppermute(gu_part, 'ep', swap_c), lax.ppermute(gu_far, 'ep', swap_c))
        wd_other = jnp.concatenate((wd_part, wd_far, lax.ppermute(wd_part, 'ep', swap_c), lax.ppermute(wd_far, 'ep', swap_c)), axis=0)
        wg_other = jnp.concatenate([p[:, :width_q] for p in gu_other], axis=1)
        wu_other = jnp.concatenate([p[:, width_q:] for p in gu_other], axis=1)
        shared = jnp.zeros((tok, model), F32)
        dx_shared = jnp.zeros((tok, model), F32)
        for wg, wu, wd in ((ws_gate, ws_up, ws_down), (wg_other, wu_other, wd_other)):
            a = rounded(dot(x, wg))
            b = rounded(dot(x, wu))
            dh = rounded(dot(grad_y, wd, NT))
            h, da, db = swiglu_bwd(a, b, dh)
            shared = shared + dot(h, wd)
            dx_shared = dx_shared + dot(da, wg, NT) + dot(db, wu, NT)
        ds_gate, ds_up, ds_down = shared_grad(x_all, dy_all, ws_gate, ws_up, ws_down)

        hit_own = jnp.any(topk_idx[:, None, :] == jnp.arange(experts, dtype=jnp.int32)[None, :, None], axis=2)
        rank_own = dot(lower, hit_own.astype(BF16))
        want = jnp.where(hit_own, rank_own, -1.0).astype(BF16)
        probs = jax.nn.softmax(dot(x, w_router), axis=-1)
        prob_parts = jnp.concatenate(split3(probs), axis=0)

        def expand(start, count):
            grp, exp, rank, valid = slot_index(count)
            col = jnp.where(valid, grp * local_exp + start + exp, -1)
            table = (jnp.arange(experts, dtype=jnp.int32)[:, None] == col[None, :]).astype(BF16)
            return table, jnp.where(valid, rank, -2).astype(F32)[None, :]

        routed = jnp.zeros((tok, model), F32)
        d_scores = jnp.zeros((tok, experts), F32)
        back = early_back
        for j in RETURN_ORDER:
            count, start = FWD_CHUNKS[j], sum(FWD_CHUNKS[:j])
            if j != early:
                recv, own = fwd_parts[j]
                back, own = lax.optimization_barrier((back, own))
                back = send_home(turn((recv, own), count), count)
            table, rank = expand(start, count)
            hits = dot(want, table) == rank
            gates = jnp.where(jnp.concatenate([hits] * 3, axis=0), dot(prob_parts, table), 0.0).astype(BF16)
            mixed = dot(gates, back)
            routed = routed + GATE_SCALE * sum3(mixed, 0)
            score = jnp.where(hits, dot(grad_y, back, NT), 0.0)
            part = dot(jnp.concatenate(split3(score), axis=0), table, NT)
            d_scores = d_scores + sum3(part, 0)
        y_out = (shared + routed).astype(BF16)

        d_scores = GATE_SCALE * d_scores
        mean_score = jnp.sum(probs * d_scores, axis=-1, keepdims=True)
        d_logits = probs * (d_scores - mean_score)
        d_other = lax.ppermute(d_logits, 'tp', swap_tp)
        for send, own in bwd_out[1:]:
            bwd_parts.append((lax.ppermute(send, 'tp', swap_tp), own))
        d_pair = jnp.where(tp_i == 0, jnp.stack([d_logits, d_other]), jnp.stack([d_other, d_logits]))
        d_logits_all = ep_gather(d_pair).reshape(devices * tok, experts)
        d_router = dot(x_all, jnp.concatenate(split3(d_logits_all), axis=1), TN)
        d_router = sum3(d_router, 1)
        dx_sum = dx_shared + sum3(dot(jnp.concatenate(split3(d_logits), axis=0), w_router, NT), 0)

        def hits_of(grp, start, count):
            slot = jnp.arange(count * cap, dtype=jnp.int32)
            col = grp * local_exp + start + slot // cap
            table = (jnp.arange(experts, dtype=jnp.int32)[:, None] == col[None, :]).astype(BF16)
            return (dot(want, table) == (slot % cap).astype(F32)[None, :]).astype(BF16)

        swaps = (swap_x, swap_c, [(i, core_partner(d)) for i, d in swap_x])
        for c, (recv, own) in enumerate(bwd_parts[:-1]):
            rows = (recv + own).astype(BF16)
            slot = jnp.arange(per_chunk * cap, dtype=jnp.int32)
            for k, pairs in enumerate(swaps):
                old = slot // cap * other + k * cap + slot % cap
                perm = (old[:, None] == jnp.arange(per_chunk * other, dtype=jnp.int32)[None, :]).astype(BF16)
                back = dot(perm, rows).astype(BF16)
                back = lax.ppermute(back, 'ep', pairs)
                hits = hits_of(ep_order[1 + k], c * per_chunk, per_chunk)
                dx_sum = dx_sum + dot(hits, back)
            dx_sum = lax.optimization_barrier(dx_sum)
        recv, own = bwd_parts[-1]
        dx_sum = dx_sum + dot(hits_of(ep_i, 0, local_exp), (recv + own).astype(BF16))
        return y_out, dx_sum.astype(BF16), d_router, d_w_gate, d_w_up, d_w_down, ds_gate, ds_up, ds_down

    tok_spec = P(('ep', 'tp'), None)
    in_specs = (tok_spec, tok_spec, P(None, None), P('ep', None, 'tp'), P('ep', None, 'tp'), P('ep', 'tp', None), P(None, 'tp'), P(None, 'tp'), P('tp', None), tok_spec)
    out_specs = (tok_spec, tok_spec, P(None, None), P('ep', None, 'tp'), P('ep', None, 'tp'), P('ep', 'tp', None), P(None, 'tp'), P(None, 'tp'), P('tp', None))

    return jax.shard_map(device_step, mesh=mesh, in_specs=in_specs, out_specs=out_specs, check_vma=False)
```

```python
import functools

import jax
import jax.numpy as jnp
from jax import lax
from jax.experimental import pallas as pl
from jax.experimental.pallas import tpu as pltpu
from jax.sharding import PartitionSpec as P


GATE_SCALE = 16.0
BF16 = jnp.bfloat16
F32 = jnp.float32
FWD_CHUNKS = (2, 8, 6)
BWD_CHUNKS = 2
RETURN_ORDER = (1, 0, 2)
MESH = pl.DeviceIdType.MESH

NN = (((1,), (0,)), ((), ()))
NT = (((1,), (1,)), ((), ()))
TN = (((0,), (0,)), ((), ()))


def dot(a, b, dims=NN):
    return lax.dot_general(a, b, dims, preferred_element_type=F32)


def sigmoid(v):
    return 1.0 / (1.0 + jnp.exp(-jnp.maximum(v, -88.0)))


def swiglu_fwd(a, b):
    return (a * sigmoid(a) * b).astype(BF16)


def swiglu_bwd(a, b, dh):
    sig = sigmoid(a)
    silu = a * sig
    h = (silu * b).astype(BF16)
    da = (dh * b * (sig * (1.0 + a * (1.0 - sig)))).astype(BF16)
    db = (dh * silu).astype(BF16)
    return h, da, db


def rounded(v):
    return v.astype(BF16).astype(F32)


def half_rows(cap, ep_size):
    half = cap * ep_size
    return half, half + (-half) % 8


def store_parts(parity, part, send_ref, own_ref, half, padded):
    shift = padded - half

    @pl.when(parity == 0)
    def _():
        send_ref[0:half, :] = part[0:half]
        own_ref[0:half, :] = part[padded:padded + half]

    @pl.when(parity == 1)
    def _():
        send_ref[half:2 * half, :] = part[shift:padded]
        own_ref[half:2 * half, :] = part[padded + shift:2 * padded]


def pick_matrix(row_ref, rows):
    ids = row_ref[0]
    iota = lax.broadcasted_iota(jnp.int32, (rows, ids.shape[1]), 0)
    return iota == ids


def pick_rows(pick_ref, table_ref, out_ref, scale=None, step=512):
    @pl.loop(0, table_ref.shape[1] // step)
    def _(i):
        cols = pl.ds(pl.multiple_of(i * step, step), step)
        rows = dot(pick_ref[...], table_ref[:, cols])
        out_ref[:, cols] = (rows if scale is None else rows * scale).astype(out_ref.dtype)


def fwd_kernel(half, padded, x_ref, row_ref, w1_ref, w3_ref, w2_ref, send_ref, own_ref, pick_ref, rows_ref):
    pick_ref[...] = jnp.where(pick_matrix(row_ref, 2 * padded), 1.0, 0.0).astype(BF16)
    pick_rows(pick_ref, x_ref, rows_ref)
    rows = rows_ref[...]
    a = rounded(dot(rows, w1_ref[0]))
    b = rounded(dot(rows, w3_ref[0]))
    h = swiglu_fwd(a, b)
    part = dot(h, w2_ref[0])
    store_parts(pl.program_id(0) % 2, part, send_ref, own_ref, half, padded)


def windows(cap, ep_size):
    other, own = (ep_size - 1) * cap, cap
    return other, other + 7 + (-other - 7) % 8, own, own + 7 + (-own - 7) % 8


def bwd_kernel(sizes, per_chunk, x_ref, dy_ref, row_ref, gate_ref, w1_ref, w3_ref, w2_ref, *refs):
    other, win_other, own, win_own = sizes
    dw1_ref, dw3_ref, dw2_ref = refs[:3]
    outs, (far_ref, near_ref, sem, pick_ref, rows_ref, d_out_ref) = refs[3:-6], refs[-6:]
    chunks = far_ref.shape[0] // 2
    e = pl.program_id(0)
    total = 2 * (win_other + win_own)

    @pl.when(e == 0)
    def _():
        far_ref[...] = jnp.zeros_like(far_ref)
        near_ref[...] = jnp.zeros_like(near_ref)

    hit = pick_matrix(row_ref, total)
    pick_ref[...] = jnp.where(hit, 1.0, 0.0).astype(BF16)
    gates = jnp.sum(jnp.where(hit, gate_ref[0], 0.0), axis=1, keepdims=True)
    pick_rows(pick_ref, x_ref, rows_ref)
    pick_rows(pick_ref, dy_ref, d_out_ref, gates)
    rows, d_out = rows_ref[...], d_out_ref[...]
    a = rounded(dot(rows, w1_ref[0]))
    b = rounded(dot(rows, w3_ref[0]))
    dh = rounded(dot(d_out, w2_ref[0], NT))
    h, da, db = swiglu_bwd(a, b, dh)

    chunk = e // per_chunk
    far_base = pl.multiple_of((e % per_chunk) * other // 8 * 8, 8)
    near_base = pl.multiple_of(e * own // 8 * 8, 8)
    step = 512

    @pl.loop(0, rows_ref.shape[1] // step)
    def _(i):
        cols = pl.ds(pl.multiple_of(i * step, step), step)
        dw2_ref[0, :, cols] = dot(h, d_out_ref[:, cols], TN)
        dw1_ref[0, cols, :] = dot(rows_ref[:, cols], da, TN)
        dw3_ref[0, cols, :] = dot(rows_ref[:, cols], db, TN)
        part = dot(da, w1_ref[0, cols, :], NT) + dot(db, w3_ref[0, cols, :], NT)
        for side in range(2):
            far_ref[chunk * 2 + side, pl.ds(far_base, win_other), cols] += part[side * win_other:(side + 1) * win_other]
            first = 2 * win_other + side * win_own
            near_ref[side, pl.ds(near_base, win_own), cols] += part[first:first + win_own]

    def copies(c):
        out = []
        for side in range(2):
            k = 2 * c + side
            src = far_ref.at[k] if c < chunks else near_ref.at[side]
            out.append(pltpu.make_async_copy(src.at[pl.ds(0, outs[k].shape[0])], outs[k], sem.at[k]))
        return out

    for c in range(chunks):
        @pl.when(e == (c + 1) * per_chunk - 1)
        def _():
            for copy in copies(c):
                copy.start()

    @pl.when(e == chunks * per_chunk - 1)
    def _():
        for copy in copies(chunks):
            copy.start()
        for c in range(chunks + 1):
            for copy in copies(c):
                copy.wait()


def expert_fwd(start, count, half, padded, x_all, row_ids, w_gate, w_up, w_down):
    tokens, model = x_all.shape
    width = w_gate.shape[2]
    out = jax.ShapeDtypeStruct((count * half, model), F32)
    return pl.pallas_call(
        functools.partial(fwd_kernel, half, padded),
        grid=(count,),
        in_specs=[
            pl.BlockSpec((tokens, model), lambda i: (0, 0), pipeline_mode=pl.Buffered(1)),
            pl.BlockSpec((1, 1, tokens), lambda i: (start + i, 0, 0)),
            pl.BlockSpec((1, model, width), lambda i: (start + i, 0, 0)),
            pl.BlockSpec((1, model, width), lambda i: (start + i, 0, 0)),
            pl.BlockSpec((1, width, model), lambda i: (start + i, 0, 0)),
        ],
        out_specs=[pl.BlockSpec((2 * half, model), lambda i: (i // 2, 0))] * 2,
        out_shape=[out, out],
        scratch_shapes=[pltpu.VMEM((2 * padded, tokens), BF16), pltpu.VMEM((2 * padded, model), BF16)],
        cost_estimate=pl.CostEstimate(
            flops=count * 2 * 2 * padded * model * (tokens + 3 * width),
            bytes_accessed=count * (6 * model * width + 8 * half * model) + 2 * tokens * model,
            transcendentals=count * 2 * padded * width),
        compiler_params=pltpu.CompilerParams(dimension_semantics=('arbitrary',), vmem_limit_bytes=48 << 20),
    )(x_all, row_ids, w_gate, w_up, w_down)


def expert_bwd(chunks, sizes, x_all, dy_all, row_ids, gates, w_gate, w_up, w_down):
    other, win_other, own, win_own = sizes
    tokens, model = x_all.shape
    count, _, width = w_gate.shape
    per_chunk = count // chunks
    far_rows, near_rows = per_chunk * other, count * own
    far_pad = max(j * other // 8 * 8 + win_other for j in range(per_chunk))
    near_pad = max(j * own // 8 * 8 + win_own for j in range(count))
    part_shapes = [jax.ShapeDtypeStruct((far_rows, model), F32)] * (2 * chunks) + [jax.ShapeDtypeStruct((near_rows, model), F32)] * 2
    rows = 2 * (win_other + win_own)
    outs = pl.pallas_call(
        functools.partial(bwd_kernel, sizes, per_chunk),
        grid=(count,),
        in_specs=[
            pl.BlockSpec((tokens, model), lambda i: (0, 0), pipeline_mode=pl.Buffered(1)),
            pl.BlockSpec((tokens, model), lambda i: (0, 0), pipeline_mode=pl.Buffered(1)),
            pl.BlockSpec((1, 1, tokens), lambda i: (i, 0, 0)),
            pl.BlockSpec((1, 1, tokens), lambda i: (i, 0, 0)),
            pl.BlockSpec((1, model, width), lambda i: (i, 0, 0)),
            pl.BlockSpec((1, model, width), lambda i: (i, 0, 0)),
            pl.BlockSpec((1, width, model), lambda i: (i, 0, 0)),
        ],
        out_specs=[
            pl.BlockSpec((1, model, width), lambda i: (i, 0, 0)),
            pl.BlockSpec((1, model, width), lambda i: (i, 0, 0)),
            pl.BlockSpec((1, width, model), lambda i: (i, 0, 0)),
        ] + [pl.BlockSpec(memory_space=pl.ANY)] * len(part_shapes),
        out_shape=[
            jax.ShapeDtypeStruct((count, model, width), F32),
            jax.ShapeDtypeStruct((count, model, width), F32),
            jax.ShapeDtypeStruct((count, width, model), F32),
        ] + part_shapes,
        scratch_shapes=[
            pltpu.VMEM((2 * chunks, far_pad, model), F32),
            pltpu.VMEM((2, near_pad, model), F32),
            pltpu.SemaphoreType.DMA((len(part_shapes),)),
            pltpu.VMEM((rows, tokens), BF16),
            pltpu.VMEM((rows, model), BF16),
            pltpu.VMEM((rows, model), BF16),
        ],
        cost_estimate=pl.CostEstimate(
            flops=count * 2 * rows * model * (2 * tokens + 8 * width),
            bytes_accessed=count * (18 * model * width + 4 * rows * model) + 4 * tokens * model,
            transcendentals=count * rows * width),
        compiler_params=pltpu.CompilerParams(dimension_semantics=('arbitrary',), vmem_limit_bytes=60 << 20),
        name='expert_bwd',
    )(x_all, dy_all, row_ids, gates, w_gate, w_up, w_down)
    parts = outs[3:]
    return outs[:3], [(parts[2 * c], parts[2 * c + 1]) for c in range(chunks + 1)]


def shared_grad_kernel(step, x_ref, dy_ref, wg_ref, wu_ref, wd_ref, dg_ref, du_ref, dd_ref, h_ref, da_ref, db_ref):
    tokens, model = x_ref.shape

    @pl.loop(0, tokens // step)
    def _(i):
        rows = pl.ds(pl.multiple_of(i * step, step), step)
        a = rounded(dot(x_ref[rows, :], wg_ref[...]))
        b = rounded(dot(x_ref[rows, :], wu_ref[...]))
        dh = rounded(dot(dy_ref[rows, :], wd_ref[...], NT))
        h_ref[rows, :], da_ref[rows, :], db_ref[rows, :] = swiglu_bwd(a, b, dh)

    @pl.loop(0, model // step)
    def _(i):
        cols = pl.ds(pl.multiple_of(i * step, step), step)
        dd_ref[:, cols] = dot(h_ref[...], dy_ref[:, cols], TN)
        dg_ref[cols, :] = dot(x_ref[:, cols], da_ref[...], TN)
        du_ref[cols, :] = dot(x_ref[:, cols], db_ref[...], TN)


def shared_grad(x_all, dy_all, ws_gate, ws_up, ws_down):
    tokens, model = x_all.shape
    width = ws_gate.shape[1]
    block = min(width, 256)
    full = pl.BlockSpec((tokens, model), lambda i: (0, 0), pipeline_mode=pl.Buffered(1))
    col = pl.BlockSpec((model, block), lambda i: (0, i))
    row = pl.BlockSpec((block, model), lambda i: (i, 0))
    return pl.pallas_call(
        functools.partial(shared_grad_kernel, 256),
        grid=(width // block,),
        in_specs=[full, full, col, col, row],
        out_specs=[col, col, row],
        out_shape=[jax.ShapeDtypeStruct((model, width), F32)] * 2 + [jax.ShapeDtypeStruct((width, model), F32)],
        scratch_shapes=[pltpu.VMEM((tokens, block), BF16)] * 3,
        cost_estimate=pl.CostEstimate(
            flops=12 * tokens * model * width, bytes_accessed=4 * tokens * model + 18 * model * width,
            transcendentals=tokens * width),
        compiler_params=pltpu.CompilerParams(dimension_semantics=('arbitrary',), vmem_limit_bytes=48 << 20),
        name='shared_grad',
    )(x_all, dy_all, ws_gate, ws_up, ws_down)


def last_join_kernel(hits_ref, recv_ref, own_ref, sum_ref, out_ref):
    rows = (recv_ref[...] + own_ref[...]).astype(BF16)
    out_ref[...] = (sum_ref[...] + dot(hits_ref[...], rows)).astype(out_ref.dtype)


def last_join(hits, recv, own, dx_sum, block=256):
    tok, slots = hits.shape
    model = recv.shape[1]
    part = pl.BlockSpec((slots, block), lambda i: (0, i))
    token = pl.BlockSpec((tok, block), lambda i: (0, i))
    return pl.pallas_call(
        last_join_kernel,
        grid=(model // block,),
        in_specs=[pl.BlockSpec((tok, slots), lambda i: (0, 0)), part, part, token],
        out_specs=token,
        out_shape=jax.ShapeDtypeStruct((tok, model), BF16),
        cost_estimate=pl.CostEstimate(
            flops=2 * tok * slots * model, bytes_accessed=8 * slots * model + 6 * tok * model, transcendentals=0),
        compiler_params=pltpu.CompilerParams(dimension_semantics=('arbitrary',)),
        name='last_join',
    )(hits, recv, own, dx_sum)


def split3(v):
    hi = lax.reduce_precision(v, 8, 7)
    rest = v - hi
    mid = lax.reduce_precision(rest, 8, 7)
    low = rest - mid
    return hi.astype(BF16), mid.astype(BF16), low.astype(BF16)


def sum3(v, axis):
    first, second, third = jnp.split(v, 3, axis=axis)
    return first + second + third


def core_partner(ep):
    return ep + 1 - 2 * (ep % 2)


def gather_kernel(x_ref, idx_ref, dy_ref, wg_ref, wu_ref, wd_ref, x_all, idx_all, dy_pair, wd_part, quarter, send_sem, recv_sem, idx_send, idx_recv, local_sem, x_buf, dy_buf, q_buf):
    tp = lax.axis_index('tp')
    ep = lax.axis_index('ep')
    eps = x_all.shape[0] // 2
    half = eps // 2
    tp_o = 1 - tp
    ep_x = (ep + half) % eps
    ep_c = core_partner(ep)

    def slot(e, t):
        return e * 2 + t

    others = [(tp_o, ep)]
    for k in range(1, eps):
        others += [(tp, (ep + k) % eps), (tp_o, (ep + k) % eps)]
    barrier = pltpu.get_barrier_semaphore()
    for t, e in others:
        pl.semaphore_signal(barrier, inc=1, device_id={'tp': t, 'ep': e}, device_id_type=MESH)
    pl.semaphore_wait(barrier, len(others))

    def send(k, src, dst, t, e):
        copy = pltpu.make_async_remote_copy(
            src_ref=src, dst_ref=dst, send_sem=send_sem.at[k], recv_sem=recv_sem.at[k],
            device_id={'tp': t, 'ep': e}, device_id_type=MESH)
        copy.start()
        return copy

    def block(e, t):
        return x_all.at[slot(e, t)]

    mine = block(ep, tp)
    to_y = send(0, x_ref, mine, tp_o, ep)
    to_x = send(1, x_ref, mine, tp, ep_x)
    to_c = send(2, x_ref, mine, tp, ep_c)
    own_idx = idx_all.at[slot(ep, tp)]
    idx_copies = []
    for k, (t, e) in enumerate(others):
        copy = pltpu.make_async_remote_copy(
            src_ref=idx_ref, dst_ref=own_idx, send_sem=idx_send.at[k], recv_sem=idx_recv.at[k],
            device_id={'tp': t, 'ep': e}, device_id_type=MESH)
        copy.start()
        idx_copies.append(copy)
    width = quarter.shape[1] // 2
    cols = pl.ds(pl.multiple_of(ep * width, width), width)
    load = [
        pltpu.make_async_copy(x_ref, x_buf, local_sem.at[0]),
        pltpu.make_async_copy(dy_ref, dy_buf, local_sem.at[1]),
        pltpu.make_async_copy(wg_ref.at[:, cols], q_buf.at[:, pl.ds(0, width)], local_sem.at[2]),
        pltpu.make_async_copy(wu_ref.at[:, cols], q_buf.at[:, pl.ds(width, width)], local_sem.at[3]),
    ]
    store = [
        pltpu.make_async_copy(x_buf, mine, local_sem.at[4]),
        pltpu.make_async_copy(dy_buf, dy_pair.at[tp], local_sem.at[5]),
        pltpu.make_async_copy(q_buf, quarter, local_sem.at[6]),
        pltpu.make_async_copy(idx_ref, own_idx, local_sem.at[7]),
    ]
    for copy in load:
        copy.start()
    dy_y = send(3, dy_ref, dy_pair.at[tp], tp_o, ep)
    rows = wd_part.shape[0]
    wd_y = send(4, wd_ref.at[pl.ds(ep * rows, rows)], wd_part, tp_o, ep)

    for copy in load:
        copy.wait()
    for copy in store:
        copy.start()
    to_y.wait_recv()
    y_to_x = send(5, block(ep, tp_o), block(ep, tp_o), tp, ep_x)
    y_to_c = send(6, block(ep, tp_o), block(ep, tp_o), tp, ep_c)
    to_x.wait_recv()
    x_to_c = send(7, block(ep_x, tp), block(ep_x, tp), tp, ep_c)
    y_to_x.wait_recv()
    xy_to_c = send(8, block(ep_x, tp_o), block(ep_x, tp_o), tp, ep_c)
    for copy in (to_c, dy_y, wd_y, y_to_c, x_to_c, xy_to_c):
        copy.wait_recv()
    for copy in idx_copies:
        copy.wait_recv()
    for copy in store:
        copy.wait()
    for copy in (to_y, to_x, to_c, dy_y, wd_y, y_to_x, y_to_c, x_to_c, xy_to_c):
        copy.wait_send()
    for copy in idx_copies:
        copy.wait_send()


def gather_rows(devices, ep_size, x, idx_t, dy, ws_gate, ws_up, ws_down):
    _, model = x.shape
    any_spec = pl.BlockSpec(memory_space=pl.ANY)
    return pl.pallas_call(
        gather_kernel,
        in_specs=[any_spec] * 6,
        out_specs=[any_spec] * 5,
        out_shape=[
            jax.ShapeDtypeStruct((devices,) + x.shape, x.dtype),
            jax.ShapeDtypeStruct((devices,) + idx_t.shape, idx_t.dtype),
            jax.ShapeDtypeStruct((2,) + dy.shape, dy.dtype),
            jax.ShapeDtypeStruct((ws_down.shape[0] // ep_size, model), ws_down.dtype),
            jax.ShapeDtypeStruct((model, 2 * ws_gate.shape[1] // ep_size), ws_gate.dtype),
        ],
        scratch_shapes=[
            pltpu.SemaphoreType.DMA((9,)),
            pltpu.SemaphoreType.DMA((9,)),
            pltpu.SemaphoreType.DMA((devices - 1,)),
            pltpu.SemaphoreType.DMA((devices - 1,)),
            pltpu.SemaphoreType.DMA((8,)),
            pltpu.VMEM(x.shape, x.dtype),
            pltpu.VMEM(dy.shape, dy.dtype),
            pltpu.VMEM((model, 2 * ws_gate.shape[1] // ep_size), ws_gate.dtype),
        ],
        cost_estimate=pl.CostEstimate(flops=60_000_000_000, bytes_accessed=4 * devices * x.size, transcendentals=0),
        compiler_params=pltpu.CompilerParams(collective_id=0, has_side_effects=True),
        name='gather_rows',
    )(x, idx_t, dy, ws_gate, ws_up, ws_down)


def solution(mesh):
    tp_size = mesh.shape['tp']
    ep_size = mesh.shape['ep']
    swap_tp = [(i, tp_size - 1 - i) for i in range(tp_size)]
    swap_x = [(i, (i + ep_size // 2) % ep_size) for i in range(ep_size)]
    swap_c = [(i, core_partner(i)) for i in range(ep_size)]

    def device_step(x, grad_y, w_router, w_gate, w_up, w_down, ws_gate, ws_up, ws_down, topk_idx):
        tok, model = x.shape
        top_k = topk_idx.shape[1]
        experts = w_router.shape[1]
        local_exp = w_gate.shape[0]
        groups = top_k // 2
        most = groups * tok // (2 * ep_size) + min(groups, ep_size // 2) * tok // ep_size
        cap = (2 * most + local_exp - 1) // local_exp
        half, padded = half_rows(cap, ep_size)
        shift = padded - half
        ep_i = lax.axis_index('ep')
        tp_i = lax.axis_index('tp')
        devices = ep_size * tp_size
        ep_order = (ep_i, (ep_i + ep_size // 2) % ep_size, core_partner(ep_i), core_partner((ep_i + ep_size // 2) % ep_size))

        def ep_pieces(piece):
            far = lax.ppermute(piece, 'ep', swap_x)
            return piece, far, lax.ppermute(piece, 'ep', swap_c), lax.ppermute(far, 'ep', swap_c)

        def ep_gather(piece):
            out = jnp.zeros((ep_size,) + piece.shape, piece.dtype)
            for e, part in zip(ep_order, ep_pieces(piece)):
                out = lax.dynamic_update_slice_in_dim(out, part[None], e, 0)
            return out

        x_blocks, idx_all, dy_pair, wd_part, quarter = gather_rows(devices, ep_size, x, topk_idx.T, grad_y, ws_gate, ws_up, ws_down)
        x_all = x_blocks.reshape(devices * tok, model)

        width_q = ws_gate.shape[1] // ep_size
        gu_part = lax.ppermute(quarter, 'tp', swap_tp)

        lower = (lax.broadcasted_iota(jnp.int32, (tok, tok), 0) > lax.broadcasted_iota(jnp.int32, (tok, tok), 1)).astype(BF16)
        local_ids = ep_i * local_exp + jnp.arange(local_exp, dtype=jnp.int32)
        hit = jnp.any(idx_all[None] == local_ids[:, None, None, None], axis=2)
        rank = jnp.einsum('edj,ij->edi', hit.astype(BF16), lower, preferred_element_type=F32).astype(jnp.int32)
        dev = jnp.arange(devices, dtype=jnp.int32)
        is_own = (dev % tp_size) == tp_i
        parity = jnp.arange(local_exp, dtype=jnp.int32) % 2
        base = (jnp.where(is_own, padded, 0) + (dev // tp_size) * cap)[None, :] + (parity * shift)[:, None]
        row_ids = jnp.where(hit, base[:, :, None] + rank, -1).reshape(local_exp, 1, devices * tok)

        fwd_parts = []
        start = 0
        rows_now = row_ids
        for count in FWD_CHUNKS:
            send, own = expert_fwd(start, count, half, padded, x_all, rows_now, w_gate, w_up, w_down)
            start += count
            rows_now, own = lax.optimization_barrier((rows_now, own))
            fwd_parts.append((lax.ppermute(send, 'tp', swap_tp), own))

        own0 = fwd_parts[-1][1]
        x_late, hit, rank, w_router, own0 = lax.optimization_barrier((x_all, hit, rank, w_router, own0))
        fwd_parts[-1] = (fwd_parts[-1][0], own0)

        logits_t = jnp.einsum('de,td->et', w_router, x_late, preferred_element_type=F32)
        probs_t = jax.nn.softmax(logits_t, axis=0)
        gates_local = GATE_SCALE * lax.dynamic_slice_in_dim(probs_t, ep_i * local_exp, local_exp, 0).reshape(local_exp, 1, devices * tok)

        sizes = windows(cap, ep_size)
        other, win_other, near, win_near = sizes
        per_chunk = local_exp // BWD_CHUNKS
        dev_ep = dev // tp_size
        place = jnp.zeros_like(dev)
        for k, e in enumerate(ep_order[1:]):
            place = jnp.where(dev_ep == e, k * cap, place)
        exp = jnp.arange(local_exp, dtype=jnp.int32)
        far_first = (jnp.where(is_own, win_other, 0) + place)[None, :] + ((exp % per_chunk) * other % 8)[:, None]
        near_first = jnp.where(is_own, win_near, 0)[None, :] + (2 * win_other + exp * near % 8)[:, None]
        first = jnp.where((dev_ep == ep_i)[None, :], near_first, far_first)
        bwd_ids = jnp.where(hit, first[:, :, None] + rank, -1).reshape(local_exp, 1, devices * tok)
        dy_all = ep_gather(dy_pair).reshape(devices * tok, model)
        (d_w_gate, d_w_up, d_w_down), bwd_out = expert_bwd(BWD_CHUNKS, sizes, x_all, dy_all, bwd_ids, gates_local, w_gate, w_up, w_down)
        bwd_parts = [(lax.ppermute(bwd_out[0][0], 'tp', swap_tp), bwd_out[0][1])]

        own_last = bwd_out[-1][1]
        own_first = fwd_parts[0][1]
        gu_far = lax.ppermute(gu_part, 'ep', swap_x)
        wd_far = lax.ppermute(wd_part, 'ep', swap_x)
        x, grad_y, x_all, dy_all, topk_idx, w_router, gu_part, wd_part, gu_far, wd_far, own_first, own_last = lax.optimization_barrier(
            (x, grad_y, x_all, dy_all, topk_idx, w_router, gu_part, wd_part, gu_far, wd_far, own_first, own_last))
        fwd_parts[0] = (fwd_parts[0][0], own_first)
        bwd_out[-1] = (bwd_out[-1][0], own_last)

        def back_rows(count):
            return count * cap + (-count * cap) % 8

        def slot_index(count):
            new = jnp.arange(ep_size * back_rows(count), dtype=jnp.int32)
            block, rest = new // back_rows(count), new % back_rows(count)
            return block, rest // cap, rest % cap, rest < count * cap

        def turn(parts, count):
            recv, own = parts
            rows = (recv + own).astype(BF16)
            src, exp, rank, valid = slot_index(count)
            old = jnp.where(valid, exp * half + src * cap + rank, -1)
            perm = (old[:, None] == jnp.arange(count * half, dtype=jnp.int32)[None, :]).astype(BF16)
            return dot(perm, rows).astype(BF16)

        def send_home(out, count):
            out = out.reshape(ep_size, back_rows(count), model)
            out = lax.all_to_all(out, 'ep', 0, 0)
            return out.reshape(ep_size * back_rows(count), model)

        early = RETURN_ORDER[0]
        early_rows = turn(fwd_parts[early], FWD_CHUNKS[early])
        x, grad_y, topk_idx, gu_part, wd_part, gu_far, wd_far, early_rows = lax.optimization_barrier(
            (x, grad_y, topk_idx, gu_part, wd_part, gu_far, wd_far, early_rows))
        early_back = send_home(early_rows, FWD_CHUNKS[early])

        gu_other = (gu_part, gu_far, lax.ppermute(gu_part, 'ep', swap_c), lax.ppermute(gu_far, 'ep', swap_c))
        wd_other = jnp.concatenate((wd_part, wd_far, lax.ppermute(wd_part, 'ep', swap_c), lax.ppermute(wd_far, 'ep', swap_c)), axis=0)
        wg_other = jnp.concatenate([p[:, :width_q] for p in gu_other], axis=1)
        wu_other = jnp.concatenate([p[:, width_q:] for p in gu_other], axis=1)
        shared = jnp.zeros((tok, model), F32)
        dx_shared = jnp.zeros((tok, model), F32)
        for wg, wu, wd in ((ws_gate, ws_up, ws_down), (wg_other, wu_other, wd_other)):
            a = rounded(dot(x, wg))
            b = rounded(dot(x, wu))
            dh = rounded(dot(grad_y, wd, NT))
            h, da, db = swiglu_bwd(a, b, dh)
            shared = shared + dot(h, wd)
            dx_shared = dx_shared + dot(da, wg, NT) + dot(db, wu, NT)
        ds_gate, ds_up, ds_down = shared_grad(x_all, dy_all, ws_gate, ws_up, ws_down)

        hit_own = jnp.any(topk_idx[:, None, :] == jnp.arange(experts, dtype=jnp.int32)[None, :, None], axis=2)
        rank_own = dot(lower, hit_own.astype(BF16))
        want = jnp.where(hit_own, rank_own, -1.0).astype(BF16)
        probs = jax.nn.softmax(dot(x, w_router), axis=-1)
        prob_parts = jnp.concatenate(split3(probs), axis=0)

        def expand(start, count):
            grp, exp, rank, valid = slot_index(count)
            col = jnp.where(valid, grp * local_exp + start + exp, -1)
            table = (jnp.arange(experts, dtype=jnp.int32)[:, None] == col[None, :]).astype(BF16)
            return table, jnp.where(valid, rank, -2).astype(F32)[None, :]

        routed = jnp.zeros((tok, model), F32)
        d_scores = jnp.zeros((tok, experts), F32)
        back = early_back
        for j in RETURN_ORDER:
            count, start = FWD_CHUNKS[j], sum(FWD_CHUNKS[:j])
            if j != early:
                recv, own = fwd_parts[j]
                back, own = lax.optimization_barrier((back, own))
                back = send_home(turn((recv, own), count), count)
            table, rank = expand(start, count)
            hits = dot(want, table) == rank
            gates = jnp.where(jnp.concatenate([hits] * 3, axis=0), dot(prob_parts, table), 0.0).astype(BF16)
            mixed = dot(gates, back)
            routed = routed + GATE_SCALE * sum3(mixed, 0)
            score = jnp.where(hits, dot(grad_y, back, NT), 0.0)
            part = dot(jnp.concatenate(split3(score), axis=0), table, NT)
            d_scores = d_scores + sum3(part, 0)
        y_out = (shared + routed).astype(BF16)

        d_scores = GATE_SCALE * d_scores
        mean_score = jnp.sum(probs * d_scores, axis=-1, keepdims=True)
        d_logits = probs * (d_scores - mean_score)
        d_other = lax.ppermute(d_logits, 'tp', swap_tp)
        for send, own in bwd_out[1:]:
            bwd_parts.append((lax.ppermute(send, 'tp', swap_tp), own))
        d_pair = jnp.where(tp_i == 0, jnp.stack([d_logits, d_other]), jnp.stack([d_other, d_logits]))
        d_logits_all = ep_gather(d_pair).reshape(devices * tok, experts)
        d_router = dot(x_all, jnp.concatenate(split3(d_logits_all), axis=1), TN)
        d_router = sum3(d_router, 1)
        dx_sum = dx_shared + sum3(dot(jnp.concatenate(split3(d_logits), axis=0), w_router, NT), 0)

        def hits_of(grp, start, count):
            slot = jnp.arange(count * cap, dtype=jnp.int32)
            col = grp * local_exp + start + slot // cap
            table = (jnp.arange(experts, dtype=jnp.int32)[:, None] == col[None, :]).astype(BF16)
            return (dot(want, table) == (slot % cap).astype(F32)[None, :]).astype(BF16)

        swaps = (swap_x, swap_c, [(i, core_partner(d)) for i, d in swap_x])
        for c, (recv, own) in enumerate(bwd_parts[:-1]):
            rows = (recv + own).astype(BF16)
            slot = jnp.arange(per_chunk * cap, dtype=jnp.int32)
            for k, pairs in enumerate(swaps):
                old = slot // cap * other + k * cap + slot % cap
                perm = (old[:, None] == jnp.arange(per_chunk * other, dtype=jnp.int32)[None, :]).astype(BF16)
                back = dot(perm, rows).astype(BF16)
                back = lax.ppermute(back, 'ep', pairs)
                hits = hits_of(ep_order[1 + k], c * per_chunk, per_chunk)
                dx_sum = dx_sum + dot(hits, back)
            dx_sum = lax.optimization_barrier(dx_sum)
        recv, own = bwd_parts[-1]
        dx = last_join(hits_of(ep_i, 0, local_exp), recv, own, dx_sum)
        return y_out, dx, d_router, d_w_gate, d_w_up, d_w_down, ds_gate, ds_up, ds_down

    tok_spec = P(('ep', 'tp'), None)
    in_specs = (tok_spec, tok_spec, P(None, None), P('ep', None, 'tp'), P('ep', None, 'tp'), P('ep', 'tp', None), P(None, 'tp'), P(None, 'tp'), P('tp', None), tok_spec)
    out_specs = (tok_spec, tok_spec, P(None, None), P('ep', None, 'tp'), P('ep', None, 'tp'), P('ep', 'tp', None), P(None, 'tp'), P(None, 'tp'), P('tp', None))

    return jax.shard_map(device_step, mesh=mesh, in_specs=in_specs, out_specs=out_specs, check_vma=False)
```

```python
import functools

import jax
import jax.numpy as jnp
from jax import lax
from jax.experimental import pallas as pl
from jax.experimental.pallas import tpu as pltpu
from jax.sharding import PartitionSpec as P


GATE_SCALE = 16.0
BF16 = jnp.bfloat16
F32 = jnp.float32
FWD_CHUNKS = (2, 8, 6)
BWD_CHUNKS = 2
RETURN_ORDER = (1, 0, 2)
MESH = pl.DeviceIdType.MESH

NN = (((1,), (0,)), ((), ()))
NT = (((1,), (1,)), ((), ()))
TN = (((0,), (0,)), ((), ()))


def dot(a, b, dims=NN):
    return lax.dot_general(a, b, dims, preferred_element_type=F32)


def sigmoid(v):
    return 1.0 / (1.0 + jnp.exp(-jnp.maximum(v, -88.0)))


def swiglu_fwd(a, b):
    return (a * sigmoid(a) * b).astype(BF16)


def swiglu_bwd(a, b, dh):
    sig = sigmoid(a)
    silu = a * sig
    h = (silu * b).astype(BF16)
    da = (dh * b * (sig * (1.0 + a * (1.0 - sig)))).astype(BF16)
    db = (dh * silu).astype(BF16)
    return h, da, db


def rounded(v):
    return v.astype(BF16).astype(F32)


def half_rows(cap, ep_size):
    half = cap * ep_size
    return half, half + (-half) % 8


def store_parts(parity, part, send_ref, own_ref, half, padded):
    shift = padded - half

    @pl.when(parity == 0)
    def _():
        send_ref[0:half, :] = part[0:half]
        own_ref[0:half, :] = part[padded:padded + half]

    @pl.when(parity == 1)
    def _():
        send_ref[half:2 * half, :] = part[shift:padded]
        own_ref[half:2 * half, :] = part[padded + shift:2 * padded]


def pick_matrix(row_ref, rows):
    ids = row_ref[0]
    iota = lax.broadcasted_iota(jnp.int32, (rows, ids.shape[1]), 0)
    return iota == ids


def pick_rows(pick_ref, table_ref, out_ref, scale=None, step=512):
    @pl.loop(0, table_ref.shape[1] // step)
    def _(i):
        cols = pl.ds(pl.multiple_of(i * step, step), step)
        rows = dot(pick_ref[...], table_ref[:, cols])
        out_ref[:, cols] = (rows if scale is None else rows * scale).astype(out_ref.dtype)


def fwd_kernel(half, padded, x_ref, row_ref, w1_ref, w3_ref, w2_ref, send_ref, own_ref, pick_ref, rows_ref):
    pick_ref[...] = jnp.where(pick_matrix(row_ref, 2 * padded), 1.0, 0.0).astype(BF16)
    pick_rows(pick_ref, x_ref, rows_ref)
    rows = rows_ref[...]
    a = rounded(dot(rows, w1_ref[0]))
    b = rounded(dot(rows, w3_ref[0]))
    h = swiglu_fwd(a, b)
    part = dot(h, w2_ref[0])
    store_parts(pl.program_id(0) % 2, part, send_ref, own_ref, half, padded)


def windows(cap, ep_size):
    other, own = (ep_size - 1) * cap, cap
    return other, other + 7 + (-other - 7) % 8, own, own + 7 + (-own - 7) % 8


def bwd_kernel(sizes, per_chunk, x_ref, dy_ref, row_ref, gate_ref, w1_ref, w3_ref, w2_ref, *refs):
    other, win_other, own, win_own = sizes
    dw1_ref, dw3_ref, dw2_ref = refs[:3]
    outs, (far_ref, near_ref, sem, pick_ref, rows_ref, d_out_ref) = refs[3:-6], refs[-6:]
    chunks = far_ref.shape[0] // 2
    e = pl.program_id(0)
    total = 2 * (win_other + win_own)

    @pl.when(e == 0)
    def _():
        far_ref[...] = jnp.zeros_like(far_ref)
        near_ref[...] = jnp.zeros_like(near_ref)

    hit = pick_matrix(row_ref, total)
    pick_ref[...] = jnp.where(hit, 1.0, 0.0).astype(BF16)
    gates = jnp.sum(jnp.where(hit, gate_ref[0], 0.0), axis=1, keepdims=True)
    pick_rows(pick_ref, x_ref, rows_ref)
    pick_rows(pick_ref, dy_ref, d_out_ref, gates)
    rows, d_out = rows_ref[...], d_out_ref[...]
    a = rounded(dot(rows, w1_ref[0]))
    b = rounded(dot(rows, w3_ref[0]))
    dh = rounded(dot(d_out, w2_ref[0], NT))
    h, da, db = swiglu_bwd(a, b, dh)

    chunk = e // per_chunk
    far_base = pl.multiple_of((e % per_chunk) * other // 8 * 8, 8)
    near_base = pl.multiple_of(e * own // 8 * 8, 8)
    step = 512

    @pl.loop(0, rows_ref.shape[1] // step)
    def _(i):
        cols = pl.ds(pl.multiple_of(i * step, step), step)
        dw2_ref[0, :, cols] = dot(h, d_out_ref[:, cols], TN)
        dw1_ref[0, cols, :] = dot(rows_ref[:, cols], da, TN)
        dw3_ref[0, cols, :] = dot(rows_ref[:, cols], db, TN)
        part = dot(da, w1_ref[0, cols, :], NT) + dot(db, w3_ref[0, cols, :], NT)
        for side in range(2):
            far_ref[chunk * 2 + side, pl.ds(far_base, win_other), cols] += part[side * win_other:(side + 1) * win_other]
            first = 2 * win_other + side * win_own
            near_ref[side, pl.ds(near_base, win_own), cols] += part[first:first + win_own]

    def copies(c):
        out = []
        for side in range(2):
            for near in range(2):
                k = 2 * (c + near * chunks) + side
                rows = outs[k].shape[0]
                src = near_ref.at[side, pl.ds(c * rows, rows)] if near else far_ref.at[2 * c + side, pl.ds(0, rows)]
                out.append(pltpu.make_async_copy(src, outs[k], sem.at[k]))
        return out

    for c in range(chunks):
        @pl.when(e == (c + 1) * per_chunk - 1)
        def _():
            for copy in copies(c):
                copy.start()

    @pl.when(e == chunks * per_chunk - 1)
    def _():
        for c in range(chunks):
            for copy in copies(c):
                copy.wait()


def expert_fwd(start, count, half, padded, x_all, row_ids, w_gate, w_up, w_down):
    tokens, model = x_all.shape
    width = w_gate.shape[2]
    out = jax.ShapeDtypeStruct((count * half, model), F32)
    return pl.pallas_call(
        functools.partial(fwd_kernel, half, padded),
        grid=(count,),
        in_specs=[
            pl.BlockSpec((tokens, model), lambda i: (0, 0), pipeline_mode=pl.Buffered(1)),
            pl.BlockSpec((1, 1, tokens), lambda i: (start + i, 0, 0)),
            pl.BlockSpec((1, model, width), lambda i: (start + i, 0, 0)),
            pl.BlockSpec((1, model, width), lambda i: (start + i, 0, 0)),
            pl.BlockSpec((1, width, model), lambda i: (start + i, 0, 0)),
        ],
        out_specs=[pl.BlockSpec((2 * half, model), lambda i: (i // 2, 0))] * 2,
        out_shape=[out, out],
        scratch_shapes=[pltpu.VMEM((2 * padded, tokens), BF16), pltpu.VMEM((2 * padded, model), BF16)],
        cost_estimate=pl.CostEstimate(
            flops=count * 2 * 2 * padded * model * (tokens + 3 * width),
            bytes_accessed=count * (6 * model * width + 8 * half * model) + 2 * tokens * model,
            transcendentals=count * 2 * padded * width),
        compiler_params=pltpu.CompilerParams(dimension_semantics=('arbitrary',), vmem_limit_bytes=48 << 20),
    )(x_all, row_ids, w_gate, w_up, w_down)


def expert_bwd(chunks, sizes, x_all, dy_all, row_ids, gates, w_gate, w_up, w_down):
    other, win_other, own, win_own = sizes
    tokens, model = x_all.shape
    count, _, width = w_gate.shape
    per_chunk = count // chunks
    far_rows, near_rows = per_chunk * other, per_chunk * own
    far_pad = max(j * other // 8 * 8 + win_other for j in range(per_chunk))
    near_pad = max(j * own // 8 * 8 + win_own for j in range(count))
    part_shapes = [jax.ShapeDtypeStruct((n, model), F32) for n in (far_rows, near_rows) for _ in range(2 * chunks)]
    rows = 2 * (win_other + win_own)
    outs = pl.pallas_call(
        functools.partial(bwd_kernel, sizes, per_chunk),
        grid=(count,),
        in_specs=[
            pl.BlockSpec((tokens, model), lambda i: (0, 0), pipeline_mode=pl.Buffered(1)),
            pl.BlockSpec((tokens, model), lambda i: (0, 0), pipeline_mode=pl.Buffered(1)),
            pl.BlockSpec((1, 1, tokens), lambda i: (i, 0, 0)),
            pl.BlockSpec((1, 1, tokens), lambda i: (i, 0, 0)),
            pl.BlockSpec((1, model, width), lambda i: (i, 0, 0)),
            pl.BlockSpec((1, model, width), lambda i: (i, 0, 0)),
            pl.BlockSpec((1, width, model), lambda i: (i, 0, 0)),
        ],
        out_specs=[
            pl.BlockSpec((1, model, width), lambda i: (i, 0, 0)),
            pl.BlockSpec((1, model, width), lambda i: (i, 0, 0)),
            pl.BlockSpec((1, width, model), lambda i: (i, 0, 0)),
        ] + [pl.BlockSpec(memory_space=pl.ANY)] * len(part_shapes),
        out_shape=[
            jax.ShapeDtypeStruct((count, model, width), F32),
            jax.ShapeDtypeStruct((count, model, width), F32),
            jax.ShapeDtypeStruct((count, width, model), F32),
        ] + part_shapes,
        scratch_shapes=[
            pltpu.VMEM((2 * chunks, far_pad, model), F32),
            pltpu.VMEM((2, near_pad, model), F32),
            pltpu.SemaphoreType.DMA((len(part_shapes),)),
            pltpu.VMEM((rows, tokens), BF16),
            pltpu.VMEM((rows, model), BF16),
            pltpu.VMEM((rows, model), BF16),
        ],
        cost_estimate=pl.CostEstimate(
            flops=count * 2 * rows * model * (2 * tokens + 8 * width),
            bytes_accessed=count * (18 * model * width + 4 * rows * model) + 4 * tokens * model,
            transcendentals=count * rows * width),
        compiler_params=pltpu.CompilerParams(dimension_semantics=('arbitrary',), vmem_limit_bytes=60 << 20),
        name='expert_bwd',
    )(x_all, dy_all, row_ids, gates, w_gate, w_up, w_down)
    parts = outs[3:]
    return outs[:3], [(parts[2 * c], parts[2 * c + 1]) for c in range(2 * chunks)]


def shared_grad_kernel(step, x_ref, dy_ref, wg_ref, wu_ref, wd_ref, dg_ref, du_ref, dd_ref, h_ref, da_ref, db_ref):
    tokens, model = x_ref.shape

    @pl.loop(0, tokens // step)
    def _(i):
        rows = pl.ds(pl.multiple_of(i * step, step), step)
        a = rounded(dot(x_ref[rows, :], wg_ref[...]))
        b = rounded(dot(x_ref[rows, :], wu_ref[...]))
        dh = rounded(dot(dy_ref[rows, :], wd_ref[...], NT))
        h_ref[rows, :], da_ref[rows, :], db_ref[rows, :] = swiglu_bwd(a, b, dh)

    @pl.loop(0, model // step)
    def _(i):
        cols = pl.ds(pl.multiple_of(i * step, step), step)
        dd_ref[:, cols] = dot(h_ref[...], dy_ref[:, cols], TN)
        dg_ref[cols, :] = dot(x_ref[:, cols], da_ref[...], TN)
        du_ref[cols, :] = dot(x_ref[:, cols], db_ref[...], TN)


def shared_grad(x_all, dy_all, ws_gate, ws_up, ws_down):
    tokens, model = x_all.shape
    width = ws_gate.shape[1]
    block = min(width, 256)
    full = pl.BlockSpec((tokens, model), lambda i: (0, 0), pipeline_mode=pl.Buffered(1))
    col = pl.BlockSpec((model, block), lambda i: (0, i))
    row = pl.BlockSpec((block, model), lambda i: (i, 0))
    return pl.pallas_call(
        functools.partial(shared_grad_kernel, 256),
        grid=(width // block,),
        in_specs=[full, full, col, col, row],
        out_specs=[col, col, row],
        out_shape=[jax.ShapeDtypeStruct((model, width), F32)] * 2 + [jax.ShapeDtypeStruct((width, model), F32)],
        scratch_shapes=[pltpu.VMEM((tokens, block), BF16)] * 3,
        cost_estimate=pl.CostEstimate(
            flops=12 * tokens * model * width, bytes_accessed=4 * tokens * model + 18 * model * width,
            transcendentals=tokens * width),
        compiler_params=pltpu.CompilerParams(dimension_semantics=('arbitrary',), vmem_limit_bytes=48 << 20),
        name='shared_grad',
    )(x_all, dy_all, ws_gate, ws_up, ws_down)


def split3(v):
    hi = lax.reduce_precision(v, 8, 7)
    rest = v - hi
    mid = lax.reduce_precision(rest, 8, 7)
    low = rest - mid
    return hi.astype(BF16), mid.astype(BF16), low.astype(BF16)


def sum3(v, axis):
    first, second, third = jnp.split(v, 3, axis=axis)
    return first + second + third


def core_partner(ep):
    return ep + 1 - 2 * (ep % 2)


def gather_kernel(x_ref, idx_ref, dy_ref, wg_ref, wu_ref, wd_ref, x_all, idx_all, dy_pair, wd_part, quarter, send_sem, recv_sem, idx_send, idx_recv, local_sem, x_buf, dy_buf, q_buf):
    tp = lax.axis_index('tp')
    ep = lax.axis_index('ep')
    eps = x_all.shape[0] // 2
    half = eps // 2
    tp_o = 1 - tp
    ep_x = (ep + half) % eps
    ep_c = core_partner(ep)

    def slot(e, t):
        return e * 2 + t

    others = [(tp_o, ep)]
    for k in range(1, eps):
        others += [(tp, (ep + k) % eps), (tp_o, (ep + k) % eps)]
    barrier = pltpu.get_barrier_semaphore()
    for t, e in others:
        pl.semaphore_signal(barrier, inc=1, device_id={'tp': t, 'ep': e}, device_id_type=MESH)
    pl.semaphore_wait(barrier, len(others))

    def send(k, src, dst, t, e):
        copy = pltpu.make_async_remote_copy(
            src_ref=src, dst_ref=dst, send_sem=send_sem.at[k], recv_sem=recv_sem.at[k],
            device_id={'tp': t, 'ep': e}, device_id_type=MESH)
        copy.start()
        return copy

    def block(e, t):
        return x_all.at[slot(e, t)]

    mine = block(ep, tp)
    to_y = send(0, x_ref, mine, tp_o, ep)
    to_x = send(1, x_ref, mine, tp, ep_x)
    to_c = send(2, x_ref, mine, tp, ep_c)
    own_idx = idx_all.at[slot(ep, tp)]
    idx_copies = []
    for k, (t, e) in enumerate(others):
        copy = pltpu.make_async_remote_copy(
            src_ref=idx_ref, dst_ref=own_idx, send_sem=idx_send.at[k], recv_sem=idx_recv.at[k],
            device_id={'tp': t, 'ep': e}, device_id_type=MESH)
        copy.start()
        idx_copies.append(copy)
    width = quarter.shape[1] // 2
    cols = pl.ds(pl.multiple_of(ep * width, width), width)
    load = [
        pltpu.make_async_copy(x_ref, x_buf, local_sem.at[0]),
        pltpu.make_async_copy(dy_ref, dy_buf, local_sem.at[1]),
        pltpu.make_async_copy(wg_ref.at[:, cols], q_buf.at[:, pl.ds(0, width)], local_sem.at[2]),
        pltpu.make_async_copy(wu_ref.at[:, cols], q_buf.at[:, pl.ds(width, width)], local_sem.at[3]),
    ]
    store = [
        pltpu.make_async_copy(x_buf, mine, local_sem.at[4]),
        pltpu.make_async_copy(dy_buf, dy_pair.at[tp], local_sem.at[5]),
        pltpu.make_async_copy(q_buf, quarter, local_sem.at[6]),
        pltpu.make_async_copy(idx_ref, own_idx, local_sem.at[7]),
    ]
    for copy in load:
        copy.start()
    dy_y = send(3, dy_ref, dy_pair.at[tp], tp_o, ep)
    rows = wd_part.shape[0]
    wd_y = send(4, wd_ref.at[pl.ds(ep * rows, rows)], wd_part, tp_o, ep)

    for copy in load:
        copy.wait()
    for copy in store:
        copy.start()
    to_y.wait_recv()
    y_to_x = send(5, block(ep, tp_o), block(ep, tp_o), tp, ep_x)
    y_to_c = send(6, block(ep, tp_o), block(ep, tp_o), tp, ep_c)
    to_x.wait_recv()
    x_to_c = send(7, block(ep_x, tp), block(ep_x, tp), tp, ep_c)
    y_to_x.wait_recv()
    xy_to_c = send(8, block(ep_x, tp_o), block(ep_x, tp_o), tp, ep_c)
    for copy in (to_c, dy_y, wd_y, y_to_c, x_to_c, xy_to_c):
        copy.wait_recv()
    for copy in idx_copies:
        copy.wait_recv()
    for copy in store:
        copy.wait()
    for copy in (to_y, to_x, to_c, dy_y, wd_y, y_to_x, y_to_c, x_to_c, xy_to_c):
        copy.wait_send()
    for copy in idx_copies:
        copy.wait_send()


def gather_rows(devices, ep_size, x, idx_t, dy, ws_gate, ws_up, ws_down):
    _, model = x.shape
    any_spec = pl.BlockSpec(memory_space=pl.ANY)
    return pl.pallas_call(
        gather_kernel,
        in_specs=[any_spec] * 6,
        out_specs=[any_spec] * 5,
        out_shape=[
            jax.ShapeDtypeStruct((devices,) + x.shape, x.dtype),
            jax.ShapeDtypeStruct((devices,) + idx_t.shape, idx_t.dtype),
            jax.ShapeDtypeStruct((2,) + dy.shape, dy.dtype),
            jax.ShapeDtypeStruct((ws_down.shape[0] // ep_size, model), ws_down.dtype),
            jax.ShapeDtypeStruct((model, 2 * ws_gate.shape[1] // ep_size), ws_gate.dtype),
        ],
        scratch_shapes=[
            pltpu.SemaphoreType.DMA((9,)),
            pltpu.SemaphoreType.DMA((9,)),
            pltpu.SemaphoreType.DMA((devices - 1,)),
            pltpu.SemaphoreType.DMA((devices - 1,)),
            pltpu.SemaphoreType.DMA((8,)),
            pltpu.VMEM(x.shape, x.dtype),
            pltpu.VMEM(dy.shape, dy.dtype),
            pltpu.VMEM((model, 2 * ws_gate.shape[1] // ep_size), ws_gate.dtype),
        ],
        cost_estimate=pl.CostEstimate(flops=60_000_000_000, bytes_accessed=4 * devices * x.size, transcendentals=0),
        compiler_params=pltpu.CompilerParams(collective_id=0, has_side_effects=True),
        name='gather_rows',
    )(x, idx_t, dy, ws_gate, ws_up, ws_down)


def solution(mesh):
    tp_size = mesh.shape['tp']
    ep_size = mesh.shape['ep']
    swap_tp = [(i, tp_size - 1 - i) for i in range(tp_size)]
    swap_x = [(i, (i + ep_size // 2) % ep_size) for i in range(ep_size)]
    swap_c = [(i, core_partner(i)) for i in range(ep_size)]

    def device_step(x, grad_y, w_router, w_gate, w_up, w_down, ws_gate, ws_up, ws_down, topk_idx):
        tok, model = x.shape
        top_k = topk_idx.shape[1]
        experts = w_router.shape[1]
        local_exp = w_gate.shape[0]
        groups = top_k // 2
        most = groups * tok // (2 * ep_size) + min(groups, ep_size // 2) * tok // ep_size
        cap = (2 * most + local_exp - 1) // local_exp
        half, padded = half_rows(cap, ep_size)
        shift = padded - half
        ep_i = lax.axis_index('ep')
        tp_i = lax.axis_index('tp')
        devices = ep_size * tp_size
        ep_order = (ep_i, (ep_i + ep_size // 2) % ep_size, core_partner(ep_i), core_partner((ep_i + ep_size // 2) % ep_size))

        def ep_pieces(piece):
            far = lax.ppermute(piece, 'ep', swap_x)
            return piece, far, lax.ppermute(piece, 'ep', swap_c), lax.ppermute(far, 'ep', swap_c)

        def ep_gather(piece):
            out = jnp.zeros((ep_size,) + piece.shape, piece.dtype)
            for e, part in zip(ep_order, ep_pieces(piece)):
                out = lax.dynamic_update_slice_in_dim(out, part[None], e, 0)
            return out

        x_blocks, idx_all, dy_pair, wd_part, quarter = gather_rows(devices, ep_size, x, topk_idx.T, grad_y, ws_gate, ws_up, ws_down)
        x_all = x_blocks.reshape(devices * tok, model)

        width_q = ws_gate.shape[1] // ep_size
        gu_part = lax.ppermute(quarter, 'tp', swap_tp)

        lower = (lax.broadcasted_iota(jnp.int32, (tok, tok), 0) > lax.broadcasted_iota(jnp.int32, (tok, tok), 1)).astype(BF16)
        local_ids = ep_i * local_exp + jnp.arange(local_exp, dtype=jnp.int32)
        hit = jnp.any(idx_all[None] == local_ids[:, None, None, None], axis=2)
        rank = jnp.einsum('edj,ij->edi', hit.astype(BF16), lower, preferred_element_type=F32).astype(jnp.int32)
        dev = jnp.arange(devices, dtype=jnp.int32)
        is_own = (dev % tp_size) == tp_i
        parity = jnp.arange(local_exp, dtype=jnp.int32) % 2
        base = (jnp.where(is_own, padded, 0) + (dev // tp_size) * cap)[None, :] + (parity * shift)[:, None]
        row_ids = jnp.where(hit, base[:, :, None] + rank, -1).reshape(local_exp, 1, devices * tok)

        fwd_parts = []
        start = 0
        rows_now = row_ids
        for count in FWD_CHUNKS:
            send, own = expert_fwd(start, count, half, padded, x_all, rows_now, w_gate, w_up, w_down)
            start += count
            rows_now, own = lax.optimization_barrier((rows_now, own))
            fwd_parts.append((lax.ppermute(send, 'tp', swap_tp), own))

        own0 = fwd_parts[-1][1]
        x_late, hit, rank, w_router, own0 = lax.optimization_barrier((x_all, hit, rank, w_router, own0))
        fwd_parts[-1] = (fwd_parts[-1][0], own0)

        logits_t = jnp.einsum('de,td->et', w_router, x_late, preferred_element_type=F32)
        probs_t = jax.nn.softmax(logits_t, axis=0)
        gates_local = GATE_SCALE * lax.dynamic_slice_in_dim(probs_t, ep_i * local_exp, local_exp, 0).reshape(local_exp, 1, devices * tok)

        sizes = windows(cap, ep_size)
        other, win_other, near, win_near = sizes
        per_chunk = local_exp // BWD_CHUNKS
        dev_ep = dev // tp_size
        place = jnp.zeros_like(dev)
        for k, e in enumerate(ep_order[1:]):
            place = jnp.where(dev_ep == e, k * cap, place)
        exp = jnp.arange(local_exp, dtype=jnp.int32)
        far_first = (jnp.where(is_own, win_other, 0) + place)[None, :] + ((exp % per_chunk) * other % 8)[:, None]
        near_first = jnp.where(is_own, win_near, 0)[None, :] + (2 * win_other + exp * near % 8)[:, None]
        first = jnp.where((dev_ep == ep_i)[None, :], near_first, far_first)
        bwd_ids = jnp.where(hit, first[:, :, None] + rank, -1).reshape(local_exp, 1, devices * tok)
        dy_all = ep_gather(dy_pair).reshape(devices * tok, model)
        (d_w_gate, d_w_up, d_w_down), bwd_out = expert_bwd(BWD_CHUNKS, sizes, x_all, dy_all, bwd_ids, gates_local, w_gate, w_up, w_down)
        bwd_parts = [(lax.ppermute(bwd_out[0][0], 'tp', swap_tp), bwd_out[0][1])]

        own_last = bwd_out[-1][1]
        own_first = fwd_parts[0][1]
        gu_far = lax.ppermute(gu_part, 'ep', swap_x)
        wd_far = lax.ppermute(wd_part, 'ep', swap_x)
        x, grad_y, x_all, dy_all, topk_idx, w_router, gu_part, wd_part, gu_far, wd_far, own_first, own_last = lax.optimization_barrier(
            (x, grad_y, x_all, dy_all, topk_idx, w_router, gu_part, wd_part, gu_far, wd_far, own_first, own_last))
        fwd_parts[0] = (fwd_parts[0][0], own_first)
        bwd_out[-1] = (bwd_out[-1][0], own_last)

        def back_rows(count):
            return count * cap + (-count * cap) % 8

        def slot_index(count):
            new = jnp.arange(ep_size * back_rows(count), dtype=jnp.int32)
            block, rest = new // back_rows(count), new % back_rows(count)
            return block, rest // cap, rest % cap, rest < count * cap

        def turn(parts, count):
            recv, own = parts
            rows = (recv + own).astype(BF16)
            src, exp, rank, valid = slot_index(count)
            old = jnp.where(valid, exp * half + src * cap + rank, -1)
            perm = (old[:, None] == jnp.arange(count * half, dtype=jnp.int32)[None, :]).astype(BF16)
            return dot(perm, rows).astype(BF16)

        def send_home(out, count):
            out = out.reshape(ep_size, back_rows(count), model)
            out = lax.all_to_all(out, 'ep', 0, 0)
            return out.reshape(ep_size * back_rows(count), model)

        early = RETURN_ORDER[0]
        early_rows = turn(fwd_parts[early], FWD_CHUNKS[early])
        x, grad_y, topk_idx, gu_part, wd_part, gu_far, wd_far, early_rows = lax.optimization_barrier(
            (x, grad_y, topk_idx, gu_part, wd_part, gu_far, wd_far, early_rows))
        early_back = send_home(early_rows, FWD_CHUNKS[early])

        gu_other = (gu_part, gu_far, lax.ppermute(gu_part, 'ep', swap_c), lax.ppermute(gu_far, 'ep', swap_c))
        wd_other = jnp.concatenate((wd_part, wd_far, lax.ppermute(wd_part, 'ep', swap_c), lax.ppermute(wd_far, 'ep', swap_c)), axis=0)
        wg_other = jnp.concatenate([p[:, :width_q] for p in gu_other], axis=1)
        wu_other = jnp.concatenate([p[:, width_q:] for p in gu_other], axis=1)
        shared = jnp.zeros((tok, model), F32)
        dx_shared = jnp.zeros((tok, model), F32)
        for wg, wu, wd in ((ws_gate, ws_up, ws_down), (wg_other, wu_other, wd_other)):
            a = rounded(dot(x, wg))
            b = rounded(dot(x, wu))
            dh = rounded(dot(grad_y, wd, NT))
            h, da, db = swiglu_bwd(a, b, dh)
            shared = shared + dot(h, wd)
            dx_shared = dx_shared + dot(da, wg, NT) + dot(db, wu, NT)
        ds_gate, ds_up, ds_down = shared_grad(x_all, dy_all, ws_gate, ws_up, ws_down)

        hit_own = jnp.any(topk_idx[:, None, :] == jnp.arange(experts, dtype=jnp.int32)[None, :, None], axis=2)
        rank_own = dot(lower, hit_own.astype(BF16))
        want = jnp.where(hit_own, rank_own, -1.0).astype(BF16)
        probs = jax.nn.softmax(dot(x, w_router), axis=-1)
        prob_parts = jnp.concatenate(split3(probs), axis=0)

        def expand(start, count):
            grp, exp, rank, valid = slot_index(count)
            col = jnp.where(valid, grp * local_exp + start + exp, -1)
            table = (jnp.arange(experts, dtype=jnp.int32)[:, None] == col[None, :]).astype(BF16)
            return table, jnp.where(valid, rank, -2).astype(F32)[None, :]

        routed = jnp.zeros((tok, model), F32)
        d_scores = jnp.zeros((tok, experts), F32)
        back = early_back
        for j in RETURN_ORDER:
            count, start = FWD_CHUNKS[j], sum(FWD_CHUNKS[:j])
            if j != early:
                recv, own = fwd_parts[j]
                back, own = lax.optimization_barrier((back, own))
                back = send_home(turn((recv, own), count), count)
            table, rank = expand(start, count)
            hits = dot(want, table) == rank
            gates = jnp.where(jnp.concatenate([hits] * 3, axis=0), dot(prob_parts, table), 0.0).astype(BF16)
            mixed = dot(gates, back)
            routed = routed + GATE_SCALE * sum3(mixed, 0)
            score = jnp.where(hits, dot(grad_y, back, NT), 0.0)
            part = dot(jnp.concatenate(split3(score), axis=0), table, NT)
            d_scores = d_scores + sum3(part, 0)
        y_out = (shared + routed).astype(BF16)

        d_scores = GATE_SCALE * d_scores
        mean_score = jnp.sum(probs * d_scores, axis=-1, keepdims=True)
        d_logits = probs * (d_scores - mean_score)
        d_other = lax.ppermute(d_logits, 'tp', swap_tp)
        for send, own in bwd_out[1:]:
            bwd_parts.append((lax.ppermute(send, 'tp', swap_tp), own))
        d_pair = jnp.where(tp_i == 0, jnp.stack([d_logits, d_other]), jnp.stack([d_other, d_logits]))
        d_logits_all = ep_gather(d_pair).reshape(devices * tok, experts)
        d_router = dot(x_all, jnp.concatenate(split3(d_logits_all), axis=1), TN)
        d_router = sum3(d_router, 1)
        dx_sum = dx_shared + sum3(dot(jnp.concatenate(split3(d_logits), axis=0), w_router, NT), 0)

        def hits_of(grp, start, count):
            slot = jnp.arange(count * cap, dtype=jnp.int32)
            col = grp * local_exp + start + slot // cap
            table = (jnp.arange(experts, dtype=jnp.int32)[:, None] == col[None, :]).astype(BF16)
            return (dot(want, table) == (slot % cap).astype(F32)[None, :]).astype(BF16)

        swaps = (swap_x, swap_c, [(i, core_partner(d)) for i, d in swap_x])
        for c, (recv, own) in enumerate(bwd_parts[:BWD_CHUNKS]):
            rows = (recv + own).astype(BF16)
            slot = jnp.arange(per_chunk * cap, dtype=jnp.int32)
            for k, pairs in enumerate(swaps):
                old = slot // cap * other + k * cap + slot % cap
                perm = (old[:, None] == jnp.arange(per_chunk * other, dtype=jnp.int32)[None, :]).astype(BF16)
                back = dot(perm, rows).astype(BF16)
                back = lax.ppermute(back, 'ep', pairs)
                hits = hits_of(ep_order[1 + k], c * per_chunk, per_chunk)
                dx_sum = dx_sum + dot(hits, back)
            dx_sum = lax.optimization_barrier(dx_sum)
        for c, (recv, own) in enumerate(bwd_parts[BWD_CHUNKS:]):
            hits = hits_of(ep_i, c * per_chunk, per_chunk)
            dx_sum = dx_sum + dot(hits, (recv + own).astype(BF16))
            if c + 1 < BWD_CHUNKS:
                dx_sum = lax.optimization_barrier(dx_sum)
        return y_out, dx_sum.astype(BF16), d_router, d_w_gate, d_w_up, d_w_down, ds_gate, ds_up, ds_down

    tok_spec = P(('ep', 'tp'), None)
    in_specs = (tok_spec, tok_spec, P(None, None), P('ep', None, 'tp'), P('ep', None, 'tp'), P('ep', 'tp', None), P(None, 'tp'), P(None, 'tp'), P('tp', None), tok_spec)
    out_specs = (tok_spec, tok_spec, P(None, None), P('ep', None, 'tp'), P('ep', None, 'tp'), P('ep', 'tp', None), P(None, 'tp'), P(None, 'tp'), P('tp', None))

    return jax.shard_map(device_step, mesh=mesh, in_specs=in_specs, out_specs=out_specs, check_vma=False)
```

```python
import functools

import jax
import jax.numpy as jnp
from jax import lax
from jax.experimental import pallas as pl
from jax.experimental.pallas import tpu as pltpu
from jax.sharding import PartitionSpec as P


GATE_SCALE = 16.0
BF16 = jnp.bfloat16
F32 = jnp.float32
FWD_CHUNKS = (2, 8, 6)
BWD_CHUNKS = 2
RETURN_ORDER = (1, 0, 2)
MESH = pl.DeviceIdType.MESH

NN = (((1,), (0,)), ((), ()))
NT = (((1,), (1,)), ((), ()))
TN = (((0,), (0,)), ((), ()))


def dot(a, b, dims=NN):
    return lax.dot_general(a, b, dims, preferred_element_type=F32)


def sigmoid(v):
    return 1.0 / (1.0 + jnp.exp(-jnp.maximum(v, -88.0)))


def swiglu_fwd(a, b):
    return (a * sigmoid(a) * b).astype(BF16)


def swiglu_bwd(a, b, dh):
    sig = sigmoid(a)
    silu = a * sig
    h = (silu * b).astype(BF16)
    da = (dh * b * (sig * (1.0 + a * (1.0 - sig)))).astype(BF16)
    db = (dh * silu).astype(BF16)
    return h, da, db


def rounded(v):
    return v.astype(BF16).astype(F32)


def half_rows(cap, ep_size):
    half = cap * ep_size
    return half, half + (-half) % 8


def store_parts(parity, part, send_ref, own_ref, half, padded):
    shift = padded - half

    @pl.when(parity == 0)
    def _():
        send_ref[0:half, :] = part[0:half]
        own_ref[0:half, :] = part[padded:padded + half]

    @pl.when(parity == 1)
    def _():
        send_ref[half:2 * half, :] = part[shift:padded]
        own_ref[half:2 * half, :] = part[padded + shift:2 * padded]


def pick_matrix(row_ref, rows):
    ids = row_ref[0]
    iota = lax.broadcasted_iota(jnp.int32, (rows, ids.shape[1]), 0)
    return iota == ids


def pick_rows(pick_ref, table_ref, out_ref, scale=None, step=512):
    @pl.loop(0, table_ref.shape[1] // step)
    def _(i):
        cols = pl.ds(pl.multiple_of(i * step, step), step)
        rows = dot(pick_ref[...], table_ref[:, cols])
        out_ref[:, cols] = (rows if scale is None else rows * scale).astype(out_ref.dtype)


def fwd_kernel(half, padded, x_ref, row_ref, w1_ref, w3_ref, w2_ref, send_ref, own_ref, pick_ref, rows_ref):
    pick_ref[...] = jnp.where(pick_matrix(row_ref, 2 * padded), 1.0, 0.0).astype(BF16)
    pick_rows(pick_ref, x_ref, rows_ref)
    rows = rows_ref[...]
    a = rounded(dot(rows, w1_ref[0]))
    b = rounded(dot(rows, w3_ref[0]))
    h = swiglu_fwd(a, b)
    part = dot(h, w2_ref[0])
    store_parts(pl.program_id(0) % 2, part, send_ref, own_ref, half, padded)


def windows(cap, ep_size):
    other, own = (ep_size - 1) * cap, cap
    return other, other + 7 + (-other - 7) % 8, own, own + 7 + (-own - 7) % 8


def bwd_kernel(sizes, per_chunk, x_ref, dy_ref, row_ref, gate_ref, w1_ref, w3_ref, w2_ref, *refs):
    other, win_other, own, win_own = sizes
    dw1_ref, dw3_ref, dw2_ref = refs[:3]
    outs, (far_ref, near_ref, sem, pick_ref, rows_ref, d_out_ref) = refs[3:-6], refs[-6:]
    chunks = far_ref.shape[0] // 2
    e = pl.program_id(0)
    total = 2 * (win_other + win_own)

    @pl.when(e == 0)
    def _():
        far_ref[...] = jnp.zeros_like(far_ref)
        near_ref[...] = jnp.zeros_like(near_ref)

    hit = pick_matrix(row_ref, total)
    pick_ref[...] = jnp.where(hit, 1.0, 0.0).astype(BF16)
    gates = jnp.sum(jnp.where(hit, gate_ref[0], 0.0), axis=1, keepdims=True)
    pick_rows(pick_ref, x_ref, rows_ref)
    pick_rows(pick_ref, dy_ref, d_out_ref, gates)
    rows, d_out = rows_ref[...], d_out_ref[...]
    a = rounded(dot(rows, w1_ref[0]))
    b = rounded(dot(rows, w3_ref[0]))
    dh = rounded(dot(d_out, w2_ref[0], NT))
    h, da, db = swiglu_bwd(a, b, dh)

    chunk = e // per_chunk
    far_base = pl.multiple_of((e % per_chunk) * other // 8 * 8, 8)
    near_base = pl.multiple_of(e * own // 8 * 8, 8)
    step = 512

    @pl.loop(0, rows_ref.shape[1] // step)
    def _(i):
        cols = pl.ds(pl.multiple_of(i * step, step), step)
        dw2_ref[0, :, cols] = dot(h, d_out_ref[:, cols], TN)
        dw1_ref[0, cols, :] = dot(rows_ref[:, cols], da, TN)
        dw3_ref[0, cols, :] = dot(rows_ref[:, cols], db, TN)
        part = dot(da, w1_ref[0, cols, :], NT) + dot(db, w3_ref[0, cols, :], NT)
        for side in range(2):
            far_ref[chunk * 2 + side, pl.ds(far_base, win_other), cols] += part[side * win_other:(side + 1) * win_other]
            first = 2 * win_other + side * win_own
            near_ref[side, pl.ds(near_base, win_own), cols] += part[first:first + win_own]

    def copies(c):
        out = []
        for side in range(2):
            for near in range(2):
                k = 2 * (c + near * chunks) + side
                rows = outs[k].shape[0]
                src = near_ref.at[side, pl.ds(c * rows, rows)] if near else far_ref.at[2 * c + side, pl.ds(0, rows)]
                out.append(pltpu.make_async_copy(src, outs[k], sem.at[k]))
        return out

    for c in range(chunks):
        @pl.when(e == (c + 1) * per_chunk - 1)
        def _():
            for copy in copies(c):
                copy.start()

    @pl.when(e == chunks * per_chunk - 1)
    def _():
        for c in range(chunks):
            for copy in copies(c):
                copy.wait()


def expert_fwd(start, count, half, padded, x_all, row_ids, w_gate, w_up, w_down):
    tokens, model = x_all.shape
    width = w_gate.shape[2]
    out = jax.ShapeDtypeStruct((count * half, model), F32)
    return pl.pallas_call(
        functools.partial(fwd_kernel, half, padded),
        grid=(count,),
        in_specs=[
            pl.BlockSpec((tokens, model), lambda i: (0, 0), pipeline_mode=pl.Buffered(1)),
            pl.BlockSpec((1, 1, tokens), lambda i: (start + i, 0, 0)),
            pl.BlockSpec((1, model, width), lambda i: (start + i, 0, 0)),
            pl.BlockSpec((1, model, width), lambda i: (start + i, 0, 0)),
            pl.BlockSpec((1, width, model), lambda i: (start + i, 0, 0)),
        ],
        out_specs=[pl.BlockSpec((2 * half, model), lambda i: (i // 2, 0))] * 2,
        out_shape=[out, out],
        scratch_shapes=[pltpu.VMEM((2 * padded, tokens), BF16), pltpu.VMEM((2 * padded, model), BF16)],
        cost_estimate=pl.CostEstimate(
            flops=count * 2 * 2 * padded * model * (tokens + 3 * width),
            bytes_accessed=count * (6 * model * width + 8 * half * model) + 2 * tokens * model,
            transcendentals=count * 2 * padded * width),
        compiler_params=pltpu.CompilerParams(dimension_semantics=('arbitrary',), vmem_limit_bytes=48 << 20),
    )(x_all, row_ids, w_gate, w_up, w_down)


def expert_bwd(chunks, sizes, x_all, dy_all, row_ids, gates, w_gate, w_up, w_down):
    other, win_other, own, win_own = sizes
    tokens, model = x_all.shape
    count, _, width = w_gate.shape
    per_chunk = count // chunks
    far_rows, near_rows = per_chunk * other, per_chunk * own
    far_pad = max(j * other // 8 * 8 + win_other for j in range(per_chunk))
    near_pad = max(j * own // 8 * 8 + win_own for j in range(count))
    part_shapes = [jax.ShapeDtypeStruct((n, model), F32) for n in (far_rows, near_rows) for _ in range(2 * chunks)]
    rows = 2 * (win_other + win_own)
    outs = pl.pallas_call(
        functools.partial(bwd_kernel, sizes, per_chunk),
        grid=(count,),
        in_specs=[
            pl.BlockSpec((tokens, model), lambda i: (0, 0), pipeline_mode=pl.Buffered(1)),
            pl.BlockSpec((tokens, model), lambda i: (0, 0), pipeline_mode=pl.Buffered(1)),
            pl.BlockSpec((1, 1, tokens), lambda i: (i, 0, 0)),
            pl.BlockSpec((1, 1, tokens), lambda i: (i, 0, 0)),
            pl.BlockSpec((1, model, width), lambda i: (i, 0, 0)),
            pl.BlockSpec((1, model, width), lambda i: (i, 0, 0)),
            pl.BlockSpec((1, width, model), lambda i: (i, 0, 0)),
        ],
        out_specs=[
            pl.BlockSpec((1, model, width), lambda i: (i, 0, 0)),
            pl.BlockSpec((1, model, width), lambda i: (i, 0, 0)),
            pl.BlockSpec((1, width, model), lambda i: (i, 0, 0)),
        ] + [pl.BlockSpec(memory_space=pl.ANY)] * len(part_shapes),
        out_shape=[
            jax.ShapeDtypeStruct((count, model, width), F32),
            jax.ShapeDtypeStruct((count, model, width), F32),
            jax.ShapeDtypeStruct((count, width, model), F32),
        ] + part_shapes,
        scratch_shapes=[
            pltpu.VMEM((2 * chunks, far_pad, model), F32),
            pltpu.VMEM((2, near_pad, model), F32),
            pltpu.SemaphoreType.DMA((len(part_shapes),)),
            pltpu.VMEM((rows, tokens), BF16),
            pltpu.VMEM((rows, model), BF16),
            pltpu.VMEM((rows, model), BF16),
        ],
        cost_estimate=pl.CostEstimate(
            flops=count * 2 * rows * model * (2 * tokens + 8 * width),
            bytes_accessed=count * (18 * model * width + 4 * rows * model) + 4 * tokens * model,
            transcendentals=count * rows * width),
        compiler_params=pltpu.CompilerParams(dimension_semantics=('arbitrary',), vmem_limit_bytes=60 << 20),
        name='expert_bwd',
    )(x_all, dy_all, row_ids, gates, w_gate, w_up, w_down)
    parts = outs[3:]
    return outs[:3], [(parts[2 * c], parts[2 * c + 1]) for c in range(2 * chunks)]


def shared_grad_kernel(step, x_ref, dy_ref, wg_ref, wu_ref, wd_ref, dg_ref, du_ref, dd_ref, h_ref, da_ref, db_ref):
    tokens, model = x_ref.shape

    @pl.loop(0, tokens // step)
    def _(i):
        rows = pl.ds(pl.multiple_of(i * step, step), step)
        a = rounded(dot(x_ref[rows, :], wg_ref[...]))
        b = rounded(dot(x_ref[rows, :], wu_ref[...]))
        dh = rounded(dot(dy_ref[rows, :], wd_ref[...], NT))
        h_ref[rows, :], da_ref[rows, :], db_ref[rows, :] = swiglu_bwd(a, b, dh)

    @pl.loop(0, model // step)
    def _(i):
        cols = pl.ds(pl.multiple_of(i * step, step), step)
        dd_ref[:, cols] = dot(h_ref[...], dy_ref[:, cols], TN)
        dg_ref[cols, :] = dot(x_ref[:, cols], da_ref[...], TN)
        du_ref[cols, :] = dot(x_ref[:, cols], db_ref[...], TN)


def shared_grad(x_all, dy_all, ws_gate, ws_up, ws_down):
    tokens, model = x_all.shape
    width = ws_gate.shape[1]
    block = min(width, 256)
    full = pl.BlockSpec((tokens, model), lambda i: (0, 0), pipeline_mode=pl.Buffered(1))
    col = pl.BlockSpec((model, block), lambda i: (0, i))
    row = pl.BlockSpec((block, model), lambda i: (i, 0))
    return pl.pallas_call(
        functools.partial(shared_grad_kernel, 256),
        grid=(width // block,),
        in_specs=[full, full, col, col, row],
        out_specs=[col, col, row],
        out_shape=[jax.ShapeDtypeStruct((model, width), F32)] * 2 + [jax.ShapeDtypeStruct((width, model), F32)],
        scratch_shapes=[pltpu.VMEM((tokens, block), BF16)] * 3,
        cost_estimate=pl.CostEstimate(
            flops=12 * tokens * model * width, bytes_accessed=4 * tokens * model + 18 * model * width,
            transcendentals=tokens * width),
        compiler_params=pltpu.CompilerParams(dimension_semantics=('arbitrary',), vmem_limit_bytes=48 << 20),
        name='shared_grad',
    )(x_all, dy_all, ws_gate, ws_up, ws_down)


def split3(v):
    hi = lax.reduce_precision(v, 8, 7)
    rest = v - hi
    mid = lax.reduce_precision(rest, 8, 7)
    low = rest - mid
    return hi.astype(BF16), mid.astype(BF16), low.astype(BF16)


def sum3(v, axis):
    first, second, third = jnp.split(v, 3, axis=axis)
    return first + second + third


def core_partner(ep):
    return ep + 1 - 2 * (ep % 2)


def gather_kernel(x_ref, idx_ref, dy_ref, wg_ref, wu_ref, wd_ref, x_all, idx_all, dy_pair, wd_part, quarter, send_sem, recv_sem, idx_send, idx_recv, local_sem, x_buf, dy_buf, q_buf):
    tp = lax.axis_index('tp')
    ep = lax.axis_index('ep')
    eps = x_all.shape[0] // 2
    half = eps // 2
    tp_o = 1 - tp
    ep_x = (ep + half) % eps
    ep_c = core_partner(ep)

    def slot(e, t):
        return e * 2 + t

    others = [(tp_o, ep)]
    for k in range(1, eps):
        others += [(tp, (ep + k) % eps), (tp_o, (ep + k) % eps)]
    barrier = pltpu.get_barrier_semaphore()
    for t, e in others:
        pl.semaphore_signal(barrier, inc=1, device_id={'tp': t, 'ep': e}, device_id_type=MESH)
    pl.semaphore_wait(barrier, len(others))

    def send(k, src, dst, t, e):
        copy = pltpu.make_async_remote_copy(
            src_ref=src, dst_ref=dst, send_sem=send_sem.at[k], recv_sem=recv_sem.at[k],
            device_id={'tp': t, 'ep': e}, device_id_type=MESH)
        copy.start()
        return copy

    def block(e, t):
        return x_all.at[slot(e, t)]

    mine = block(ep, tp)
    to_y = send(0, x_ref, mine, tp_o, ep)
    to_x = send(1, x_ref, mine, tp, ep_x)
    to_c = send(2, x_ref, mine, tp, ep_c)
    own_idx = idx_all.at[slot(ep, tp)]
    idx_copies = []
    for k, (t, e) in enumerate(others):
        copy = pltpu.make_async_remote_copy(
            src_ref=idx_ref, dst_ref=own_idx, send_sem=idx_send.at[k], recv_sem=idx_recv.at[k],
            device_id={'tp': t, 'ep': e}, device_id_type=MESH)
        copy.start()
        idx_copies.append(copy)
    width = quarter.shape[1] // 2
    cols = pl.ds(pl.multiple_of(ep * width, width), width)
    load = [
        pltpu.make_async_copy(x_ref, x_buf, local_sem.at[0]),
        pltpu.make_async_copy(dy_ref, dy_buf, local_sem.at[1]),
        pltpu.make_async_copy(wg_ref.at[:, cols], q_buf.at[:, pl.ds(0, width)], local_sem.at[2]),
        pltpu.make_async_copy(wu_ref.at[:, cols], q_buf.at[:, pl.ds(width, width)], local_sem.at[3]),
    ]
    store = [
        pltpu.make_async_copy(x_buf, mine, local_sem.at[4]),
        pltpu.make_async_copy(dy_buf, dy_pair.at[tp], local_sem.at[5]),
        pltpu.make_async_copy(q_buf, quarter, local_sem.at[6]),
        pltpu.make_async_copy(idx_ref, own_idx, local_sem.at[7]),
    ]
    for copy in load:
        copy.start()
    dy_y = send(3, dy_ref, dy_pair.at[tp], tp_o, ep)
    rows = wd_part.shape[0]
    wd_y = send(4, wd_ref.at[pl.ds(ep * rows, rows)], wd_part, tp_o, ep)

    for copy in load:
        copy.wait()
    for copy in store:
        copy.start()
    to_y.wait_recv()
    y_to_x = send(5, block(ep, tp_o), block(ep, tp_o), tp, ep_x)
    y_to_c = send(6, block(ep, tp_o), block(ep, tp_o), tp, ep_c)
    to_x.wait_recv()
    x_to_c = send(7, block(ep_x, tp), block(ep_x, tp), tp, ep_c)
    y_to_x.wait_recv()
    xy_to_c = send(8, block(ep_x, tp_o), block(ep_x, tp_o), tp, ep_c)
    for copy in (to_c, dy_y, wd_y, y_to_c, x_to_c, xy_to_c):
        copy.wait_recv()
    for copy in idx_copies:
        copy.wait_recv()
    for copy in store:
        copy.wait()
    for copy in (to_y, to_x, to_c, dy_y, wd_y, y_to_x, y_to_c, x_to_c, xy_to_c):
        copy.wait_send()
    for copy in idx_copies:
        copy.wait_send()


def gather_rows(devices, ep_size, x, idx_t, dy, ws_gate, ws_up, ws_down):
    _, model = x.shape
    any_spec = pl.BlockSpec(memory_space=pl.ANY)
    return pl.pallas_call(
        gather_kernel,
        in_specs=[any_spec] * 6,
        out_specs=[any_spec] * 5,
        out_shape=[
            jax.ShapeDtypeStruct((devices,) + x.shape, x.dtype),
            jax.ShapeDtypeStruct((devices,) + idx_t.shape, idx_t.dtype),
            jax.ShapeDtypeStruct((2,) + dy.shape, dy.dtype),
            jax.ShapeDtypeStruct((ws_down.shape[0] // ep_size, model), ws_down.dtype),
            jax.ShapeDtypeStruct((model, 2 * ws_gate.shape[1] // ep_size), ws_gate.dtype),
        ],
        scratch_shapes=[
            pltpu.SemaphoreType.DMA((9,)),
            pltpu.SemaphoreType.DMA((9,)),
            pltpu.SemaphoreType.DMA((devices - 1,)),
            pltpu.SemaphoreType.DMA((devices - 1,)),
            pltpu.SemaphoreType.DMA((8,)),
            pltpu.VMEM(x.shape, x.dtype),
            pltpu.VMEM(dy.shape, dy.dtype),
            pltpu.VMEM((model, 2 * ws_gate.shape[1] // ep_size), ws_gate.dtype),
        ],
        cost_estimate=pl.CostEstimate(flops=60_000_000_000, bytes_accessed=4 * devices * x.size, transcendentals=0),
        compiler_params=pltpu.CompilerParams(collective_id=0, has_side_effects=True),
        name='gather_rows',
    )(x, idx_t, dy, ws_gate, ws_up, ws_down)


def solution(mesh):
    tp_size = mesh.shape['tp']
    ep_size = mesh.shape['ep']
    swap_tp = [(i, tp_size - 1 - i) for i in range(tp_size)]
    swap_x = [(i, (i + ep_size // 2) % ep_size) for i in range(ep_size)]
    swap_c = [(i, core_partner(i)) for i in range(ep_size)]

    def device_step(x, grad_y, w_router, w_gate, w_up, w_down, ws_gate, ws_up, ws_down, topk_idx):
        tok, model = x.shape
        top_k = topk_idx.shape[1]
        experts = w_router.shape[1]
        local_exp = w_gate.shape[0]
        groups = top_k // 2
        most = groups * tok // (2 * ep_size) + min(groups, ep_size // 2) * tok // ep_size
        cap = (2 * most + local_exp - 1) // local_exp
        half, padded = half_rows(cap, ep_size)
        shift = padded - half
        ep_i = lax.axis_index('ep')
        tp_i = lax.axis_index('tp')
        devices = ep_size * tp_size
        ep_order = (ep_i, (ep_i + ep_size // 2) % ep_size, core_partner(ep_i), core_partner((ep_i + ep_size // 2) % ep_size))

        def ep_pieces(piece):
            far = lax.ppermute(piece, 'ep', swap_x)
            return piece, far, lax.ppermute(piece, 'ep', swap_c), lax.ppermute(far, 'ep', swap_c)

        def ep_gather(piece):
            out = jnp.zeros((ep_size,) + piece.shape, piece.dtype)
            for e, part in zip(ep_order, ep_pieces(piece)):
                out = lax.dynamic_update_slice_in_dim(out, part[None], e, 0)
            return out

        x_blocks, idx_all, dy_pair, wd_part, quarter = gather_rows(devices, ep_size, x, topk_idx.T, grad_y, ws_gate, ws_up, ws_down)
        x_all = x_blocks.reshape(devices * tok, model)

        width_q = ws_gate.shape[1] // ep_size
        gu_part = lax.ppermute(quarter, 'tp', swap_tp)

        lower = (lax.broadcasted_iota(jnp.int32, (tok, tok), 0) > lax.broadcasted_iota(jnp.int32, (tok, tok), 1)).astype(BF16)
        local_ids = ep_i * local_exp + jnp.arange(local_exp, dtype=jnp.int32)
        hit = jnp.any(idx_all[None] == local_ids[:, None, None, None], axis=2)
        rank = jnp.einsum('edj,ij->edi', hit.astype(BF16), lower, preferred_element_type=F32).astype(jnp.int32)
        dev = jnp.arange(devices, dtype=jnp.int32)
        is_own = (dev % tp_size) == tp_i
        parity = jnp.arange(local_exp, dtype=jnp.int32) % 2
        base = (jnp.where(is_own, padded, 0) + (dev // tp_size) * cap)[None, :] + (parity * shift)[:, None]
        row_ids = jnp.where(hit, base[:, :, None] + rank, -1).reshape(local_exp, 1, devices * tok)

        fwd_parts = []
        start = 0
        rows_now = row_ids
        for count in FWD_CHUNKS:
            send, own = expert_fwd(start, count, half, padded, x_all, rows_now, w_gate, w_up, w_down)
            start += count
            rows_now, own = lax.optimization_barrier((rows_now, own))
            fwd_parts.append((lax.ppermute(send, 'tp', swap_tp), own))

        own0 = fwd_parts[-1][1]
        x_late, hit, rank, w_router, own0 = lax.optimization_barrier((x_all, hit, rank, w_router, own0))
        fwd_parts[-1] = (fwd_parts[-1][0], own0)

        logits_t = jnp.einsum('de,td->et', w_router, x_late, preferred_element_type=F32)
        probs_t = jax.nn.softmax(logits_t, axis=0)
        gates_local = GATE_SCALE * lax.dynamic_slice_in_dim(probs_t, ep_i * local_exp, local_exp, 0).reshape(local_exp, 1, devices * tok)

        sizes = windows(cap, ep_size)
        other, win_other, near, win_near = sizes
        per_chunk = local_exp // BWD_CHUNKS
        dev_ep = dev // tp_size
        place = jnp.zeros_like(dev)
        for k, e in enumerate(ep_order[1:]):
            place = jnp.where(dev_ep == e, k * cap, place)
        exp = jnp.arange(local_exp, dtype=jnp.int32)
        far_first = (jnp.where(is_own, win_other, 0) + place)[None, :] + ((exp % per_chunk) * other % 8)[:, None]
        near_first = jnp.where(is_own, win_near, 0)[None, :] + (2 * win_other + exp * near % 8)[:, None]
        first = jnp.where((dev_ep == ep_i)[None, :], near_first, far_first)
        bwd_ids = jnp.where(hit, first[:, :, None] + rank, -1).reshape(local_exp, 1, devices * tok)
        dy_all = ep_gather(dy_pair).reshape(devices * tok, model)
        (d_w_gate, d_w_up, d_w_down), bwd_out = expert_bwd(BWD_CHUNKS, sizes, x_all, dy_all, bwd_ids, gates_local, w_gate, w_up, w_down)
        bwd_parts = [(lax.ppermute(bwd_out[0][0], 'tp', swap_tp), bwd_out[0][1])]

        own_last = bwd_out[-1][1]
        own_first = fwd_parts[0][1]
        gu_far = lax.ppermute(gu_part, 'ep', swap_x)
        wd_far = lax.ppermute(wd_part, 'ep', swap_x)
        x, grad_y, x_all, dy_all, topk_idx, w_router, gu_part, wd_part, gu_far, wd_far, own_first, own_last = lax.optimization_barrier(
            (x, grad_y, x_all, dy_all, topk_idx, w_router, gu_part, wd_part, gu_far, wd_far, own_first, own_last))
        fwd_parts[0] = (fwd_parts[0][0], own_first)
        bwd_out[-1] = (bwd_out[-1][0], own_last)

        def back_rows(count):
            return count * cap + (-count * cap) % 8

        def slot_index(count):
            new = jnp.arange(ep_size * back_rows(count), dtype=jnp.int32)
            block, rest = new // back_rows(count), new % back_rows(count)
            return block, rest // cap, rest % cap, rest < count * cap

        def turn(parts, count):
            recv, own = parts
            rows = (recv + own).astype(BF16)
            src, exp, rank, valid = slot_index(count)
            old = jnp.where(valid, exp * half + src * cap + rank, -1)
            perm = (old[:, None] == jnp.arange(count * half, dtype=jnp.int32)[None, :]).astype(BF16)
            return dot(perm, rows).astype(BF16)

        def send_home(out, count):
            out = out.reshape(ep_size, back_rows(count), model)
            out = lax.all_to_all(out, 'ep', 0, 0)
            return out.reshape(ep_size * back_rows(count), model)

        early = RETURN_ORDER[0]
        early_rows = turn(fwd_parts[early], FWD_CHUNKS[early])
        x, grad_y, topk_idx, gu_part, wd_part, gu_far, wd_far, early_rows = lax.optimization_barrier(
            (x, grad_y, topk_idx, gu_part, wd_part, gu_far, wd_far, early_rows))
        early_back = send_home(early_rows, FWD_CHUNKS[early])

        gu_other = (gu_part, gu_far, lax.ppermute(gu_part, 'ep', swap_c), lax.ppermute(gu_far, 'ep', swap_c))
        wd_other = jnp.concatenate((wd_part, wd_far, lax.ppermute(wd_part, 'ep', swap_c), lax.ppermute(wd_far, 'ep', swap_c)), axis=0)
        wg_other = jnp.concatenate([p[:, :width_q] for p in gu_other], axis=1)
        wu_other = jnp.concatenate([p[:, width_q:] for p in gu_other], axis=1)
        shared = jnp.zeros((tok, model), F32)
        dx_shared = jnp.zeros((tok, model), F32)
        for wg, wu, wd in ((ws_gate, ws_up, ws_down), (wg_other, wu_other, wd_other)):
            a = rounded(dot(x, wg))
            b = rounded(dot(x, wu))
            dh = rounded(dot(grad_y, wd, NT))
            h, da, db = swiglu_bwd(a, b, dh)
            shared = shared + dot(h, wd)
            dx_shared = dx_shared + dot(da, wg, NT) + dot(db, wu, NT)
        ds_gate, ds_up, ds_down = shared_grad(x_all, dy_all, ws_gate, ws_up, ws_down)

        hit_own = jnp.any(topk_idx[:, None, :] == jnp.arange(experts, dtype=jnp.int32)[None, :, None], axis=2)
        rank_own = dot(lower, hit_own.astype(BF16))
        want = jnp.where(hit_own, rank_own, -1.0).astype(BF16)
        probs = jax.nn.softmax(dot(x, w_router), axis=-1)
        prob_parts = jnp.concatenate(split3(probs), axis=0)

        def expand(start, count):
            grp, exp, rank, valid = slot_index(count)
            col = jnp.where(valid, grp * local_exp + start + exp, -1)
            table = (jnp.arange(experts, dtype=jnp.int32)[:, None] == col[None, :]).astype(BF16)
            return table, jnp.where(valid, rank, -2).astype(F32)[None, :]

        routed = jnp.zeros((tok, model), F32)
        d_scores = jnp.zeros((tok, experts), F32)
        back = early_back
        for j in RETURN_ORDER:
            count, start = FWD_CHUNKS[j], sum(FWD_CHUNKS[:j])
            if j != early:
                recv, own = fwd_parts[j]
                back, own = lax.optimization_barrier((back, own))
                back = send_home(turn((recv, own), count), count)
            table, rank = expand(start, count)
            hits = dot(want, table) == rank
            gates = jnp.where(jnp.concatenate([hits] * 3, axis=0), dot(prob_parts, table), 0.0).astype(BF16)
            mixed = dot(gates, back)
            routed = routed + GATE_SCALE * sum3(mixed, 0)
            score = jnp.where(hits, dot(grad_y, back, NT), 0.0)
            part = dot(jnp.concatenate(split3(score), axis=0), table, NT)
            d_scores = d_scores + sum3(part, 0)
        y_out = (shared + routed).astype(BF16)

        d_scores = GATE_SCALE * d_scores
        mean_score = jnp.sum(probs * d_scores, axis=-1, keepdims=True)
        d_logits = probs * (d_scores - mean_score)
        d_other = lax.ppermute(d_logits, 'tp', swap_tp)
        for send, own in bwd_out[1:]:
            bwd_parts.append((lax.ppermute(send, 'tp', swap_tp), own))
        d_pair = jnp.where(tp_i == 0, jnp.stack([d_logits, d_other]), jnp.stack([d_other, d_logits]))
        d_logits_all = ep_gather(d_pair).reshape(devices * tok, experts)
        d_router = dot(x_all, jnp.concatenate(split3(d_logits_all), axis=1), TN)
        d_router = sum3(d_router, 1)
        dx_sum = dx_shared + sum3(dot(jnp.concatenate(split3(d_logits), axis=0), w_router, NT), 0)

        def hits_of(grp, start, count):
            slot = jnp.arange(count * cap, dtype=jnp.int32)
            col = grp * local_exp + start + slot // cap
            table = (jnp.arange(experts, dtype=jnp.int32)[:, None] == col[None, :]).astype(BF16)
            return (dot(want, table) == (slot % cap).astype(F32)[None, :]).astype(BF16)

        swaps = (swap_x, swap_c, [(i, core_partner(d)) for i, d in swap_x])

        def join_near(c, total):
            recv, own = bwd_parts[BWD_CHUNKS + c]
            hits = hits_of(ep_i, c * per_chunk, per_chunk)
            return total + dot(hits, (recv + own).astype(BF16))

        for c, (recv, own) in enumerate(bwd_parts[:BWD_CHUNKS]):
            rows = (recv + own).astype(BF16)
            slot = jnp.arange(per_chunk * cap, dtype=jnp.int32)
            for k, pairs in enumerate(swaps):
                old = slot // cap * other + k * cap + slot % cap
                perm = (old[:, None] == jnp.arange(per_chunk * other, dtype=jnp.int32)[None, :]).astype(BF16)
                back = dot(perm, rows).astype(BF16)
                back = lax.ppermute(back, 'ep', pairs)
                hits = hits_of(ep_order[1 + k], c * per_chunk, per_chunk)
                dx_sum = dx_sum + dot(hits, back)
            if c + 1 < BWD_CHUNKS:
                dx_sum = join_near(c, lax.optimization_barrier(dx_sum))
            dx_sum = lax.optimization_barrier(dx_sum)
        dx_sum = join_near(BWD_CHUNKS - 1, dx_sum)
        return y_out, dx_sum.astype(BF16), d_router, d_w_gate, d_w_up, d_w_down, ds_gate, ds_up, ds_down

    tok_spec = P(('ep', 'tp'), None)
    in_specs = (tok_spec, tok_spec, P(None, None), P('ep', None, 'tp'), P('ep', None, 'tp'), P('ep', 'tp', None), P(None, 'tp'), P(None, 'tp'), P('tp', None), tok_spec)
    out_specs = (tok_spec, tok_spec, P(None, None), P('ep', None, 'tp'), P('ep', None, 'tp'), P('ep', 'tp', None), P(None, 'tp'), P(None, 'tp'), P('tp', None))

    return jax.shard_map(device_step, mesh=mesh, in_specs=in_specs, out_specs=out_specs, check_vma=False)
```
